16 devices in a mesh: ep: 16 (over z, y, x, core).
Axes of the slice: x: 2, y: 2, z: 2, core: 2. Of those that a mesh axis runs over, the one named last changes fastest.
Arguments:
- tokens: bfloat16 [2048, 4096], P('ep')
- k_cache: bfloat16 [2048, 256, 4, 128], P('ep')
- v_cache: bfloat16 [2048, 256, 4, 128], P('ep')
- positions: int32 [2048], P('ep')
- expert_one: int32 [2048], P('ep')
- expert_two: int32 [2048], P('ep')
- eligible: int32 [2048, 16], P('ep')
- ln1_gain: bfloat16 [4096], replicated
- ln1_bias: bfloat16 [4096], replicated
- w_query: bfloat16 [4096, 2048], replicated
- b_query: bfloat16 [2048], replicated
- w_key: bfloat16 [4096, 512], replicated
- b_key: bfloat16 [512], replicated
- w_value: bfloat16 [4096, 512], replicated
- b_value: bfloat16 [512], replicated
- w_out: bfloat16 [2048, 4096], replicated
- b_out: bfloat16 [4096], replicated
- ln2_gain: bfloat16 [4096], replicated
- ln2_bias: bfloat16 [4096], replicated
- w_router: bfloat16 [4096, 16], replicated
- w_gate: bfloat16 [16, 4096, 448], P('ep')
- w_up: bfloat16 [16, 4096, 448], P('ep')
- w_down: bfloat16 [16, 448, 4096], P('ep')
Outputs:
- output 1: bfloat16 [2048, 4096], P('ep')
- output 2: bfloat16 [2048, 4, 128], P('ep')
- output 3: bfloat16 [2048, 4, 128], P('ep')
All inputs are finite; a program needn't handle non-finite values.
Results may differ from the reference program's by a relative error of at most 0.00967011.
Values are sent between devices in bfloat16 or wider.
A program may use at most 1 GiB of HBM per device.

```python
import jax
import jax.numpy as jnp
from jax import lax

D_MODEL = 4096
NUM_HEADS = 16
NUM_KV_HEADS = 4
HEAD_DIM = 128
FF_DIM = 448
NUM_EXPERTS = 16
TOK_DEV = 128
SEQ_LEN = 256
NUM_GROUPS = 16
BATCH = TOK_DEV * NUM_GROUPS
GROUP_SIZE = NUM_HEADS // NUM_KV_HEADS
Q_DIM = NUM_HEADS * HEAD_DIM
KV_DIM = NUM_KV_HEADS * HEAD_DIM
ROPE_BASE = 10000.0
LN_EPS = 1e-5


def draw_normal(key, arr_shape, std_dev):
    return (jax.random.normal(key, arr_shape, jnp.float32) * std_dev).astype(jnp.bfloat16)


def draw_positions(key):
    k_pos, k_top, k_low = jax.random.split(key, 3)
    row_ids = jnp.arange(BATCH)
    pos_vals = jax.random.randint(k_pos, (BATCH,), 0, SEQ_LEN)
    top_row = jax.random.randint(k_top, (), 0, BATCH)
    low_row = (top_row + 1 + jax.random.randint(k_low, (), 0, BATCH - 1)) % BATCH
    pos_vals = jnp.where(row_ids == top_row, SEQ_LEN - 1, pos_vals)
    return jnp.where(row_ids == low_row, 0, pos_vals).astype(jnp.int32)


def draw_routes(key):
    k_mix, k_hot, k_src, k_rot, k_sec, k_elig = jax.random.split(key, 6)
    row_ids = jnp.arange(BATCH)
    mix_draw = jax.random.randint(k_mix, (BATCH,), 0, 4 * NUM_EXPERTS)
    hot_expert = jax.random.randint(k_hot, (), 0, NUM_EXPERTS)
    first_choice = jnp.where(mix_draw < 2 * NUM_EXPERTS, mix_draw % NUM_EXPERTS, (hot_expert + mix_draw % 2) % NUM_EXPERTS)
    src_group = jax.random.randint(k_src, (), 0, NUM_GROUPS)
    first_choice = jnp.where(row_ids // TOK_DEV == src_group, hot_expert, first_choice)
    rotation = jax.random.randint(k_rot, (), 0, NUM_EXPERTS)
    offset_rows = (row_ids - (src_group + 1) * TOK_DEV) % BATCH
    first_choice = jnp.where(offset_rows < NUM_EXPERTS, (offset_rows + rotation) % NUM_EXPERTS, first_choice)
    second_choice = (first_choice + 1 + jax.random.randint(k_sec, (BATCH,), 0, NUM_EXPERTS - 1)) % NUM_EXPERTS
    expert_ids = jnp.arange(NUM_EXPERTS)[None, :]
    extra_elig = jax.random.randint(k_elig, (BATCH, NUM_EXPERTS), 0, 8) == 0
    eligible = extra_elig | (expert_ids == first_choice[:, None]) | (expert_ids == second_choice[:, None])
    return first_choice.astype(jnp.int32), second_choice.astype(jnp.int32), eligible.astype(jnp.int32)


def setup_inputs(seed: int = 0) -> dict:
    keys = jax.random.split(jax.random.key(seed), 22)
    expert_one, expert_two, eligible = draw_routes(keys[0])
    value_mean = jax.random.normal(keys[3], (BATCH, 1, NUM_KV_HEADS, HEAD_DIM), jnp.float32)
    value_draw = jax.random.normal(keys[4], (BATCH, SEQ_LEN, NUM_KV_HEADS, HEAD_DIM), jnp.float32)
    ln1_gain = (1.0 + 0.3 * jax.random.normal(keys[6], (D_MODEL,), jnp.float32)).astype(jnp.bfloat16)
    ln2_gain = (1.0 + 0.3 * jax.random.normal(keys[16], (D_MODEL,), jnp.float32)).astype(jnp.bfloat16)
    return {
        'tokens': draw_normal(keys[1], (BATCH, D_MODEL), 1.0),
        'k_cache': draw_normal(keys[2], (BATCH, SEQ_LEN, NUM_KV_HEADS, HEAD_DIM), 2.0),
        'v_cache': (value_draw + value_mean).astype(jnp.bfloat16),
        'positions': draw_positions(keys[5]),
        'expert_one': expert_one,
        'expert_two': expert_two,
        'eligible': eligible,
        'ln1_gain': ln1_gain,
        'ln1_bias': draw_normal(keys[7], (D_MODEL,), 0.3),
        'w_query': draw_normal(keys[8], (D_MODEL, Q_DIM), D_MODEL ** -0.5),
        'b_query': draw_normal(keys[9], (Q_DIM,), 0.5),
        'w_key': draw_normal(keys[10], (D_MODEL, KV_DIM), D_MODEL ** -0.5),
        'b_key': draw_normal(keys[11], (KV_DIM,), 0.5),
        'w_value': draw_normal(keys[12], (D_MODEL, KV_DIM), D_MODEL ** -0.5),
        'b_value': draw_normal(keys[13], (KV_DIM,), 0.5),
        'w_out': draw_normal(keys[14], (Q_DIM, D_MODEL), Q_DIM ** -0.5),
        'b_out': draw_normal(keys[15], (D_MODEL,), 0.3),
        'ln2_gain': ln2_gain,
        'ln2_bias': draw_normal(keys[17], (D_MODEL,), 0.3),
        'w_router': draw_normal(keys[18], (D_MODEL, NUM_EXPERTS), D_MODEL ** -0.5),
        'w_gate': draw_normal(keys[19], (NUM_EXPERTS, D_MODEL, FF_DIM), D_MODEL ** -0.5),
        'w_up': draw_normal(keys[20], (NUM_EXPERTS, D_MODEL, FF_DIM), D_MODEL ** -0.5),
        'w_down': draw_normal(keys[21], (NUM_EXPERTS, FF_DIM, D_MODEL), FF_DIM ** -0.5),
    }


def layer_norm(values_in, gain, bias):
    mean_val = jnp.mean(values_in, axis=-1, keepdims=True)
    centered = values_in - mean_val
    var_val = jnp.mean(centered * centered, axis=-1, keepdims=True)
    return centered * lax.rsqrt(var_val + LN_EPS) * gain.astype(jnp.float32) + bias.astype(jnp.float32)


def rope_tables(positions):
    half_dim = HEAD_DIM // 2
    inv_freq = ROPE_BASE ** (jnp.arange(half_dim, dtype=jnp.float32) * (-2.0 / HEAD_DIM))
    angles = positions.astype(jnp.float32)[:, None] * inv_freq[None, :]
    angles = jnp.concatenate([angles, angles], axis=-1)
    return jnp.cos(angles), jnp.sin(angles)


def apply_rope(values_in, cos_tab, sin_tab):
    half_dim = values_in.shape[-1] // 2
    rotated = jnp.concatenate([-values_in[..., half_dim:], values_in[..., :half_dim]], axis=-1)
    return values_in * cos_tab[:, None, :] + rotated * sin_tab[:, None, :]


def attend_one(seq_parts):
    q_seq, k_seq, v_seq, k_one, v_one, pos_one = seq_parts
    score_scale = HEAD_DIM ** -0.5
    q_f = q_seq.astype(jnp.float32)
    s_cache = jnp.einsum('kgd,skd->kgs', q_f, k_seq.astype(jnp.float32)) * score_scale
    valid_mask = jnp.arange(SEQ_LEN)[None, None, :] < pos_one
    s_cache = jnp.where(valid_mask, s_cache, -jnp.inf)
    s_new = jnp.einsum('kgd,kd->kg', q_f, k_one.astype(jnp.float32)) * score_scale
    top_val = jnp.maximum(jnp.max(s_cache, axis=-1), s_new)
    e_cache = jnp.exp(s_cache - top_val[..., None])
    e_new = jnp.exp(s_new - top_val)
    denom_sum = jnp.sum(e_cache, axis=-1) + e_new
    p_cache = (e_cache / denom_sum[..., None]).astype(jnp.bfloat16).astype(jnp.float32)
    p_new = (e_new / denom_sum).astype(jnp.bfloat16).astype(jnp.float32)
    attn_vals = jnp.einsum('kgs,skd->kgd', p_cache, v_seq.astype(jnp.float32))
    return attn_vals + p_new[..., None] * v_one.astype(jnp.float32)[:, None, :]


def router_gates(h_two, w_router, expert_one, expert_two, eligible):
    logits = jnp.dot(h_two, w_router, preferred_element_type=jnp.float32)
    expert_ids = jnp.arange(NUM_EXPERTS)[None, :]
    hit_one = expert_ids == expert_one[:, None]
    hit_two = expert_ids == expert_two[:, None]
    keep_one = eligible == 1
    keep_two = keep_one & jnp.logical_not(hit_one)
    prob_one = jax.nn.softmax(jnp.where(keep_one, logits, -jnp.inf), axis=-1)
    prob_two = jax.nn.softmax(jnp.where(keep_two, logits, -jnp.inf), axis=-1)
    gate_one = jnp.sum(jnp.where(hit_one, prob_one, 0.0), axis=-1)
    gate_two = jnp.sum(jnp.where(hit_two, prob_two, 0.0), axis=-1)
    return gate_one, gate_two


def reference(tokens, k_cache, v_cache, positions, expert_one, expert_two, eligible, ln1_gain, ln1_bias, w_query, b_query, w_key, b_key, w_value, b_value, w_out, b_out, ln2_gain, ln2_bias, w_router, w_gate, w_up, w_down):
    x_f = tokens.astype(jnp.float32)
    h_one = layer_norm(x_f, ln1_gain, ln1_bias).astype(jnp.bfloat16)
    cos_tab, sin_tab = rope_tables(positions)
    q_lin = jnp.dot(h_one, w_query, preferred_element_type=jnp.float32) + b_query.astype(jnp.float32)
    q_rot = apply_rope(q_lin.reshape(BATCH, NUM_HEADS, HEAD_DIM), cos_tab, sin_tab).astype(jnp.bfloat16)
    k_lin = jnp.dot(h_one, w_key, preferred_element_type=jnp.float32) + b_key.astype(jnp.float32)
    key_new = apply_rope(k_lin.reshape(BATCH, NUM_KV_HEADS, HEAD_DIM), cos_tab, sin_tab).astype(jnp.bfloat16)
    v_lin = jnp.dot(h_one, w_value, preferred_element_type=jnp.float32) + b_value.astype(jnp.float32)
    value_new = v_lin.astype(jnp.bfloat16).reshape(BATCH, NUM_KV_HEADS, HEAD_DIM)
    q_grp = q_rot.reshape(BATCH, NUM_KV_HEADS, GROUP_SIZE, HEAD_DIM)
    attn_vals = lax.map(attend_one, (q_grp, k_cache, v_cache, key_new, value_new, positions))
    attn_flat = attn_vals.astype(jnp.bfloat16).reshape(BATCH, Q_DIM)
    x_mid = (x_f + jnp.dot(attn_flat, w_out, preferred_element_type=jnp.float32) + b_out.astype(jnp.float32)).astype(jnp.bfloat16)
    h_two = layer_norm(x_mid.astype(jnp.float32), ln2_gain, ln2_bias).astype(jnp.bfloat16)
    gate_one, gate_two = router_gates(h_two, w_router, expert_one, expert_two, eligible)

    def expert_step(acc_sum, expert_parts):
        gate_w, up_w, down_w, expert_idx = expert_parts
        u_val = jnp.dot(h_two, gate_w, preferred_element_type=jnp.float32)
        v_val = jnp.dot(h_two, up_w, preferred_element_type=jnp.float32)
        z_val = (jax.nn.silu(u_val) * v_val).astype(jnp.bfloat16)
        out_val = jnp.dot(z_val, down_w, preferred_element_type=jnp.float32).astype(jnp.bfloat16)
        weight_col = jnp.where(expert_one == expert_idx, gate_one, 0.0) + jnp.where(expert_two == expert_idx, gate_two, 0.0)
        return acc_sum + weight_col[:, None] * out_val.astype(jnp.float32), None

    y_sum, _ = lax.scan(expert_step, jnp.zeros((BATCH, D_MODEL), jnp.float32), (w_gate, w_up, w_down, jnp.arange(NUM_EXPERTS)))
    tokens_out = (x_mid.astype(jnp.float32) + y_sum).astype(jnp.bfloat16)
    return tokens_out, key_new, value_new
```

```python
import jax
import jax.numpy as jnp
from jax import lax
from jax.sharding import PartitionSpec as P

ROPE_BASE = 10000.0
LN_EPS = 1e-5


def layer_norm(values_in, gain, bias):
    mean_val = jnp.mean(values_in, axis=-1, keepdims=True)
    centered = values_in - mean_val
    var_val = jnp.mean(centered * centered, axis=-1, keepdims=True)
    return centered * lax.rsqrt(var_val + LN_EPS) * gain.astype(jnp.float32) + bias.astype(jnp.float32)


def rope_tables(positions, head_dim):
    half_dim = head_dim // 2
    inv_freq = ROPE_BASE ** (jnp.arange(half_dim, dtype=jnp.float32) * (-2.0 / head_dim))
    angles = positions.astype(jnp.float32)[:, None] * inv_freq[None, :]
    angles = jnp.concatenate([angles, angles], axis=-1)
    return jnp.cos(angles), jnp.sin(angles)


def apply_rope(values_in, cos_tab, sin_tab):
    half_dim = values_in.shape[-1] // 2
    rotated = jnp.concatenate([-values_in[..., half_dim:], values_in[..., :half_dim]], axis=-1)
    return values_in * cos_tab[:, None, :] + rotated * sin_tab[:, None, :]


def attention_block(tokens, k_cache, v_cache, positions, ln1_gain, ln1_bias, w_query, b_query, w_key, b_key, w_value, b_value, w_out, b_out):
    tok_count, seq_len, kv_heads, head_dim = k_cache.shape
    num_heads = w_query.shape[1] // head_dim
    group_size = num_heads // kv_heads
    x_f = tokens.astype(jnp.float32)
    h_one = layer_norm(x_f, ln1_gain, ln1_bias).astype(jnp.bfloat16)
    cos_tab, sin_tab = rope_tables(positions, head_dim)
    q_lin = jnp.dot(h_one, w_query, preferred_element_type=jnp.float32) + b_query.astype(jnp.float32)
    q_rot = apply_rope(q_lin.reshape(tok_count, num_heads, head_dim), cos_tab, sin_tab).astype(jnp.bfloat16)
    q_grp = q_rot.reshape(tok_count, kv_heads, group_size, head_dim)
    k_lin = jnp.dot(h_one, w_key, preferred_element_type=jnp.float32) + b_key.astype(jnp.float32)
    key_new = apply_rope(k_lin.reshape(tok_count, kv_heads, head_dim), cos_tab, sin_tab).astype(jnp.bfloat16)
    v_lin = jnp.dot(h_one, w_value, preferred_element_type=jnp.float32) + b_value.astype(jnp.float32)
    value_new = v_lin.astype(jnp.bfloat16).reshape(tok_count, kv_heads, head_dim)
    score_scale = head_dim ** -0.5
    s_cache = jnp.einsum('tkgd,tskd->tkgs', q_grp, k_cache, preferred_element_type=jnp.float32) * score_scale
    valid_mask = jnp.arange(seq_len)[None, None, None, :] < positions[:, None, None, None]
    s_cache = jnp.where(valid_mask, s_cache, -jnp.inf)
    s_new = jnp.einsum('tkgd,tkd->tkg', q_grp, key_new, preferred_element_type=jnp.float32) * score_scale
    top_val = jnp.maximum(jnp.max(s_cache, axis=-1), s_new)
    e_cache = jnp.exp(s_cache - top_val[..., None])
    e_new = jnp.exp(s_new - top_val)
    denom_sum = jnp.sum(e_cache, axis=-1) + e_new
    p_cache = (e_cache / denom_sum[..., None]).astype(jnp.bfloat16)
    p_new = (e_new / denom_sum).astype(jnp.bfloat16)
    attn_vals = jnp.einsum('tkgs,tskd->tkgd', p_cache, v_cache, preferred_element_type=jnp.float32)
    attn_vals = attn_vals + p_new.astype(jnp.float32)[..., None] * value_new.astype(jnp.float32)[:, :, None, :]
    attn_flat = attn_vals.astype(jnp.bfloat16).reshape(tok_count, num_heads * head_dim)
    x_mid = (x_f + jnp.dot(attn_flat, w_out, preferred_element_type=jnp.float32) + b_out.astype(jnp.float32)).astype(jnp.bfloat16)
    return x_mid, key_new, value_new


def router_gates(h_two, w_router, expert_one, expert_two, eligible):
    logits = jnp.dot(h_two, w_router, preferred_element_type=jnp.float32)
    expert_ids = jnp.arange(logits.shape[1])[None, :]
    hit_one = expert_ids == expert_one[:, None]
    hit_two = expert_ids == expert_two[:, None]
    keep_one = eligible == 1
    keep_two = keep_one & jnp.logical_not(hit_one)
    prob_one = jax.nn.softmax(jnp.where(keep_one, logits, -jnp.inf), axis=-1)
    prob_two = jax.nn.softmax(jnp.where(keep_two, logits, -jnp.inf), axis=-1)
    gate_one = jnp.sum(jnp.where(hit_one, prob_one, 0.0), axis=-1)
    gate_two = jnp.sum(jnp.where(hit_two, prob_two, 0.0), axis=-1)
    return gate_one, gate_two


def expert_mlp(expert_in, w_gate, w_up, w_down):
    u_val = jnp.einsum('emd,edf->emf', expert_in, w_gate, preferred_element_type=jnp.float32)
    v_val = jnp.einsum('emd,edf->emf', expert_in, w_up, preferred_element_type=jnp.float32)
    z_val = (jax.nn.silu(u_val) * v_val).astype(jnp.bfloat16)
    return jnp.einsum('emf,efd->emd', z_val, w_down, preferred_element_type=jnp.float32).astype(jnp.bfloat16)


def solution(mesh):
    groups = mesh.shape['ep']

    def local_step(tokens, k_cache, v_cache, positions, expert_one, expert_two, eligible, ln1_gain, ln1_bias, w_query, b_query, w_key, b_key, w_value, b_value, w_out, b_out, ln2_gain, ln2_bias, w_router, w_gate, w_up, w_down):
        x_mid, key_new, value_new = attention_block(tokens, k_cache, v_cache, positions, ln1_gain, ln1_bias, w_query, b_query, w_key, b_key, w_value, b_value, w_out, b_out)
        h_two = layer_norm(x_mid.astype(jnp.float32), ln2_gain, ln2_bias).astype(jnp.bfloat16)
        gate_one, gate_two = router_gates(h_two, w_router, expert_one, expert_two, eligible)
        tok_count, d_model = h_two.shape
        local_experts = w_gate.shape[0]
        num_experts = local_experts * groups
        me = lax.axis_index('ep')
        all_rows = lax.all_gather(h_two, 'ep', axis=0, tiled=True)
        all_experts = lax.all_gather(jnp.stack([expert_one, expert_two], axis=1), 'ep', axis=0, tiled=True)
        expert_out = expert_mlp(all_rows[None], w_gate, w_up, w_down)[0]
        mine = (all_experts == me)[:, :, None]
        slots = jnp.where(mine, expert_out[:, None, :], jnp.zeros((), jnp.bfloat16))
        slots = slots.reshape(groups, tok_count, 2, d_model).transpose(0, 2, 1, 3).reshape(groups * 2 * tok_count, d_model)
        back = lax.psum_scatter(slots, 'ep', scatter_dimension=0, tiled=True)
        y_sum = gate_one[:, None] * back[:tok_count].astype(jnp.float32) + gate_two[:, None] * back[tok_count:].astype(jnp.float32)
        tokens_out = (x_mid.astype(jnp.float32) + y_sum).astype(jnp.bfloat16)
        return tokens_out, key_new, value_new

    row_spec = P('ep', None)
    cache_spec = P('ep', None, None, None)
    vec_spec = P('ep')
    rep_one = P(None)
    rep_two = P(None, None)
    expert_spec = P('ep', None, None)
    in_specs = (row_spec, cache_spec, cache_spec, vec_spec, vec_spec, vec_spec, row_spec, rep_one, rep_one, rep_two, rep_one, rep_two, rep_one, rep_two, rep_one, rep_two, rep_one, rep_one, rep_one, rep_two, expert_spec, expert_spec, expert_spec)
    out_specs = (row_spec, expert_spec, expert_spec)
    return jax.shard_map(local_step, mesh=mesh, in_specs=in_specs, out_specs=out_specs, check_vma=False)
```

```python
import functools

import jax
import jax.numpy as jnp
from jax import lax
from jax.experimental import pallas as pl
from jax.experimental.pallas import tpu as pltpu
from jax.sharding import PartitionSpec as P

ROPE_BASE = 10000.0
LN_EPS = 1e-5


def layer_norm(values_in, gain, bias):
    mean_val = jnp.mean(values_in, axis=-1, keepdims=True)
    centered = values_in - mean_val
    var_val = jnp.mean(centered * centered, axis=-1, keepdims=True)
    return centered * lax.rsqrt(var_val + LN_EPS) * gain.astype(jnp.float32) + bias.astype(jnp.float32)


def rope_tables(positions, head_dim):
    half_dim = head_dim // 2
    inv_freq = ROPE_BASE ** (jnp.arange(half_dim, dtype=jnp.float32) * (-2.0 / head_dim))
    angles = positions.astype(jnp.float32)[:, None] * inv_freq[None, :]
    angles = jnp.concatenate([angles, angles], axis=-1)
    return jnp.cos(angles), jnp.sin(angles)


def apply_rope(values_in, cos_tab, sin_tab):
    half_dim = values_in.shape[-1] // 2
    rotated = jnp.concatenate([-values_in[..., half_dim:], values_in[..., :half_dim]], axis=-1)
    return values_in * cos_tab[:, None, :] + rotated * sin_tab[:, None, :]


def attention_block(tokens, k_cache, v_cache, positions, ln1_gain, ln1_bias, w_query, b_query, w_key, b_key, w_value, b_value, w_out, b_out):
    tok_count, seq_len, kv_heads, head_dim = k_cache.shape
    num_heads = w_query.shape[1] // head_dim
    group_size = num_heads // kv_heads
    x_f = tokens.astype(jnp.float32)
    h_one = layer_norm(x_f, ln1_gain, ln1_bias).astype(jnp.bfloat16)
    cos_tab, sin_tab = rope_tables(positions, head_dim)
    q_lin = jnp.dot(h_one, w_query, preferred_element_type=jnp.float32) + b_query.astype(jnp.float32)
    q_rot = apply_rope(q_lin.reshape(tok_count, num_heads, head_dim), cos_tab, sin_tab).astype(jnp.bfloat16)
    q_grp = q_rot.reshape(tok_count, kv_heads, group_size, head_dim)
    k_lin = jnp.dot(h_one, w_key, preferred_element_type=jnp.float32) + b_key.astype(jnp.float32)
    key_new = apply_rope(k_lin.reshape(tok_count, kv_heads, head_dim), cos_tab, sin_tab).astype(jnp.bfloat16)
    v_lin = jnp.dot(h_one, w_value, preferred_element_type=jnp.float32) + b_value.astype(jnp.float32)
    value_new = v_lin.astype(jnp.bfloat16).reshape(tok_count, kv_heads, head_dim)
    score_scale = head_dim ** -0.5
    s_cache = jnp.einsum('tkgd,tskd->tkgs', q_grp, k_cache, preferred_element_type=jnp.float32) * score_scale
    valid_mask = jnp.arange(seq_len)[None, None, None, :] < positions[:, None, None, None]
    s_cache = jnp.where(valid_mask, s_cache, -jnp.inf)
    s_new = jnp.einsum('tkgd,tkd->tkg', q_grp, key_new, preferred_element_type=jnp.float32) * score_scale
    top_val = jnp.maximum(jnp.max(s_cache, axis=-1), s_new)
    e_cache = jnp.exp(s_cache - top_val[..., None])
    e_new = jnp.exp(s_new - top_val)
    denom_sum = jnp.sum(e_cache, axis=-1) + e_new
    p_cache = (e_cache / denom_sum[..., None]).astype(jnp.bfloat16)
    p_new = (e_new / denom_sum).astype(jnp.bfloat16)
    attn_vals = jnp.einsum('tkgs,tskd->tkgd', p_cache, v_cache, preferred_element_type=jnp.float32)
    attn_vals = attn_vals + p_new.astype(jnp.float32)[..., None] * value_new.astype(jnp.float32)[:, :, None, :]
    attn_flat = attn_vals.astype(jnp.bfloat16).reshape(tok_count, num_heads * head_dim)
    x_mid = (x_f + jnp.dot(attn_flat, w_out, preferred_element_type=jnp.float32) + b_out.astype(jnp.float32)).astype(jnp.bfloat16)
    return x_mid, key_new, value_new


def router_gates(h_two, w_router, expert_one, expert_two, eligible):
    logits = jnp.dot(h_two, w_router, preferred_element_type=jnp.float32)
    expert_ids = jnp.arange(logits.shape[1])[None, :]
    hit_one = expert_ids == expert_one[:, None]
    hit_two = expert_ids == expert_two[:, None]
    keep_one = eligible == 1
    keep_two = keep_one & jnp.logical_not(hit_one)
    prob_one = jax.nn.softmax(jnp.where(keep_one, logits, -jnp.inf), axis=-1)
    prob_two = jax.nn.softmax(jnp.where(keep_two, logits, -jnp.inf), axis=-1)
    gate_one = jnp.sum(jnp.where(hit_one, prob_one, 0.0), axis=-1)
    gate_two = jnp.sum(jnp.where(hit_two, prob_two, 0.0), axis=-1)
    return gate_one, gate_two


MESH = pl.DeviceIdType.MESH
ORDERS = ((1, 2, 4), (2, 4, 1), (4, 1, 2))
LANES = 128
WIDTH = 256


def flip(me, bit):
    return me + bit - 2 * bit * ((me // bit) % 2)


def meet_neighbours():
    me = lax.axis_index('ep')
    barrier = pltpu.get_barrier_semaphore()
    for bit in (1, 2, 4, 8):
        pl.semaphore_signal(barrier, inc=1, device_id=(flip(me, bit),), device_id_type=MESH)
    pl.semaphore_wait(barrier, 4)
    return me


def gather_kernel(bounds, h_ref, wg_ref, wu_ref, z_ref, id_ref, x_a, x_b, x_c, own_sem, send_sem, recv_sem, side_send, side_recv):
    rows = x_a.shape[1] // 2
    bufs = (x_a, x_b, x_c)
    copies = []
    for f in range(3):
        lo, hi = bounds[f]
        copies.append(pltpu.make_async_copy(h_ref.at[:, pl.ds(lo, hi - lo)], bufs[f].at[0, pl.ds(0, rows)], own_sem.at[f]))
        copies[-1].start()
    me = meet_neighbours()

    def hop(f, src, bit):
        return pltpu.make_async_remote_copy(
            src_ref=bufs[f].at[src, pl.ds(0, rows)], dst_ref=bufs[f].at[src ^ bit, pl.ds(0, rows)],
            send_sem=send_sem.at[f, src ^ bit], recv_sem=recv_sem.at[f, src ^ bit],
            device_id=(flip(me, 2 * bit),), device_id_type=MESH)

    def side(f, src):
        return pltpu.make_async_remote_copy(
            src_ref=bufs[f].at[src, pl.ds(0, rows)], dst_ref=bufs[f].at[src, pl.ds(rows, rows)],
            send_sem=side_send.at[f, src], recv_sem=side_recv.at[f, src],
            device_id=(flip(me, 1),), device_id_type=MESH)

    def landed(f, slot):
        hop(f, 0, slot).wait_recv()

    def activate(pair):
        u_val = v_val = None
        for f in range(3):
            lo, hi = bounds[f]
            hi = min(hi, wg_ref.shape[0])
            x_val = bufs[f][pair, :, : hi - lo]
            u_part = jnp.dot(x_val, wg_ref[lo:hi, :], preferred_element_type=jnp.float32)
            v_part = jnp.dot(x_val, wu_ref[lo:hi, :], preferred_element_type=jnp.float32)
            u_val = u_part if u_val is None else u_val + u_part
            v_val = v_part if v_val is None else v_val + v_part
        z_ref[pair] = (jax.nn.silu(u_val) * v_val).astype(jnp.bfloat16)
        id_ref[pair] = bufs[2][pair, :, pl.ds(bounds[2][1] - bounds[2][0] - LANES, LANES)]

    for f in range(3):
        copies[f].wait()
        hop(f, 0, ORDERS[f][0]).start()
    for f in range(3):
        side(f, 0).start()
    for stage in (1, 2):
        for f in range(3):
            hop(f, 0, ORDERS[f][stage]).start()
    for f in range(3):
        side(f, 0).wait_recv()
    activate(0)
    for f in range(3):
        a, b, g = ORDERS[f]
        landed(f, a)
        hop(f, a, b).start()
        hop(f, a, g).start()
        side(f, a).start()
    for f in range(3):
        a, b, g = ORDERS[f]
        landed(f, b)
        hop(f, b, g).start()
        side(f, b).start()
    for f in range(3):
        a, b, g = ORDERS[f]
        landed(f, a ^ b)
        hop(f, a ^ b, g).start()
        side(f, a ^ b).start()
    for f in range(3):
        g = ORDERS[f][2]
        landed(f, g)
        side(f, g).start()
    for f in range(3):
        for slot in (1, 2, 4):
            side(f, slot).wait_recv()

    @pl.loop(0, 3)
    def _(i):
        activate(i * (i + 1) // 2 + 1)

    for f in range(3):
        a, b, g = ORDERS[f]
        landed(f, a ^ g)
        side(f, a ^ g).start()
        landed(f, b ^ g)
        side(f, b ^ g).start()
    for f in range(3):
        for slot in (3, 5, 6):
            side(f, slot).wait_recv()

    @pl.loop(0, 3)
    def _(i):
        activate(6 - i * (i + 1) // 2)

    for f in range(3):
        landed(f, 7)
        side(f, 7).start()
    for f in range(3):
        side(f, 7).wait_recv()
    activate(7)
    for f in range(3):
        for slot in range(8):
            side(f, slot).wait_send()
        for slot in range(1, 8):
            hop(f, 0, slot).wait_send()


def return_kernel(z_ref, wd_ref, rel_ref, gate_ref, x_ref, out_ref, pair_buf, side_buf, near_buf, turn_buf, turn_in, last_buf, last_in, side_send, side_recv, hop_send, hop_recv):
    rows = x_ref.shape[0]
    chunks = pair_buf.shape[0]
    me = meet_neighbours()

    def slot_of(f, place):
        a, b, g = ORDERS[f]
        return a * (place // 4) + b * (place // 2 % 2) + g * (place % 2)

    def remote(src, dst, send, recv, bit):
        return pltpu.make_async_remote_copy(src_ref=src, dst_ref=dst, send_sem=send, recv_sem=recv, device_id=(flip(me, bit),), device_id_type=MESH)

    def side(q):
        return remote(side_buf.at[q], pair_buf.at[q, 1], side_send.at[q], side_recv.at[q], 1)

    def hop_one(f, q):
        return remote(pair_buf.at[q, :, pl.ds(4 * rows, 4 * rows)], near_buf.at[q], hop_send.at[0, q], hop_recv.at[0, q], 2 * ORDERS[f][0])

    def hop_two(f, q):
        return remote(turn_buf.at[q], turn_in.at[q], hop_send.at[1, q], hop_recv.at[1, q], 2 * ORDERS[f][1])

    def hop_three(f, q):
        return remote(last_buf.at[q], last_in.at[q], hop_send.at[2, q], hop_recv.at[2, q], 2 * ORDERS[f][2])

    def project(f, q):
        w_val = wd_ref[:, pl.ds(pl.multiple_of(q * WIDTH, WIDTH), WIDTH)]
        for place in range(8):
            e_val = jnp.dot(z_ref[slot_of(f, place)], w_val, preferred_element_type=jnp.float32).astype(jnp.bfloat16)
            pair_buf[q, 0, place * rows:(place + 1) * rows, :] = e_val[:rows]
            side_buf[q, place * rows:(place + 1) * rows, :] = e_val[rows:]
        side(q).start()

    def send_far(f, q):
        side(q).wait_recv()
        hop_one(f, q).start()

    def choose(f, q, place, k, other):
        rel = rel_ref[slot_of(f, place)][:, k:k + 1]
        at = pl.ds(place * rows, rows)
        far = 2 * ORDERS[f][0]
        val = other
        if val is None:
            val = near_buf[q, 1, at, :].astype(jnp.float32)
        else:
            val = jnp.where(rel == far + 1, near_buf[q, 1, at, :].astype(jnp.float32), val)
        val = jnp.where(rel == far, near_buf[q, 0, at, :].astype(jnp.float32), val)
        val = jnp.where(rel == 1, pair_buf[q, 1, at, :].astype(jnp.float32), val)
        return jnp.where(rel == 0, pair_buf[q, 0, at, :].astype(jnp.float32), val)

    def turn(f, q):
        hop_one(f, q).wait_recv()
        for k in range(2):
            for half in range(2):
                turn_buf[q, k, half * rows:(half + 1) * rows, :] = choose(f, q, 2 + half, k, None).astype(jnp.bfloat16)
        hop_two(f, q).start()

    def last(f, q):
        hop_two(f, q).wait_recv()
        for k in range(2):
            other = turn_in[q, k, rows:2 * rows, :].astype(jnp.float32)
            last_buf[q, k] = choose(f, q, 1, k, other).astype(jnp.bfloat16)
        hop_three(f, q).start()

    def finish(f, q):
        hop_three(f, q).wait_recv()
        g_bit = 2 * ORDERS[f][2]
        y_val = None
        for k in range(2):
            rel = rel_ref[0][:, k:k + 1]
            other = jnp.where((rel // g_bit) % 2 == 1, last_in[q, k].astype(jnp.float32), turn_in[q, k, :rows, :].astype(jnp.float32))
            part = gate_ref[:, k:k + 1] * choose(f, q, 0, k, other)
            y_val = part if y_val is None else y_val + part
        at = pl.ds(pl.multiple_of(q * WIDTH, WIDTH), WIDTH)
        out_ref[:, at] = (x_ref[:, at].astype(jnp.float32) + y_val).astype(jnp.bfloat16)

    def sweep(step):
        @pl.loop(0, chunks // 3)
        def _(j):
            for f in range(3):
                step(f, 3 * j + f)
        for q in range(chunks // 3 * 3, chunks):
            step(q % 3, q)

    for f in range(3):
        project(f, f)

    @pl.loop(1, chunks // 3)
    def _(j):
        for f in range(3):
            project(f, 3 * j + f)
            send_far(f, 3 * j + f - 3)

    for q in range(chunks // 3 * 3, chunks):
        project(q % 3, q)
    for f in range(3):
        send_far(f, chunks // 3 * 3 - 3 + f)
    for q in range(chunks // 3 * 3, chunks):
        send_far(q % 3, q)
    sweep(turn)
    sweep(last)
    sweep(finish)

    def drain(f, q):
        side(q).wait_send()
        hop_one(f, q).wait_send()
        hop_two(f, q).wait_send()
        hop_three(f, q).wait_send()
    sweep(drain)


def gather_and_activate(h_two, expert_one, expert_two, w_gate, w_up):
    rows, d_model = h_two.shape
    d_ff = w_gate.shape[1]
    ids = jnp.pad(jnp.stack([expert_one, expert_two], axis=1).astype(jnp.bfloat16), ((0, 0), (0, LANES - 2)))
    h_ext = jnp.concatenate([h_two, ids], axis=1)
    tiles = (d_model + LANES) // LANES
    cuts = [LANES * ((tiles * f + 2) // 3) for f in range(4)]
    bounds = tuple((cuts[f], cuts[f + 1]) for f in range(3))
    vmem = pl.BlockSpec(memory_space=pltpu.VMEM)
    return pl.pallas_call(
        functools.partial(gather_kernel, bounds),
        name='gather_rows',
        out_shape=(jax.ShapeDtypeStruct((8, 2 * rows, d_ff), jnp.bfloat16), jax.ShapeDtypeStruct((8, 2 * rows, LANES), jnp.bfloat16)),
        in_specs=[pl.BlockSpec(memory_space=pl.ANY), vmem, vmem],
        out_specs=(vmem, vmem),
        scratch_shapes=[pltpu.VMEM((8, 2 * rows, hi - lo), jnp.bfloat16) for lo, hi in bounds] + [
            pltpu.SemaphoreType.DMA((3,)),
            pltpu.SemaphoreType.DMA((3, 8)), pltpu.SemaphoreType.DMA((3, 8)),
            pltpu.SemaphoreType.DMA((3, 8)), pltpu.SemaphoreType.DMA((3, 8))],
        compiler_params=pltpu.CompilerParams(collective_id=0, has_side_effects=True, vmem_limit_bytes=60 * 1024 * 1024),
    )(h_ext, w_gate, w_up)


def project_and_return(z_val, w_down, rel, gates, x_mid):
    rows, d_model = x_mid.shape
    chunks = d_model // WIDTH
    vmem = pl.BlockSpec(memory_space=pltpu.VMEM)
    return pl.pallas_call(
        return_kernel,
        name='return_rows',
        out_shape=jax.ShapeDtypeStruct((rows, d_model), jnp.bfloat16),
        in_specs=[vmem] * 5,
        out_specs=vmem,
        scratch_shapes=[
            pltpu.VMEM((chunks, 2, 8 * rows, WIDTH), jnp.bfloat16),
            pltpu.VMEM((chunks, 8 * rows, WIDTH), jnp.bfloat16),
            pltpu.VMEM((chunks, 2, 4 * rows, WIDTH), jnp.bfloat16),
            pltpu.VMEM((chunks, 2, 2 * rows, WIDTH), jnp.bfloat16),
            pltpu.VMEM((chunks, 2, 2 * rows, WIDTH), jnp.bfloat16),
            pltpu.VMEM((chunks, 2, rows, WIDTH), jnp.bfloat16),
            pltpu.VMEM((chunks, 2, rows, WIDTH), jnp.bfloat16),
            pltpu.SemaphoreType.DMA((chunks,)), pltpu.SemaphoreType.DMA((chunks,)),
            pltpu.SemaphoreType.DMA((3, chunks)), pltpu.SemaphoreType.DMA((3, chunks))],
        compiler_params=pltpu.CompilerParams(collective_id=1, has_side_effects=True, vmem_limit_bytes=63 * 1024 * 1024),
    )(z_val, w_down, rel, gates, x_mid)


def solution(mesh):
    def local_step(tokens, k_cache, v_cache, positions, expert_one, expert_two, eligible, ln1_gain, ln1_bias, w_query, b_query, w_key, b_key, w_value, b_value, w_out, b_out, ln2_gain, ln2_bias, w_router, w_gate, w_up, w_down):
        x_mid, key_new, value_new = attention_block(tokens, k_cache, v_cache, positions, ln1_gain, ln1_bias, w_query, b_query, w_key, b_key, w_value, b_value, w_out, b_out)
        h_two = layer_norm(x_mid.astype(jnp.float32), ln2_gain, ln2_bias).astype(jnp.bfloat16)
        gate_one, gate_two = router_gates(h_two, w_router, expert_one, expert_two, eligible)
        z_val, ids = gather_and_activate(h_two, expert_one, expert_two, w_gate[0], w_up[0])
        rel = ids[:, :h_two.shape[0]].astype(jnp.int32) ^ lax.axis_index('ep')
        gates = jnp.pad(jnp.stack([gate_one, gate_two], axis=1), ((0, 0), (0, LANES - 2)))
        tokens_out = project_and_return(z_val, w_down[0], rel, gates, x_mid)
        return tokens_out, key_new, value_new

    row_spec = P('ep', None)
    cache_spec = P('ep', None, None, None)
    vec_spec = P('ep')
    rep_one = P(None)
    rep_two = P(None, None)
    expert_spec = P('ep', None, None)
    in_specs = (row_spec, cache_spec, cache_spec, vec_spec, vec_spec, vec_spec, row_spec, rep_one, rep_one, rep_two, rep_one, rep_two, rep_one, rep_two, rep_one, rep_two, rep_one, rep_one, rep_one, rep_two, expert_spec, expert_spec, expert_spec)
    out_specs = (row_spec, expert_spec, expert_spec)
    return jax.shard_map(local_step, mesh=mesh, in_specs=in_specs, out_specs=out_specs, check_vma=False)
```

```python
import functools

import jax
import jax.numpy as jnp
from jax import lax
from jax.experimental import pallas as pl
from jax.experimental.pallas import tpu as pltpu
from jax.sharding import PartitionSpec as P

ROPE_BASE = 10000.0
LN_EPS = 1e-5

MESH = pl.DeviceIdType.MESH
ORDERS = ((1, 2, 4), (2, 4, 1), (4, 1, 2))
LANES = 128
WIDTH = 256
ALONG = (((1,), (1,)), ((), ()))


TILE = 256
GROUP = 8
DEPTH = 3
CHUNK = 64


def normed(x_f, gain_ref, bias_ref):
    mean_val = jnp.mean(x_f, axis=-1, keepdims=True)
    centered = x_f - mean_val
    var_val = jnp.mean(centered * centered, axis=-1, keepdims=True)
    return centered * lax.rsqrt(var_val + LN_EPS) * gain_ref[...].astype(jnp.float32) + bias_ref[...].astype(jnp.float32)


def qkv_kernel(q_steps, kv_steps, x_ref, gain_ref, bias_ref, wq_ref, wk_ref, wv_ref, bq_ref, bk_ref, bv_ref, cos_ref, sin_ref, q_ref, k_ref, v_ref, h_ref):
    step = pl.program_id(0)

    @pl.when(step == 0)
    def _():
        h_ref[...] = normed(x_ref[...].astype(jnp.float32), gain_ref, bias_ref).astype(jnp.bfloat16)

    def turned(w_ref, b_ref, o_ref):
        lin = jnp.dot(h_ref[...], w_ref[...], preferred_element_type=jnp.float32) + b_ref[...].astype(jnp.float32)
        for lo in range(0, TILE, LANES):
            head = lin[:, lo:lo + LANES]
            o_ref[:, lo:lo + LANES] = (head * cos_ref[...] + pltpu.roll(head, LANES // 2, 1) * sin_ref[...]).astype(jnp.bfloat16)

    @pl.when(step < q_steps)
    def _():
        turned(wq_ref, bq_ref, q_ref)

    @pl.when((step >= q_steps) & (step < q_steps + kv_steps))
    def _():
        turned(wk_ref, bk_ref, k_ref)

    @pl.when(step >= q_steps + kv_steps)
    def _():
        lin = jnp.dot(h_ref[...], wv_ref[...], preferred_element_type=jnp.float32)
        v_ref[...] = (lin + bv_ref[...].astype(jnp.float32)).astype(jnp.bfloat16)


def project_qkv(tokens, gain, bias, w_query, b_query, w_key, b_key, w_value, b_value, positions):
    rows, d_model = tokens.shape
    q_dim, kv_dim = w_query.shape[1], w_key.shape[1]
    q_steps, kv_steps = q_dim // TILE, kv_dim // TILE
    half_dim = LANES // 2
    inv_freq = ROPE_BASE ** (jnp.arange(half_dim, dtype=jnp.float32) * (-2.0 / LANES))
    angles = positions.astype(jnp.float32)[:, None] * inv_freq[None, :]
    cos_half, sin_half = jnp.cos(angles), jnp.sin(angles)
    cos_tab = jnp.concatenate([cos_half, cos_half], axis=-1)
    sin_tab = jnp.concatenate([-sin_half, sin_half], axis=-1)

    def at_q(i):
        return 0, jnp.minimum(i, q_steps - 1)

    def at_k(i):
        return 0, jnp.clip(i - q_steps, 0, kv_steps - 1)

    def at_v(i):
        return 0, jnp.clip(i - q_steps - kv_steps, 0, kv_steps - 1)

    def whole(shape):
        return pl.BlockSpec(shape, lambda i: (0, 0))

    return pl.pallas_call(
        functools.partial(qkv_kernel, q_steps, kv_steps),
        name='project_qkv',
        grid=(q_steps + 2 * kv_steps,),
        out_shape=(jax.ShapeDtypeStruct((rows, q_dim), jnp.bfloat16), jax.ShapeDtypeStruct((rows, kv_dim), jnp.bfloat16), jax.ShapeDtypeStruct((rows, kv_dim), jnp.bfloat16)),
        in_specs=[whole((rows, d_model)), whole((1, d_model)), whole((1, d_model)),
                  pl.BlockSpec((d_model, TILE), at_q), pl.BlockSpec((d_model, TILE), at_k), pl.BlockSpec((d_model, TILE), at_v),
                  pl.BlockSpec((1, TILE), at_q), pl.BlockSpec((1, TILE), at_k), pl.BlockSpec((1, TILE), at_v),
                  whole((rows, LANES)), whole((rows, LANES))],
        out_specs=(pl.BlockSpec((rows, TILE), at_q), pl.BlockSpec((rows, TILE), at_k), pl.BlockSpec((rows, TILE), at_v)),
        scratch_shapes=[pltpu.VMEM((rows, d_model), jnp.bfloat16)],
    )(tokens, gain[None], bias[None], w_query, w_key, w_value, b_query[None], b_key[None], b_value[None], cos_tab, sin_tab)


def attend_kernel(order_ref, pos_ref, span_ref, q_ref, kn_ref, vn_ref, k_hbm, v_hbm, o_ref, k_buf, v_buf, where_ref, sems):
    groups = order_ref.shape[0] // GROUP
    heads = q_ref.shape[1]
    kv_heads = k_hbm.shape[1] // (k_hbm.shape[1] // 4)
    spans = k_hbm.shape[1] // (CHUNK * kv_heads)
    scale = LANES ** -0.5
    col = lax.broadcasted_iota(jnp.int32, where_ref.shape, 1)
    row = lax.broadcasted_iota(jnp.int32, where_ref.shape, 0)
    where_ref[...] = jnp.where(col % kv_heads == row // (heads // kv_heads), col // kv_heads, 1 << 20)

    def copies(g, n):
        slot = lax.rem(g, DEPTH)
        size = n * CHUNK * kv_heads
        for j in range(GROUP):
            t = order_ref[g * GROUP + j]
            yield pltpu.make_async_copy(k_hbm.at[t, pl.ds(0, size)], k_buf.at[slot, j, pl.ds(0, size)], sems.at[slot, 0])
            yield pltpu.make_async_copy(v_hbm.at[t, pl.ds(0, size)], v_buf.at[slot, j, pl.ds(0, size)], sems.at[slot, 1])

    def each_span(g, body):
        for n in range(1, spans + 1):
            @pl.when(span_ref[g] == n)
            def _(n=n):
                body(n)

    def fetch(g):
        def body(n):
            for copy in copies(g, n):
                copy.start()
        each_span(g, body)

    for g in range(DEPTH - 1):
        fetch(jnp.int32(g))

    @pl.loop(0, groups)
    def _(g):
        @pl.when(g + DEPTH - 1 < groups)
        def _():
            fetch(g + DEPTH - 1)

        slot = lax.rem(g, DEPTH)

        def body(n):
            size = n * CHUNK * kv_heads
            for copy in copies(g, n):
                copy.wait()
            for j in range(GROUP):
                t = order_ref[g * GROUP + j]
                pos = pos_ref[g * GROUP + j]
                q_val = q_ref[t]
                s_val = lax.dot_general(q_val, k_buf[slot, j, :size], (((1,), (1,)), ((), ())), preferred_element_type=jnp.float32) * scale
                s_new = jnp.sum(q_val.astype(jnp.float32) * kn_ref[t].astype(jnp.float32), axis=1, keepdims=True) * scale
                s_val = jnp.where(where_ref[:, :size] < pos, s_val, -jnp.inf)
                top = jnp.maximum(jnp.max(s_val, axis=1, keepdims=True), s_new)
                e_val, e_new = jnp.exp(s_val - top), jnp.exp(s_new - top)
                inv = 1.0 / (jnp.sum(e_val, axis=1, keepdims=True) + e_new)
                p_val = (e_val * inv).astype(jnp.bfloat16)
                p_new = (e_new * inv).astype(jnp.bfloat16).astype(jnp.float32)
                a_val = jnp.dot(p_val, v_buf[slot, j, :size], preferred_element_type=jnp.float32)
                o_ref[t] = (a_val + p_new * vn_ref[t].astype(jnp.float32)).astype(jnp.bfloat16)
        each_span(g, body)


def attend(q_val, k_new, v_new, k_cache, v_cache, positions):
    rows, seq_len, kv_heads, head_dim = k_cache.shape
    heads = q_val.shape[1] // head_dim
    ids = jnp.arange(rows, dtype=jnp.int32)
    ahead = (positions[None, :] < positions[:, None]) | ((positions[None, :] == positions[:, None]) & (ids[None, :] < ids[:, None]))
    rank = jnp.sum(ahead.astype(jnp.int32), axis=1)
    hit = rank[None, :] == ids[:, None]
    order = jnp.sum(jnp.where(hit, ids[None, :], 0), axis=1)
    pos_sorted = jnp.sum(jnp.where(hit, positions[None, :], 0), axis=1)
    span = jnp.clip((pos_sorted[GROUP - 1::GROUP] + CHUNK - 1) // CHUNK, 1, seq_len // CHUNK)

    def spread(val):
        return jnp.repeat(val.reshape(rows, kv_heads, head_dim), heads // kv_heads, axis=1)

    vmem = pl.BlockSpec(memory_space=pltpu.VMEM)
    smem = pl.BlockSpec(memory_space=pltpu.SMEM)
    hbm = pl.BlockSpec(memory_space=pl.ANY)
    flat = (rows, seq_len * kv_heads, head_dim)
    return pl.pallas_call(
        attend_kernel,
        name='attend',
        out_shape=jax.ShapeDtypeStruct((rows, heads, head_dim), jnp.bfloat16),
        in_specs=[smem, smem, smem, vmem, vmem, vmem, hbm, hbm],
        out_specs=vmem,
        scratch_shapes=[
            pltpu.VMEM((DEPTH, GROUP) + flat[1:], jnp.bfloat16), pltpu.VMEM((DEPTH, GROUP) + flat[1:], jnp.bfloat16),
            pltpu.VMEM((heads, flat[1]), jnp.int32),
            pltpu.SemaphoreType.DMA((DEPTH, 2))],
        compiler_params=pltpu.CompilerParams(vmem_limit_bytes=48 * 1024 * 1024),
    )(order, pos_sorted, span, q_val.reshape(rows, heads, head_dim), spread(k_new), spread(v_new), k_cache.reshape(flat), v_cache.reshape(flat))


def mix_kernel(a_ref, w_ref, x_ref, b_ref, gain_ref, bias_ref, wr_ref, pick_ref, elig_ref, ids_ref, x_out, h_out, gate_out, x_all):
    step = pl.program_id(0)
    width = w_ref.shape[1]
    d_model = x_all.shape[1]
    acc = jnp.dot(a_ref[...], w_ref[...], preferred_element_type=jnp.float32)
    x_mid = (x_ref[...].astype(jnp.float32) + acc + b_ref[...].astype(jnp.float32)).astype(jnp.bfloat16)
    x_out[...] = x_mid
    x_all[:, pl.ds(pl.multiple_of(step * width, width), width)] = x_mid

    @pl.when(step == pl.num_programs(0) - 1)
    def _():
        h_two = normed(x_all[...].astype(jnp.float32), gain_ref, bias_ref).astype(jnp.bfloat16)
        h_out[:, :d_model] = h_two
        h_out[:, d_model:] = ids_ref[...]
        logits = lax.dot_general(h_two, wr_ref[...], (((1,), (1,)), ((), ())), preferred_element_type=jnp.float32)
        experts = lax.broadcasted_iota(jnp.int32, logits.shape, 1)
        hit_one = experts == pick_ref[:, 0:1]
        hit_two = experts == pick_ref[:, 1:2]
        keep_one = elig_ref[...] == 1

        def gate(keep, hit):
            val = jnp.where(keep, logits, -jnp.inf)
            e_val = jnp.exp(val - jnp.max(val, axis=1, keepdims=True))
            return jnp.sum(jnp.where(hit, e_val, 0.0), axis=1, keepdims=True) / jnp.sum(e_val, axis=1, keepdims=True)

        lane = lax.broadcasted_iota(jnp.int32, gate_out.shape, 1)
        gate_out[...] = jnp.where(lane == 0, gate(keep_one, hit_one), gate(keep_one & jnp.logical_not(hit_one), hit_two))


def mix(attn, w_out, tokens, b_out, gain, bias, w_router, expert_one, expert_two, eligible):
    rows, d_model = tokens.shape
    inner = w_out.shape[0]
    width = 2 * TILE
    picks = jnp.stack([expert_one, expert_two], axis=1)
    ids = jnp.pad(picks.astype(jnp.bfloat16), ((0, 0), (0, LANES - 2)))

    def whole(shape):
        return pl.BlockSpec(shape, lambda i: (0, 0))

    def tile(height):
        return pl.BlockSpec((height, width), lambda i: (0, i))

    return pl.pallas_call(
        mix_kernel,
        name='mix',
        grid=(d_model // width,),
        out_shape=(jax.ShapeDtypeStruct((rows, d_model), jnp.bfloat16), jax.ShapeDtypeStruct((rows, d_model + LANES), jnp.bfloat16), jax.ShapeDtypeStruct((rows, LANES), jnp.float32)),
        in_specs=[whole((rows, inner)), tile(inner), tile(rows), tile(1), whole((1, d_model)), whole((1, d_model)),
                  whole((w_router.shape[1], d_model)), whole((rows, 2)), whole(eligible.shape), whole((rows, LANES))],
        out_specs=(tile(rows), whole((rows, d_model + LANES)), whole((rows, LANES))),
        scratch_shapes=[pltpu.VMEM((rows, d_model), jnp.bfloat16)],
    )(attn, w_out, tokens, b_out[None], gain[None], bias[None], w_router.T, picks, eligible, ids)


def flip(me, bit):
    return me + bit - 2 * bit * ((me // bit) % 2)


def meet_neighbours():
    me = lax.axis_index('ep')
    barrier = pltpu.get_barrier_semaphore()
    for bit in (1, 2, 4, 8):
        pl.semaphore_signal(barrier, inc=1, device_id=(flip(me, bit),), device_id_type=MESH)
    pl.semaphore_wait(barrier, 4)
    return me


def gather_kernel(bounds, h_ref, wg_ref, wu_ref, z_ref, id_ref, x_a, x_b, x_c, own_sem, send_sem, recv_sem, side_send, side_recv):
    rows = x_a.shape[1] // 2
    bufs = (x_a, x_b, x_c)
    copies = []
    for f in range(3):
        lo, hi = bounds[f]
        copies.append(pltpu.make_async_copy(h_ref.at[:, pl.ds(lo, hi - lo)], bufs[f].at[0, pl.ds(0, rows)], own_sem.at[f]))
        copies[-1].start()
    me = meet_neighbours()

    def hop(f, src, bit):
        return pltpu.make_async_remote_copy(
            src_ref=bufs[f].at[src, pl.ds(0, rows)], dst_ref=bufs[f].at[src ^ bit, pl.ds(0, rows)],
            send_sem=send_sem.at[f, src ^ bit], recv_sem=recv_sem.at[f, src ^ bit],
            device_id=(flip(me, 2 * bit),), device_id_type=MESH)

    def side(f, src):
        return pltpu.make_async_remote_copy(
            src_ref=bufs[f].at[src, pl.ds(0, rows)], dst_ref=bufs[f].at[src, pl.ds(rows, rows)],
            send_sem=side_send.at[f, src], recv_sem=side_recv.at[f, src],
            device_id=(flip(me, 1),), device_id_type=MESH)

    def landed(f, slot):
        hop(f, 0, slot).wait_recv()

    def activate(pair):
        u_val = v_val = None
        for f in range(3):
            lo, hi = bounds[f]
            hi = min(hi, wg_ref.shape[1])
            x_val = bufs[f][pair, :, : hi - lo]
            u_part = lax.dot_general(x_val, wg_ref[:, lo:hi], ALONG, preferred_element_type=jnp.float32)
            v_part = lax.dot_general(x_val, wu_ref[:, lo:hi], ALONG, preferred_element_type=jnp.float32)
            u_val = u_part if u_val is None else u_val + u_part
            v_val = v_part if v_val is None else v_val + v_part
        z_ref[pair] = (jax.nn.silu(u_val) * v_val).astype(jnp.bfloat16)
        id_ref[pair] = bufs[2][pair, :, pl.ds(bounds[2][1] - bounds[2][0] - LANES, LANES)]

    for f in range(3):
        copies[f].wait()
        hop(f, 0, ORDERS[f][0]).start()
    for f in range(3):
        side(f, 0).start()
    for stage in (1, 2):
        for f in range(3):
            hop(f, 0, ORDERS[f][stage]).start()
    for f in range(3):
        side(f, 0).wait_recv()
    activate(0)
    for f in range(3):
        a, b, g = ORDERS[f]
        landed(f, a)
        hop(f, a, b).start()
        hop(f, a, g).start()
        side(f, a).start()
    for f in range(3):
        a, b, g = ORDERS[f]
        landed(f, b)
        hop(f, b, g).start()
        side(f, b).start()
    for f in range(3):
        a, b, g = ORDERS[f]
        landed(f, a ^ b)
        hop(f, a ^ b, g).start()
        side(f, a ^ b).start()
    for f in range(3):
        g = ORDERS[f][2]
        landed(f, g)
        side(f, g).start()
    for f in range(3):
        for slot in (1, 2, 4):
            side(f, slot).wait_recv()

    @pl.loop(0, 3)
    def _(i):
        activate(i * (i + 1) // 2 + 1)

    for f in range(3):
        a, b, g = ORDERS[f]
        landed(f, a ^ g)
        side(f, a ^ g).start()
        landed(f, b ^ g)
        side(f, b ^ g).start()
    for f in range(3):
        for slot in (3, 5, 6):
            side(f, slot).wait_recv()

    @pl.loop(0, 3)
    def _(i):
        activate(6 - i * (i + 1) // 2)

    for f in range(3):
        landed(f, 7)
        side(f, 7).start()
    for f in range(3):
        side(f, 7).wait_recv()
    activate(7)
    for f in range(3):
        for slot in range(8):
            side(f, slot).wait_send()
        for slot in range(1, 8):
            hop(f, 0, slot).wait_send()


def return_kernel(z_ref, wd_ref, rel_ref, gate_ref, x_ref, out_ref, pair_buf, side_buf, near_buf, turn_buf, turn_in, last_buf, last_in, side_send, side_recv, hop_send, hop_recv):
    rows = x_ref.shape[0]
    chunks = pair_buf.shape[0]
    me = meet_neighbours()

    def slot_of(f, place):
        a, b, g = ORDERS[f]
        return a * (place // 4) + b * (place // 2 % 2) + g * (place % 2)

    def remote(src, dst, send, recv, bit):
        return pltpu.make_async_remote_copy(src_ref=src, dst_ref=dst, send_sem=send, recv_sem=recv, device_id=(flip(me, bit),), device_id_type=MESH)

    def side(q):
        return remote(side_buf.at[q], pair_buf.at[q, 1], side_send.at[q], side_recv.at[q], 1)

    def hop_one(f, q):
        return remote(pair_buf.at[q, :, pl.ds(4 * rows, 4 * rows)], near_buf.at[q], hop_send.at[0, q], hop_recv.at[0, q], 2 * ORDERS[f][0])

    def hop_two(f, q):
        return remote(turn_buf.at[q], turn_in.at[q], hop_send.at[1, q], hop_recv.at[1, q], 2 * ORDERS[f][1])

    def hop_three(f, q):
        return remote(last_buf.at[q], last_in.at[q], hop_send.at[2, q], hop_recv.at[2, q], 2 * ORDERS[f][2])

    def project(f, q):
        w_val = wd_ref[:, pl.ds(pl.multiple_of(q * WIDTH, WIDTH), WIDTH)]
        for place in range(8):
            e_val = jnp.dot(z_ref[slot_of(f, place)], w_val, preferred_element_type=jnp.float32).astype(jnp.bfloat16)
            pair_buf[q, 0, place * rows:(place + 1) * rows, :] = e_val[:rows]
            side_buf[q, place * rows:(place + 1) * rows, :] = e_val[rows:]
        side(q).start()

    def send_far(f, q):
        side(q).wait_recv()
        hop_one(f, q).start()

    def choose(f, q, place, k, other):
        rel = rel_ref[slot_of(f, place)][:, k:k + 1]
        at = pl.ds(place * rows, rows)
        far = 2 * ORDERS[f][0]
        val = other
        if val is None:
            val = near_buf[q, 1, at, :].astype(jnp.float32)
        else:
            val = jnp.where(rel == far + 1, near_buf[q, 1, at, :].astype(jnp.float32), val)
        val = jnp.where(rel == far, near_buf[q, 0, at, :].astype(jnp.float32), val)
        val = jnp.where(rel == 1, pair_buf[q, 1, at, :].astype(jnp.float32), val)
        return jnp.where(rel == 0, pair_buf[q, 0, at, :].astype(jnp.float32), val)

    def turn(f, q):
        hop_one(f, q).wait_recv()
        for k in range(2):
            for half in range(2):
                turn_buf[q, k, half * rows:(half + 1) * rows, :] = choose(f, q, 2 + half, k, None).astype(jnp.bfloat16)
        hop_two(f, q).start()

    def last(f, q):
        hop_two(f, q).wait_recv()
        for k in range(2):
            other = turn_in[q, k, rows:2 * rows, :].astype(jnp.float32)
            last_buf[q, k] = choose(f, q, 1, k, other).astype(jnp.bfloat16)
        hop_three(f, q).start()

    def finish(f, q):
        hop_three(f, q).wait_recv()
        g_bit = 2 * ORDERS[f][2]
        y_val = None
        for k in range(2):
            rel = rel_ref[0][:, k:k + 1]
            other = jnp.where((rel // g_bit) % 2 == 1, last_in[q, k].astype(jnp.float32), turn_in[q, k, :rows, :].astype(jnp.float32))
            part = gate_ref[:, k:k + 1] * choose(f, q, 0, k, other)
            y_val = part if y_val is None else y_val + part
        at = pl.ds(pl.multiple_of(q * WIDTH, WIDTH), WIDTH)
        out_ref[:, at] = (x_ref[:, at].astype(jnp.float32) + y_val).astype(jnp.bfloat16)

    def sweep(step):
        @pl.loop(0, chunks // 3)
        def _(j):
            for f in range(3):
                step(f, 3 * j + f)
        for q in range(chunks // 3 * 3, chunks):
            step(q % 3, q)

    for f in range(3):
        project(f, f)

    @pl.loop(1, chunks // 3)
    def _(j):
        for f in range(3):
            project(f, 3 * j + f)
            send_far(f, 3 * j + f - 3)

    for q in range(chunks // 3 * 3, chunks):
        project(q % 3, q)
    for f in range(3):
        send_far(f, chunks // 3 * 3 - 3 + f)
    for q in range(chunks // 3 * 3, chunks):
        send_far(q % 3, q)
    sweep(turn)
    sweep(last)
    sweep(finish)

    def drain(f, q):
        side(q).wait_send()
        hop_one(f, q).wait_send()
        hop_two(f, q).wait_send()
        hop_three(f, q).wait_send()
    sweep(drain)


def gather_and_activate(h_ext, w_gate, w_up):
    rows, d_model = h_ext.shape[0], h_ext.shape[1] - LANES
    d_ff = w_gate.shape[0]
    tiles = (d_model + LANES) // LANES
    cuts = [LANES * ((tiles * f + 2) // 3) for f in range(4)]
    bounds = tuple((cuts[f], cuts[f + 1]) for f in range(3))
    vmem = pl.BlockSpec(memory_space=pltpu.VMEM)
    return pl.pallas_call(
        functools.partial(gather_kernel, bounds),
        name='gather_rows',
        out_shape=(jax.ShapeDtypeStruct((8, 2 * rows, d_ff), jnp.bfloat16), jax.ShapeDtypeStruct((8, 2 * rows, LANES), jnp.bfloat16)),
        in_specs=[pl.BlockSpec(memory_space=pl.ANY), vmem, vmem],
        out_specs=(vmem, vmem),
        scratch_shapes=[pltpu.VMEM((8, 2 * rows, hi - lo), jnp.bfloat16) for lo, hi in bounds] + [
            pltpu.SemaphoreType.DMA((3,)),
            pltpu.SemaphoreType.DMA((3, 8)), pltpu.SemaphoreType.DMA((3, 8)),
            pltpu.SemaphoreType.DMA((3, 8)), pltpu.SemaphoreType.DMA((3, 8))],
        compiler_params=pltpu.CompilerParams(collective_id=0, has_side_effects=True, vmem_limit_bytes=60 * 1024 * 1024),
    )(h_ext, w_gate, w_up)


def project_and_return(z_val, w_down, rel, gates, x_mid):
    rows, d_model = x_mid.shape
    chunks = d_model // WIDTH
    vmem = pl.BlockSpec(memory_space=pltpu.VMEM)
    return pl.pallas_call(
        return_kernel,
        name='return_rows',
        out_shape=jax.ShapeDtypeStruct((rows, d_model), jnp.bfloat16),
        in_specs=[vmem] * 5,
        out_specs=vmem,
        scratch_shapes=[
            pltpu.VMEM((chunks, 2, 8 * rows, WIDTH), jnp.bfloat16),
            pltpu.VMEM((chunks, 8 * rows, WIDTH), jnp.bfloat16),
            pltpu.VMEM((chunks, 2, 4 * rows, WIDTH), jnp.bfloat16),
            pltpu.VMEM((chunks, 2, 2 * rows, WIDTH), jnp.bfloat16),
            pltpu.VMEM((chunks, 2, 2 * rows, WIDTH), jnp.bfloat16),
            pltpu.VMEM((chunks, 2, rows, WIDTH), jnp.bfloat16),
            pltpu.VMEM((chunks, 2, rows, WIDTH), jnp.bfloat16),
            pltpu.SemaphoreType.DMA((chunks,)), pltpu.SemaphoreType.DMA((chunks,)),
            pltpu.SemaphoreType.DMA((3, chunks)), pltpu.SemaphoreType.DMA((3, chunks))],
        compiler_params=pltpu.CompilerParams(collective_id=1, has_side_effects=True, vmem_limit_bytes=63 * 1024 * 1024),
    )(z_val, w_down, rel, gates, x_mid)


def solution(mesh):
    def local_step(tokens, k_cache, v_cache, positions, expert_one, expert_two, eligible, ln1_gain, ln1_bias, w_query, b_query, w_key, b_key, w_value, b_value, w_out, b_out, ln2_gain, ln2_bias, w_router, w_gate, w_up, w_down):
        rows, seq_len, kv_heads, head_dim = k_cache.shape
        q_val, k_val, v_val = project_qkv(tokens, ln1_gain, ln1_bias, w_query, b_query, w_key, b_key, w_value, b_value, positions)
        attn = attend(q_val, k_val, v_val, k_cache, v_cache, positions).reshape(rows, -1)
        x_mid, h_ext, gates = mix(attn, w_out, tokens, b_out, ln2_gain, ln2_bias, w_router, expert_one, expert_two, eligible)
        z_val, ids = gather_and_activate(h_ext, w_gate[0].T, w_up[0].T)
        rel = ids[:, :rows].astype(jnp.int32) ^ lax.axis_index('ep')
        tokens_out = project_and_return(z_val, w_down[0], rel, gates, x_mid)
        key_new, value_new = k_val.reshape(rows, kv_heads, head_dim), v_val.reshape(rows, kv_heads, head_dim)
        return tokens_out, key_new, value_new

    row_spec = P('ep', None)
    cache_spec = P('ep', None, None, None)
    vec_spec = P('ep')
    rep_one = P(None)
    rep_two = P(None, None)
    expert_spec = P('ep', None, None)
    in_specs = (row_spec, cache_spec, cache_spec, vec_spec, vec_spec, vec_spec, row_spec, rep_one, rep_one, rep_two, rep_one, rep_two, rep_one, rep_two, rep_one, rep_two, rep_one, rep_one, rep_one, rep_two, expert_spec, expert_spec, expert_spec)
    out_specs = (row_spec, expert_spec, expert_spec)
    return jax.shard_map(local_step, mesh=mesh, in_specs=in_specs, out_specs=out_specs, check_vma=False)
```

```python
import functools

import jax
import jax.numpy as jnp
from jax import lax
from jax.experimental import pallas as pl
from jax.experimental.pallas import tpu as pltpu
from jax.sharding import PartitionSpec as P

ROPE_BASE = 10000.0
LN_EPS = 1e-5

MESH = pl.DeviceIdType.MESH
ORDERS = ((1, 2, 4), (2, 4, 1), (4, 1, 2))
LANES = 128
WIDTH = 256
ALONG = (((1,), (1,)), ((), ()))


TILE = 512
HALF = 2048
GROUP = 8
PART = 4
DEPTH = 3
CHUNK = 64


def normed(x_f, gain, bias):
    mean_val = jnp.mean(x_f, axis=-1, keepdims=True)
    centered = x_f - mean_val
    var_val = jnp.mean(centered * centered, axis=-1, keepdims=True)
    return centered * lax.rsqrt(var_val + LN_EPS) * gain + bias


def attend_kernel(kv_heads, order_ref, pos_ref, span_ref, x_ref, par_ref, rot_ref, meta_ref, wr_ref, wq_hbm, wk_hbm, wv_hbm, wo_hbm, k_hbm, v_hbm,
                  k_out, v_out, x_out, h_out, gate_out, w_buf, k_buf, v_buf, q_all, kn_all, vn_all, o_all, h_buf, where_ref, w_sem, o_sem, kv_sem):
    rows, d_model = x_ref.shape
    heads = q_all.shape[1]
    share = heads // kv_heads
    groups = rows // GROUP
    spans = k_hbm.shape[1] // (CHUNK * kv_heads)
    q_tiles = wq_hbm.shape[1] // TILE
    scale = LANES ** -0.5

    def weights(w_hbm, tile, slot):
        return [pltpu.make_async_copy(w_hbm.at[pl.ds(half * HALF, HALF), pl.ds(tile * TILE, TILE)], w_buf.at[slot + half], w_sem.at[slot + half]) for half in range(2)]

    loads = [weights(wq_hbm, i, 2 * i) for i in range(q_tiles)] + [weights(wk_hbm, 0, 2 * q_tiles), weights(wv_hbm, 0, 2 * q_tiles + 2)]
    for pair in loads:
        for copy in pair:
            copy.start()

    def copies(g, n):
        slot = lax.rem(g, DEPTH)
        size = n * CHUNK * kv_heads
        for j in range(GROUP):
            t = order_ref[g * GROUP + j]
            yield pltpu.make_async_copy(k_hbm.at[t, pl.ds(0, size)], k_buf.at[slot, j, pl.ds(0, size)], kv_sem.at[slot, 0])
            yield pltpu.make_async_copy(v_hbm.at[t, pl.ds(0, size)], v_buf.at[slot, j, pl.ds(0, size)], kv_sem.at[slot, 1])

    def each_span(g, body):
        for n in range(1, spans + 1):
            @pl.when(span_ref[g] == n)
            def _(n=n):
                body(n)

    def fetch(g):
        def body(n):
            for copy in copies(g, n):
                copy.start()
        each_span(g, body)

    for g in range(DEPTH - 1):
        fetch(jnp.int32(g))

    col = lax.broadcasted_iota(jnp.int32, where_ref.shape, 1)
    row = lax.broadcasted_iota(jnp.int32, where_ref.shape, 0)
    where_ref[...] = jnp.where(col % kv_heads == (row // share) % kv_heads, col // kv_heads, 1 << 20)
    h_buf[...] = normed(x_ref[...].astype(jnp.float32), par_ref[0:1, :], par_ref[1:2, :]).astype(jnp.bfloat16)

    def product(index, bias_at):
        slot = 2 * index
        for copy in loads[index]:
            copy.wait()
        lin = jnp.dot(h_buf[:, :HALF], w_buf[slot], preferred_element_type=jnp.float32) + jnp.dot(h_buf[:, HALF:], w_buf[slot + 1], preferred_element_type=jnp.float32)
        return lin + par_ref[5:6, bias_at:bias_at + TILE]

    def turned(head):
        return (head * rot_ref[0] + pltpu.roll(head, LANES // 2, 1) * rot_ref[1]).astype(jnp.bfloat16)

    for i in range(q_tiles):
        lin = product(i, i * TILE)
        for n in range(TILE // LANES):
            q_all[:, i * (TILE // LANES) + n, :] = turned(lin[:, n * LANES:(n + 1) * LANES]).astype(jnp.float32)
    lin = product(q_tiles, q_tiles * TILE)
    for n in range(kv_heads):
        val = turned(lin[:, n * LANES:(n + 1) * LANES])
        k_out[:, n * LANES:(n + 1) * LANES] = val
        for m in range(share):
            kn_all[:, n * share + m, :] = val.astype(jnp.float32)
    lin = product(q_tiles + 1, (q_tiles + 1) * TILE)
    for n in range(kv_heads):
        val = lin[:, n * LANES:(n + 1) * LANES].astype(jnp.bfloat16)
        v_out[:, n * LANES:(n + 1) * LANES] = val
        for m in range(share):
            vn_all[:, n * share + m, :] = val.astype(jnp.float32)

    def out_weights(tile):
        return pltpu.make_async_copy(wo_hbm.at[:, pl.ds(pl.multiple_of(tile * TILE, TILE), TILE)], w_buf.at[tile], o_sem.at[tile])

    for tile in range(d_model // TILE):
        out_weights(tile).start()

    block = lax.broadcasted_iota(jnp.int32, (PART * heads, 1), 0) // heads

    @pl.loop(0, groups)
    def _(g):
        @pl.when(g + DEPTH - 1 < groups)
        def _():
            fetch(g + DEPTH - 1)

        slot = lax.rem(g, DEPTH)

        def body(n):
            size = n * CHUNK * kv_heads
            for copy in copies(g, n):
                copy.wait()
            for lo in range(0, GROUP, PART):
                toks = [order_ref[g * GROUP + lo + j] for j in range(PART)]
                q_rows = [q_all[t] for t in toks]
                s_val = jnp.concatenate([lax.dot_general(q_rows[j].astype(jnp.bfloat16), k_buf[slot, lo + j, :size], ALONG, preferred_element_type=jnp.float32) for j in range(PART)], axis=0) * scale
                q_val = jnp.concatenate(q_rows, axis=0)
                kn_val = jnp.concatenate([kn_all[t] for t in toks], axis=0)
                vn_val = jnp.concatenate([vn_all[t] for t in toks], axis=0)
                s_new = jnp.sum(q_val * kn_val, axis=1, keepdims=True) * scale
                pos = jnp.zeros((PART * heads, 1), jnp.int32)
                for j in range(PART):
                    pos = jnp.where(block == j, pos_ref[g * GROUP + lo + j], pos)
                s_val = jnp.where(where_ref[:, :size] < pos, s_val, -jnp.inf)
                top = jnp.maximum(jnp.max(s_val, axis=1, keepdims=True), s_new)
                e_val, e_new = jnp.exp(s_val - top), jnp.exp(s_new - top)
                inv = 1.0 / (jnp.sum(e_val, axis=1, keepdims=True) + e_new)
                p_val = (e_val * inv).astype(jnp.bfloat16)
                p_new = (e_new * inv).astype(jnp.bfloat16).astype(jnp.float32)
                a_val = jnp.concatenate([jnp.dot(p_val[j * heads:(j + 1) * heads], v_buf[slot, lo + j, :size], preferred_element_type=jnp.float32) for j in range(PART)], axis=0)
                a_val = (a_val + p_new * vn_val).astype(jnp.bfloat16).astype(jnp.float32)
                for j in range(PART):
                    o_all[toks[j]] = a_val[j * heads:(j + 1) * heads]
        each_span(g, body)

    for n in range(heads):
        h_buf[:, n * LANES:(n + 1) * LANES] = o_all[:, n, :].astype(jnp.bfloat16)

    @pl.loop(0, d_model // TILE)
    def _(tile):
        out_weights(tile).wait()
        at = pl.ds(pl.multiple_of(tile * TILE, TILE), TILE)
        acc = jnp.dot(h_buf[:, :heads * LANES], w_buf[tile], preferred_element_type=jnp.float32)
        x_out[:, at] = (x_ref[:, at].astype(jnp.float32) + acc + par_ref[4:5, at]).astype(jnp.bfloat16)

    h_two = normed(x_out[...].astype(jnp.float32), par_ref[2:3, :], par_ref[3:4, :]).astype(jnp.bfloat16)
    h_out[:, :d_model] = h_two
    logits = lax.dot_general(h_two, wr_ref[...], ALONG, preferred_element_type=jnp.float32)
    experts = logits.shape[1]
    expert_ids = lax.broadcasted_iota(jnp.int32, logits.shape, 1)
    pick_one, pick_two = meta_ref[:, experts:experts + 1], meta_ref[:, experts + 1:experts + 2]
    hit_one, hit_two = expert_ids == pick_one, expert_ids == pick_two
    keep_one = meta_ref[:, :experts] == 1

    def gate(keep, hit):
        val = jnp.where(keep, logits, -jnp.inf)
        e_val = jnp.exp(val - jnp.max(val, axis=1, keepdims=True))
        return jnp.sum(jnp.where(hit, e_val, 0.0), axis=1, keepdims=True) / jnp.sum(e_val, axis=1, keepdims=True)

    lane = lax.broadcasted_iota(jnp.int32, gate_out.shape, 1)
    gate_out[...] = jnp.where(lane == 0, gate(keep_one, hit_one), gate(keep_one & jnp.logical_not(hit_one), hit_two))
    ids = jnp.where(lane == 0, pick_one, jnp.where(lane == 1, pick_two, 0))
    h_out[:, d_model:] = ids.astype(jnp.float32).astype(jnp.bfloat16)


def attention_layer(tokens, k_cache, v_cache, positions, expert_one, expert_two, eligible, ln1_gain, ln1_bias, w_query, b_query, w_key, b_key, w_value, b_value, w_out, b_out, ln2_gain, ln2_bias, w_router):
    rows, seq_len, kv_heads, head_dim = k_cache.shape
    d_model = tokens.shape[1]
    heads = w_query.shape[1] // head_dim
    kv_dim = kv_heads * head_dim
    ids = jnp.arange(rows, dtype=jnp.int32)
    ahead = (positions[None, :] < positions[:, None]) | ((positions[None, :] == positions[:, None]) & (ids[None, :] < ids[:, None]))
    rank = jnp.sum(ahead.astype(jnp.int32), axis=1)
    hit = rank[None, :] == ids[:, None]
    order = jnp.sum(jnp.where(hit, ids[None, :], 0), axis=1)
    pos_sorted = jnp.sum(jnp.where(hit, positions[None, :], 0), axis=1)
    span = jnp.clip((pos_sorted[GROUP - 1::GROUP] + CHUNK - 1) // CHUNK, 1, seq_len // CHUNK)
    half_dim = head_dim // 2
    inv_freq = ROPE_BASE ** (jnp.arange(half_dim, dtype=jnp.float32) * (-2.0 / head_dim))
    angles = positions.astype(jnp.float32)[:, None] * jnp.concatenate([inv_freq, inv_freq])[None, :]
    sign = jnp.where(jnp.arange(head_dim) < half_dim, -1.0, 1.0).astype(jnp.float32)
    rot = jnp.stack([jnp.cos(angles), jnp.sin(angles) * sign[None, :]])
    biases = jnp.concatenate([b_query, b_key, b_value, jnp.zeros((d_model - heads * head_dim - 2 * kv_dim,), jnp.bfloat16)])
    par = jnp.stack([ln1_gain, ln1_bias, ln2_gain, ln2_bias, b_out, biases, biases, biases]).astype(jnp.float32)
    meta = jnp.concatenate([eligible, expert_one[:, None], expert_two[:, None], jnp.zeros((rows, LANES - 2 - eligible.shape[1]), jnp.int32)], axis=1)
    vmem = pl.BlockSpec(memory_space=pltpu.VMEM)
    smem = pl.BlockSpec(memory_space=pltpu.SMEM)
    hbm = pl.BlockSpec(memory_space=pl.ANY)
    flat = (rows, seq_len * kv_heads, head_dim)
    spread = pltpu.VMEM((rows, heads, head_dim), jnp.float32)
    return pl.pallas_call(
        functools.partial(attend_kernel, kv_heads),
        name='attention_layer',
        out_shape=(jax.ShapeDtypeStruct((rows, kv_dim), jnp.bfloat16), jax.ShapeDtypeStruct((rows, kv_dim), jnp.bfloat16),
                   jax.ShapeDtypeStruct((rows, d_model), jnp.bfloat16), jax.ShapeDtypeStruct((rows, d_model + LANES), jnp.bfloat16),
                   jax.ShapeDtypeStruct((rows, LANES), jnp.float32)),
        in_specs=[smem, smem, smem, vmem, vmem, vmem, vmem, vmem, hbm, hbm, hbm, hbm, hbm, hbm],
        out_specs=(vmem,) * 5,
        scratch_shapes=[
            pltpu.VMEM((2 * (heads * head_dim + 2 * kv_dim) // TILE, HALF, TILE), jnp.bfloat16),
            pltpu.VMEM((DEPTH, GROUP) + flat[1:], jnp.bfloat16), pltpu.VMEM((DEPTH, GROUP) + flat[1:], jnp.bfloat16),
            spread, spread, spread, spread,
            pltpu.VMEM((rows, d_model), jnp.bfloat16),
            pltpu.VMEM((PART * heads, flat[1]), jnp.int32),
            pltpu.SemaphoreType.DMA((2 * (heads * head_dim + 2 * kv_dim) // TILE,)),
            pltpu.SemaphoreType.DMA((d_model // TILE,)),
            pltpu.SemaphoreType.DMA((DEPTH, 2))],
        compiler_params=pltpu.CompilerParams(vmem_limit_bytes=62 * 1024 * 1024),
    )(order, pos_sorted, span, tokens, par, rot, meta, w_router.T, w_query, w_key, w_value, w_out, k_cache.reshape(flat), v_cache.reshape(flat))


def flip(me, bit):
    return me + bit - 2 * bit * ((me // bit) % 2)


def meet_neighbours():
    me = lax.axis_index('ep')
    barrier = pltpu.get_barrier_semaphore()
    for bit in (1, 2, 4, 8):
        pl.semaphore_signal(barrier, inc=1, device_id=(flip(me, bit),), device_id_type=MESH)
    pl.semaphore_wait(barrier, 4)
    return me


def gather_kernel(bounds, h_ref, wg_ref, wu_ref, z_ref, id_ref, x_a, x_b, x_c, own_sem, send_sem, recv_sem, side_send, side_recv):
    rows = x_a.shape[1] // 2
    bufs = (x_a, x_b, x_c)
    copies = []
    for f in range(3):
        lo, hi = bounds[f]
        copies.append(pltpu.make_async_copy(h_ref.at[:, pl.ds(lo, hi - lo)], bufs[f].at[0, pl.ds(0, rows)], own_sem.at[f]))
        copies[-1].start()
    me = meet_neighbours()

    def hop(f, src, bit):
        return pltpu.make_async_remote_copy(
            src_ref=bufs[f].at[src, pl.ds(0, rows)], dst_ref=bufs[f].at[src ^ bit, pl.ds(0, rows)],
            send_sem=send_sem.at[f, src ^ bit], recv_sem=recv_sem.at[f, src ^ bit],
            device_id=(flip(me, 2 * bit),), device_id_type=MESH)

    def side(f, src):
        return pltpu.make_async_remote_copy(
            src_ref=bufs[f].at[src, pl.ds(0, rows)], dst_ref=bufs[f].at[src, pl.ds(rows, rows)],
            send_sem=side_send.at[f, src], recv_sem=side_recv.at[f, src],
            device_id=(flip(me, 1),), device_id_type=MESH)

    def landed(f, slot):
        hop(f, 0, slot).wait_recv()

    def activate(pair):
        u_val = v_val = None
        for f in range(3):
            lo, hi = bounds[f]
            hi = min(hi, wg_ref.shape[1])
            x_val = bufs[f][pair, :, : hi - lo]
            u_part = lax.dot_general(x_val, wg_ref[:, lo:hi], ALONG, preferred_element_type=jnp.float32)
            v_part = lax.dot_general(x_val, wu_ref[:, lo:hi], ALONG, preferred_element_type=jnp.float32)
            u_val = u_part if u_val is None else u_val + u_part
            v_val = v_part if v_val is None else v_val + v_part
        z_ref[pair] = (jax.nn.silu(u_val) * v_val).astype(jnp.bfloat16)
        id_ref[pair] = bufs[2][pair, :, pl.ds(bounds[2][1] - bounds[2][0] - LANES, LANES)]

    for f in range(3):
        copies[f].wait()
        hop(f, 0, ORDERS[f][0]).start()
    for f in range(3):
        side(f, 0).start()
    for stage in (1, 2):
        for f in range(3):
            hop(f, 0, ORDERS[f][stage]).start()
    for f in range(3):
        side(f, 0).wait_recv()
    activate(0)
    for f in range(3):
        a, b, g = ORDERS[f]
        landed(f, a)
        hop(f, a, b).start()
        hop(f, a, g).start()
        side(f, a).start()
    for f in range(3):
        a, b, g = ORDERS[f]
        landed(f, b)
        hop(f, b, g).start()
        side(f, b).start()
    for f in range(3):
        a, b, g = ORDERS[f]
        landed(f, a ^ b)
        hop(f, a ^ b, g).start()
        side(f, a ^ b).start()
    for f in range(3):
        g = ORDERS[f][2]
        landed(f, g)
        side(f, g).start()
    for f in range(3):
        for slot in (1, 2, 4):
            side(f, slot).wait_recv()

    @pl.loop(0, 3)
    def _(i):
        activate(i * (i + 1) // 2 + 1)

    for f in range(3):
        a, b, g = ORDERS[f]
        landed(f, a ^ g)
        side(f, a ^ g).start()
        landed(f, b ^ g)
        side(f, b ^ g).start()
    for f in range(3):
        for slot in (3, 5, 6):
            side(f, slot).wait_recv()

    @pl.loop(0, 3)
    def _(i):
        activate(6 - i * (i + 1) // 2)

    for f in range(3):
        landed(f, 7)
        side(f, 7).start()
    for f in range(3):
        side(f, 7).wait_recv()
    activate(7)
    for f in range(3):
        for slot in range(8):
            side(f, slot).wait_send()
        for slot in range(1, 8):
            hop(f, 0, slot).wait_send()


def return_kernel(z_ref, wd_ref, rel_ref, gate_ref, x_ref, out_ref, pair_buf, side_buf, near_buf, turn_buf, turn_in, last_buf, last_in, side_send, side_recv, hop_send, hop_recv):
    rows = x_ref.shape[0]
    chunks = pair_buf.shape[0]
    me = meet_neighbours()

    def slot_of(f, place):
        a, b, g = ORDERS[f]
        return a * (place // 4) + b * (place // 2 % 2) + g * (place % 2)

    def remote(src, dst, send, recv, bit):
        return pltpu.make_async_remote_copy(src_ref=src, dst_ref=dst, send_sem=send, recv_sem=recv, device_id=(flip(me, bit),), device_id_type=MESH)

    def side(q):
        return remote(side_buf.at[q], pair_buf.at[q, 1], side_send.at[q], side_recv.at[q], 1)

    def hop_one(f, q):
        return remote(pair_buf.at[q, :, pl.ds(4 * rows, 4 * rows)], near_buf.at[q], hop_send.at[0, q], hop_recv.at[0, q], 2 * ORDERS[f][0])

    def hop_two(f, q):
        return remote(turn_buf.at[q], turn_in.at[q], hop_send.at[1, q], hop_recv.at[1, q], 2 * ORDERS[f][1])

    def hop_three(f, q):
        return remote(last_buf.at[q], last_in.at[q], hop_send.at[2, q], hop_recv.at[2, q], 2 * ORDERS[f][2])

    def project(f, q):
        w_val = wd_ref[:, pl.ds(pl.multiple_of(q * WIDTH, WIDTH), WIDTH)]
        for place in range(8):
            e_val = jnp.dot(z_ref[slot_of(f, place)], w_val, preferred_element_type=jnp.float32).astype(jnp.bfloat16)
            pair_buf[q, 0, place * rows:(place + 1) * rows, :] = e_val[:rows]
            side_buf[q, place * rows:(place + 1) * rows, :] = e_val[rows:]
        side(q).start()

    def send_far(f, q):
        side(q).wait_recv()
        hop_one(f, q).start()

    def choose(f, q, place, k, other):
        rel = rel_ref[slot_of(f, place)][:, k:k + 1]
        at = pl.ds(place * rows, rows)
        far = 2 * ORDERS[f][0]
        val = other
        if val is None:
            val = near_buf[q, 1, at, :].astype(jnp.float32)
        else:
            val = jnp.where(rel == far + 1, near_buf[q, 1, at, :].astype(jnp.float32), val)
        val = jnp.where(rel == far, near_buf[q, 0, at, :].astype(jnp.float32), val)
        val = jnp.where(rel == 1, pair_buf[q, 1, at, :].astype(jnp.float32), val)
        return jnp.where(rel == 0, pair_buf[q, 0, at, :].astype(jnp.float32), val)

    def turn(f, q):
        hop_one(f, q).wait_recv()
        for k in range(2):
            for half in range(2):
                turn_buf[q, k, half * rows:(half + 1) * rows, :] = choose(f, q, 2 + half, k, None).astype(jnp.bfloat16)
        hop_two(f, q).start()

    def last(f, q):
        hop_two(f, q).wait_recv()
        for k in range(2):
            other = turn_in[q, k, rows:2 * rows, :].astype(jnp.float32)
            last_buf[q, k] = choose(f, q, 1, k, other).astype(jnp.bfloat16)
        hop_three(f, q).start()

    def finish(f, q):
        hop_three(f, q).wait_recv()
        g_bit = 2 * ORDERS[f][2]
        y_val = None
        for k in range(2):
            rel = rel_ref[0][:, k:k + 1]
            other = jnp.where((rel // g_bit) % 2 == 1, last_in[q, k].astype(jnp.float32), turn_in[q, k, :rows, :].astype(jnp.float32))
            part = gate_ref[:, k:k + 1] * choose(f, q, 0, k, other)
            y_val = part if y_val is None else y_val + part
        at = pl.ds(pl.multiple_of(q * WIDTH, WIDTH), WIDTH)
        out_ref[:, at] = (x_ref[:, at].astype(jnp.float32) + y_val).astype(jnp.bfloat16)

    def sweep(step):
        @pl.loop(0, chunks // 3)
        def _(j):
            for f in range(3):
                step(f, 3 * j + f)
        for q in range(chunks // 3 * 3, chunks):
            step(q % 3, q)

    for f in range(3):
        project(f, f)

    @pl.loop(1, chunks // 3)
    def _(j):
        for f in range(3):
            project(f, 3 * j + f)
            send_far(f, 3 * j + f - 3)

    for q in range(chunks // 3 * 3, chunks):
        project(q % 3, q)
    for f in range(3):
        send_far(f, chunks // 3 * 3 - 3 + f)
    for q in range(chunks // 3 * 3, chunks):
        send_far(q % 3, q)
    sweep(turn)
    sweep(last)
    sweep(finish)

    def drain(f, q):
        side(q).wait_send()
        hop_one(f, q).wait_send()
        hop_two(f, q).wait_send()
        hop_three(f, q).wait_send()
    sweep(drain)


def gather_and_activate(h_ext, w_gate, w_up):
    rows, d_model = h_ext.shape[0], h_ext.shape[1] - LANES
    d_ff = w_gate.shape[0]
    tiles = (d_model + LANES) // LANES
    cuts = [LANES * ((tiles * f + 2) // 3) for f in range(4)]
    bounds = tuple((cuts[f], cuts[f + 1]) for f in range(3))
    vmem = pl.BlockSpec(memory_space=pltpu.VMEM)
    return pl.pallas_call(
        functools.partial(gather_kernel, bounds),
        name='gather_rows',
        out_shape=(jax.ShapeDtypeStruct((8, 2 * rows, d_ff), jnp.bfloat16), jax.ShapeDtypeStruct((8, 2 * rows, LANES), jnp.bfloat16)),
        in_specs=[pl.BlockSpec(memory_space=pl.ANY), vmem, vmem],
        out_specs=(vmem, vmem),
        scratch_shapes=[pltpu.VMEM((8, 2 * rows, hi - lo), jnp.bfloat16) for lo, hi in bounds] + [
            pltpu.SemaphoreType.DMA((3,)),
            pltpu.SemaphoreType.DMA((3, 8)), pltpu.SemaphoreType.DMA((3, 8)),
            pltpu.SemaphoreType.DMA((3, 8)), pltpu.SemaphoreType.DMA((3, 8))],
        compiler_params=pltpu.CompilerParams(collective_id=0, has_side_effects=True, vmem_limit_bytes=60 * 1024 * 1024),
    )(h_ext, w_gate, w_up)


def project_and_return(z_val, w_down, rel, gates, x_mid):
    rows, d_model = x_mid.shape
    chunks = d_model // WIDTH
    vmem = pl.BlockSpec(memory_space=pltpu.VMEM)
    return pl.pallas_call(
        return_kernel,
        name='return_rows',
        out_shape=jax.ShapeDtypeStruct((rows, d_model), jnp.bfloat16),
        in_specs=[vmem] * 5,
        out_specs=vmem,
        scratch_shapes=[
            pltpu.VMEM((chunks, 2, 8 * rows, WIDTH), jnp.bfloat16),
            pltpu.VMEM((chunks, 8 * rows, WIDTH), jnp.bfloat16),
            pltpu.VMEM((chunks, 2, 4 * rows, WIDTH), jnp.bfloat16),
            pltpu.VMEM((chunks, 2, 2 * rows, WIDTH), jnp.bfloat16),
            pltpu.VMEM((chunks, 2, 2 * rows, WIDTH), jnp.bfloat16),
            pltpu.VMEM((chunks, 2, rows, WIDTH), jnp.bfloat16),
            pltpu.VMEM((chunks, 2, rows, WIDTH), jnp.bfloat16),
            pltpu.SemaphoreType.DMA((chunks,)), pltpu.SemaphoreType.DMA((chunks,)),
            pltpu.SemaphoreType.DMA((3, chunks)), pltpu.SemaphoreType.DMA((3, chunks))],
        compiler_params=pltpu.CompilerParams(collective_id=1, has_side_effects=True, vmem_limit_bytes=63 * 1024 * 1024),
    )(z_val, w_down, rel, gates, x_mid)


def solution(mesh):
    def local_step(tokens, k_cache, v_cache, positions, expert_one, expert_two, eligible, ln1_gain, ln1_bias, w_query, b_query, w_key, b_key, w_value, b_value, w_out, b_out, ln2_gain, ln2_bias, w_router, w_gate, w_up, w_down):
        rows, seq_len, kv_heads, head_dim = k_cache.shape
        k_val, v_val, x_mid, h_ext, gates = attention_layer(tokens, k_cache, v_cache, positions, expert_one, expert_two, eligible, ln1_gain, ln1_bias, w_query, b_query, w_key, b_key, w_value, b_value, w_out, b_out, ln2_gain, ln2_bias, w_router)
        z_val, ids = gather_and_activate(h_ext, w_gate[0].T, w_up[0].T)
        rel = ids[:, :rows].astype(jnp.int32) ^ lax.axis_index('ep')
        tokens_out = project_and_return(z_val, w_down[0], rel, gates, x_mid)
        key_new, value_new = k_val.reshape(rows, kv_heads, head_dim), v_val.reshape(rows, kv_heads, head_dim)
        return tokens_out, key_new, value_new

    row_spec = P('ep', None)
    cache_spec = P('ep', None, None, None)
    vec_spec = P('ep')
    rep_one = P(None)
    rep_two = P(None, None)
    expert_spec = P('ep', None, None)
    in_specs = (row_spec, cache_spec, cache_spec, vec_spec, vec_spec, vec_spec, row_spec, rep_one, rep_one, rep_two, rep_one, rep_two, rep_one, rep_two, rep_one, rep_two, rep_one, rep_one, rep_one, rep_two, expert_spec, expert_spec, expert_spec)
    out_specs = (row_spec, expert_spec, expert_spec)
    return jax.shard_map(local_step, mesh=mesh, in_specs=in_specs, out_specs=out_specs, check_vma=False)
```

```python
import functools

import jax
import jax.numpy as jnp
from jax import lax
from jax.experimental import pallas as pl
from jax.experimental.pallas import tpu as pltpu
from jax.sharding import PartitionSpec as P

ROPE_BASE = 10000.0
LN_EPS = 1e-5

MESH = pl.DeviceIdType.MESH
ORDERS = ((1, 2, 4), (2, 4, 1), (4, 1, 2))
LANES = 128
WIDTH = 256
ALONG = (((1,), (1,)), ((), ()))


TILE = 512
HALF = 2048
GROUP = 8
PART = 4
DEPTH = 3
CHUNK = 64


def row_of(ref):
    return jnp.concatenate([ref[i:i + 1, :] for i in range(ref.shape[0])], axis=1).astype(jnp.float32)


def normed(x_f, gain, bias):
    mean_val = jnp.mean(x_f, axis=-1, keepdims=True)
    centered = x_f - mean_val
    var_val = jnp.mean(centered * centered, axis=-1, keepdims=True)
    return centered * lax.rsqrt(var_val + LN_EPS) * gain + bias


def attend_kernel(kv_heads, order_ref, pos_ref, span_ref, x_ref, g1_ref, c1_ref, g2_ref, c2_ref, bo_ref, bq_ref, bk_ref, bv_ref, rot_ref, elig_ref, one_ref, two_ref, wr_ref, wq_hbm, wk_hbm, wv_hbm, wo_hbm, k_hbm, v_hbm,
                  k_out, v_out, x_out, h_out, gate_out, w_buf, k_buf, v_buf, q_all, kn_all, vn_all, o_all, h_buf, where_ref, w_sem, o_sem, kv_sem):
    rows, d_model = x_ref.shape
    heads = q_all.shape[1]
    share = heads // kv_heads
    groups = rows // GROUP
    spans = k_hbm.shape[1] // (CHUNK * kv_heads)
    q_tiles = wq_hbm.shape[1] // TILE
    scale = LANES ** -0.5

    def weights(w_hbm, tile, slot):
        return [pltpu.make_async_copy(w_hbm.at[pl.ds(half * HALF, HALF), pl.ds(tile * TILE, TILE)], w_buf.at[slot + half], w_sem.at[slot + half]) for half in range(2)]

    loads = [weights(wq_hbm, i, 2 * i) for i in range(q_tiles)] + [weights(wk_hbm, 0, 2 * q_tiles), weights(wv_hbm, 0, 2 * q_tiles + 2)]
    for pair in loads:
        for copy in pair:
            copy.start()

    def copies(g, n):
        slot = lax.rem(g, DEPTH)
        size = n * CHUNK * kv_heads
        for j in range(GROUP):
            t = order_ref[g * GROUP + j]
            yield pltpu.make_async_copy(k_hbm.at[t, pl.ds(0, size)], k_buf.at[slot, j, pl.ds(0, size)], kv_sem.at[slot, 0])
            yield pltpu.make_async_copy(v_hbm.at[t, pl.ds(0, size)], v_buf.at[slot, j, pl.ds(0, size)], kv_sem.at[slot, 1])

    def each_span(g, body):
        for n in range(1, spans + 1):
            @pl.when(span_ref[g] == n)
            def _(n=n):
                body(n)

    def fetch(g):
        def body(n):
            for copy in copies(g, n):
                copy.start()
        each_span(g, body)

    for g in range(DEPTH - 1):
        fetch(jnp.int32(g))

    col = lax.broadcasted_iota(jnp.int32, where_ref.shape, 1)
    row = lax.broadcasted_iota(jnp.int32, where_ref.shape, 0)
    where_ref[...] = jnp.where(col % kv_heads == (row // share) % kv_heads, col // kv_heads, 1 << 20)
    h_buf[...] = normed(x_ref[...].astype(jnp.float32), row_of(g1_ref), row_of(c1_ref)).astype(jnp.bfloat16)

    def product(index, bias):
        slot = 2 * index
        for copy in loads[index]:
            copy.wait()
        lin = jnp.dot(h_buf[:, :HALF], w_buf[slot], preferred_element_type=jnp.float32) + jnp.dot(h_buf[:, HALF:], w_buf[slot + 1], preferred_element_type=jnp.float32)
        return lin + bias

    def turned(head):
        return (head * rot_ref[0] + pltpu.roll(head, LANES // 2, 1) * rot_ref[1]).astype(jnp.bfloat16)

    bq_row = row_of(bq_ref)
    for i in range(q_tiles):
        lin = product(i, bq_row[:, i * TILE:(i + 1) * TILE])
        for n in range(TILE // LANES):
            q_all[:, i * (TILE // LANES) + n, :] = turned(lin[:, n * LANES:(n + 1) * LANES]).astype(jnp.float32)
    lin = product(q_tiles, row_of(bk_ref))
    for n in range(kv_heads):
        val = turned(lin[:, n * LANES:(n + 1) * LANES])
        k_out[:, n * LANES:(n + 1) * LANES] = val
        for m in range(share):
            kn_all[:, n * share + m, :] = val.astype(jnp.float32)
    lin = product(q_tiles + 1, row_of(bv_ref))
    for n in range(kv_heads):
        val = lin[:, n * LANES:(n + 1) * LANES].astype(jnp.bfloat16)
        v_out[:, n * LANES:(n + 1) * LANES] = val
        for m in range(share):
            vn_all[:, n * share + m, :] = val.astype(jnp.float32)

    def out_weights(tile):
        return pltpu.make_async_copy(wo_hbm.at[:, pl.ds(tile * TILE, TILE)], w_buf.at[tile], o_sem.at[tile])

    for tile in range(d_model // TILE):
        out_weights(tile).start()

    block = lax.broadcasted_iota(jnp.int32, (PART * heads, 1), 0) // heads

    @pl.loop(0, groups)
    def _(g):
        @pl.when(g + DEPTH - 1 < groups)
        def _():
            fetch(g + DEPTH - 1)

        slot = lax.rem(g, DEPTH)

        def body(n):
            size = n * CHUNK * kv_heads
            for copy in copies(g, n):
                copy.wait()
            for lo in range(0, GROUP, PART):
                toks = [order_ref[g * GROUP + lo + j] for j in range(PART)]
                q_rows = [q_all[t] for t in toks]
                s_val = jnp.concatenate([lax.dot_general(q_rows[j].astype(jnp.bfloat16), k_buf[slot, lo + j, :size], ALONG, preferred_element_type=jnp.float32) for j in range(PART)], axis=0) * scale
                q_val = jnp.concatenate(q_rows, axis=0)
                kn_val = jnp.concatenate([kn_all[t] for t in toks], axis=0)
                vn_val = jnp.concatenate([vn_all[t] for t in toks], axis=0)
                s_new = jnp.sum(q_val * kn_val, axis=1, keepdims=True) * scale
                pos = jnp.zeros((PART * heads, 1), jnp.int32)
                for j in range(PART):
                    pos = jnp.where(block == j, pos_ref[g * GROUP + lo + j], pos)
                s_val = jnp.where(where_ref[:, :size] < pos, s_val, -jnp.inf)
                top = jnp.maximum(jnp.max(s_val, axis=1, keepdims=True), s_new)
                e_val, e_new = jnp.exp(s_val - top), jnp.exp(s_new - top)
                inv = 1.0 / (jnp.sum(e_val, axis=1, keepdims=True) + e_new)
                p_val = (e_val * inv).astype(jnp.bfloat16)
                p_new = (e_new * inv).astype(jnp.bfloat16).astype(jnp.float32)
                a_val = jnp.concatenate([jnp.dot(p_val[j * heads:(j + 1) * heads], v_buf[slot, lo + j, :size], preferred_element_type=jnp.float32) for j in range(PART)], axis=0)
                a_val = (a_val + p_new * vn_val).astype(jnp.bfloat16).astype(jnp.float32)
                for j in range(PART):
                    o_all[toks[j]] = a_val[j * heads:(j + 1) * heads]
        each_span(g, body)

    for n in range(heads):
        h_buf[:, n * LANES:(n + 1) * LANES] = o_all[:, n, :].astype(jnp.bfloat16)

    bo_row = row_of(bo_ref)
    for tile in range(d_model // TILE):
        out_weights(tile).wait()
        at = slice(tile * TILE, (tile + 1) * TILE)
        acc = jnp.dot(h_buf[:, :heads * LANES], w_buf[tile], preferred_element_type=jnp.float32)
        x_out[:, at] = (x_ref[:, at].astype(jnp.float32) + acc + bo_row[:, at]).astype(jnp.bfloat16)

    h_two = normed(x_out[...].astype(jnp.float32), row_of(g2_ref), row_of(c2_ref)).astype(jnp.bfloat16)
    h_out[:, :d_model] = h_two
    logits = lax.dot_general(h_two, wr_ref[...], ALONG, preferred_element_type=jnp.float32)
    experts = logits.shape[1]
    expert_ids = lax.broadcasted_iota(jnp.int32, logits.shape, 1)
    stacked = jnp.concatenate([elig_ref[...], one_ref[...], two_ref[...], jnp.zeros((rows - experts - 2, rows), jnp.int32)], axis=0)
    meta = stacked.astype(jnp.float32).T.astype(jnp.int32)
    pick_one, pick_two = meta[:, experts:experts + 1], meta[:, experts + 1:experts + 2]
    hit_one, hit_two = expert_ids == pick_one, expert_ids == pick_two
    keep_one = meta[:, :experts] == 1

    def gate(keep, hit):
        val = jnp.where(keep, logits, -jnp.inf)
        e_val = jnp.exp(val - jnp.max(val, axis=1, keepdims=True))
        return jnp.sum(jnp.where(hit, e_val, 0.0), axis=1, keepdims=True) / jnp.sum(e_val, axis=1, keepdims=True)

    lane = lax.broadcasted_iota(jnp.int32, gate_out.shape, 1)
    gate_out[...] = jnp.where(lane == 0, gate(keep_one, hit_one), gate(keep_one & jnp.logical_not(hit_one), hit_two))
    ids = jnp.where(lane == 0, pick_one, jnp.where(lane == 1, pick_two, 0))
    h_out[:, d_model:] = ids.astype(jnp.float32).astype(jnp.bfloat16)


def attention_layer(tokens, k_cache, v_cache, positions, expert_one, expert_two, eligible, ln1_gain, ln1_bias, w_query, b_query, w_key, b_key, w_value, b_value, w_out, b_out, ln2_gain, ln2_bias, w_router):
    rows, seq_len, kv_heads, head_dim = k_cache.shape
    d_model = tokens.shape[1]
    heads = w_query.shape[1] // head_dim
    kv_dim = kv_heads * head_dim
    ids = jnp.arange(rows, dtype=jnp.int32)
    ahead = (positions[None, :] < positions[:, None]) | ((positions[None, :] == positions[:, None]) & (ids[None, :] < ids[:, None]))
    rank = jnp.sum(ahead.astype(jnp.int32), axis=1)
    hit = rank[None, :] == ids[:, None]
    order = jnp.sum(jnp.where(hit, ids[None, :], 0), axis=1)
    pos_sorted = jnp.sum(jnp.where(hit, positions[None, :], 0), axis=1)
    span = jnp.clip((pos_sorted[GROUP - 1::GROUP] + CHUNK - 1) // CHUNK, 1, seq_len // CHUNK)
    half_dim = head_dim // 2
    inv_freq = ROPE_BASE ** (jnp.arange(half_dim, dtype=jnp.float32) * (-2.0 / head_dim))
    angles = positions.astype(jnp.float32)[:, None] * jnp.concatenate([inv_freq, inv_freq])[None, :]
    sign = jnp.where(jnp.arange(head_dim) < half_dim, -1.0, 1.0).astype(jnp.float32)
    rot = jnp.stack([jnp.cos(angles), jnp.sin(angles) * sign[None, :]])
    small = [p.reshape(-1, LANES) for p in (ln1_gain, ln1_bias, ln2_gain, ln2_bias, b_out, b_query, b_key, b_value)]
    vmem = pl.BlockSpec(memory_space=pltpu.VMEM)
    smem = pl.BlockSpec(memory_space=pltpu.SMEM)
    hbm = pl.BlockSpec(memory_space=pl.ANY)
    flat = (rows, seq_len * kv_heads, head_dim)
    spread = pltpu.VMEM((rows, heads, head_dim), jnp.float32)
    return pl.pallas_call(
        functools.partial(attend_kernel, kv_heads),
        name='attention_layer',
        out_shape=(jax.ShapeDtypeStruct((rows, kv_dim), jnp.bfloat16), jax.ShapeDtypeStruct((rows, kv_dim), jnp.bfloat16),
                   jax.ShapeDtypeStruct((rows, d_model), jnp.bfloat16), jax.ShapeDtypeStruct((rows, d_model + LANES), jnp.bfloat16),
                   jax.ShapeDtypeStruct((rows, LANES), jnp.float32)),
        in_specs=[smem, smem, smem] + [vmem] * 14 + [hbm, hbm, hbm, hbm, hbm, hbm],
        out_specs=(vmem,) * 5,
        scratch_shapes=[
            pltpu.VMEM((2 * (heads * head_dim + 2 * kv_dim) // TILE, HALF, TILE), jnp.bfloat16),
            pltpu.VMEM((DEPTH, GROUP) + flat[1:], jnp.bfloat16), pltpu.VMEM((DEPTH, GROUP) + flat[1:], jnp.bfloat16),
            spread, spread, spread, spread,
            pltpu.VMEM((rows, d_model), jnp.bfloat16),
            pltpu.VMEM((PART * heads, flat[1]), jnp.int32),
            pltpu.SemaphoreType.DMA((2 * (heads * head_dim + 2 * kv_dim) // TILE,)),
            pltpu.SemaphoreType.DMA((d_model // TILE,)),
            pltpu.SemaphoreType.DMA((DEPTH, 2))],
        compiler_params=pltpu.CompilerParams(vmem_limit_bytes=62 * 1024 * 1024),
    )(order, pos_sorted, span, tokens, *small, rot, eligible.T, expert_one[None], expert_two[None], w_router.T, w_query, w_key, w_value, w_out, k_cache.reshape(flat), v_cache.reshape(flat))


def seat(slot):
    return {3: 4, 4: 3}.get(slot, slot)


def flip(me, bit):
    return me + bit - 2 * bit * ((me // bit) % 2)


def meet_neighbours():
    me = lax.axis_index('ep')
    barrier = pltpu.get_barrier_semaphore()
    for bit in (1, 2, 4, 8):
        pl.semaphore_signal(barrier, inc=1, device_id=(flip(me, bit),), device_id_type=MESH)
    pl.semaphore_wait(barrier, 4)
    return me


def gather_kernel(bounds, h_ref, wg_hbm, wu_hbm, z_ref, rel_ref, x_a, x_b, x_c, wg_ref, wu_ref, own_sem, send_sem, recv_sem, side_send, side_recv):
    rows = x_a.shape[1] // 2
    bufs = (x_a, x_b, x_c)
    copies = []
    for f in range(3):
        lo, hi = bounds[f]
        copies.append(pltpu.make_async_copy(h_ref.at[:, pl.ds(lo, hi - lo)], bufs[f].at[0, pl.ds(0, rows)], own_sem.at[f]))
        copies[-1].start()
    me = meet_neighbours()

    def hop(f, src, bit):
        return pltpu.make_async_remote_copy(
            src_ref=bufs[f].at[seat(src), pl.ds(0, rows)], dst_ref=bufs[f].at[seat(src ^ bit), pl.ds(0, rows)],
            send_sem=send_sem.at[f, src ^ bit], recv_sem=recv_sem.at[f, src ^ bit],
            device_id=(flip(me, 2 * bit),), device_id_type=MESH)

    def side(f, src):
        return pltpu.make_async_remote_copy(
            src_ref=bufs[f].at[seat(src), pl.ds(0, rows)], dst_ref=bufs[f].at[seat(src), pl.ds(rows, rows)],
            send_sem=side_send.at[f, src], recv_sem=side_recv.at[f, src],
            device_id=(flip(me, 1),), device_id_type=MESH)

    def landed(f, slot):
        hop(f, 0, slot).wait_recv()

    def activate(first, count):
        u_val = v_val = None
        for f in range(3):
            lo, hi = bounds[f]
            hi = min(hi, wg_ref.shape[1])
            x_val = bufs[f][first:first + count, :, : hi - lo].reshape(2 * rows * count, hi - lo)
            u_part = lax.dot_general(x_val, wg_ref[:, lo:hi], ALONG, preferred_element_type=jnp.float32)
            v_part = lax.dot_general(x_val, wu_ref[:, lo:hi], ALONG, preferred_element_type=jnp.float32)
            u_val = u_part if u_val is None else u_val + u_part
            v_val = v_part if v_val is None else v_val + v_part
        z_ref[first:first + count] = (jax.nn.silu(u_val) * v_val).astype(jnp.bfloat16).reshape(count, 2 * rows, -1)
        for i in range(first, first + count):
            ids = bufs[2][i, :rows, bounds[2][1] - bounds[2][0] - LANES:]
            rel_ref[i] = ids.astype(jnp.float32).astype(jnp.int32) ^ me

    for f in range(3):
        copies[f].wait()
        hop(f, 0, ORDERS[f][0]).start()
    weights = [pltpu.make_async_copy(src, dst, own_sem.at[3 + i]) for i, (src, dst) in enumerate(((wg_hbm, wg_ref), (wu_hbm, wu_ref)))]
    for f in range(3):
        side(f, 0).start()
    for copy in weights:
        copy.start()
    for stage in (1, 2):
        for f in range(3):
            hop(f, 0, ORDERS[f][stage]).start()
    for f in range(3):
        side(f, 0).wait_recv()
    for copy in weights:
        copy.wait()
    activate(0, 1)
    for f in range(3):
        a, b, g = ORDERS[f]
        landed(f, a)
        hop(f, a, b).start()
        hop(f, a, g).start()
        side(f, a).start()
    for f in range(3):
        a, b, g = ORDERS[f]
        landed(f, b)
        hop(f, b, g).start()
        side(f, b).start()
    for f in range(3):
        a, b, g = ORDERS[f]
        landed(f, a ^ b)
        hop(f, a ^ b, g).start()
        side(f, a ^ b).start()
    for f in range(3):
        g = ORDERS[f][2]
        landed(f, g)
        side(f, g).start()
    for f in range(3):
        for slot in (1, 2, 4):
            side(f, slot).wait_recv()

    activate(1, 3)
    for f in range(3):
        a, b, g = ORDERS[f]
        landed(f, a ^ g)
        side(f, a ^ g).start()
        landed(f, b ^ g)
        side(f, b ^ g).start()
    for f in range(3):
        for slot in (3, 5, 6):
            side(f, slot).wait_recv()

    activate(4, 3)
    for f in range(3):
        landed(f, 7)
        side(f, 7).start()
    for f in range(3):
        side(f, 7).wait_recv()
    activate(7, 1)
    for f in range(3):
        for slot in range(8):
            side(f, slot).wait_send()
        for slot in range(1, 8):
            hop(f, 0, slot).wait_send()


def return_kernel(z_ref, wd_ref, rel_ref, gate_ref, x_ref, out_ref, pair_buf, side_buf, near_buf, turn_buf, turn_in, last_buf, last_in, side_send, side_recv, hop_send, hop_recv):
    rows = x_ref.shape[0]
    chunks = pair_buf.shape[0]
    me = meet_neighbours()

    def slot_of(f, place):
        a, b, g = ORDERS[f]
        return a * (place // 4) + b * (place // 2 % 2) + g * (place % 2)

    def remote(src, dst, send, recv, bit):
        return pltpu.make_async_remote_copy(src_ref=src, dst_ref=dst, send_sem=send, recv_sem=recv, device_id=(flip(me, bit),), device_id_type=MESH)

    def side(part):
        f, q, s, lo, width = part
        cols = pl.ds(lo, width)
        return remote(side_buf.at[q, :, cols], pair_buf.at[q, 1, :, cols], side_send.at[s], side_recv.at[s], 1)

    def hop_one(part):
        f, q, s, lo, width = part
        cols = pl.ds(lo, width)
        return remote(pair_buf.at[q, :, pl.ds(4 * rows, 4 * rows), cols], near_buf.at[q, :, :, cols], hop_send.at[0, s], hop_recv.at[0, s], 2 * ORDERS[f][0])

    def hop_two(part):
        f, q, s, lo, width = part
        cols = pl.ds(lo, width)
        return remote(turn_buf.at[q, :, :, cols], turn_in.at[q, :, :, cols], hop_send.at[1, s], hop_recv.at[1, s], 2 * ORDERS[f][1])

    def hop_three(part):
        f, q, s, lo, width = part
        cols = pl.ds(lo, width)
        return remote(last_buf.at[q, :, :, cols], last_in.at[q, :, :, cols], hop_send.at[2, s], hop_recv.at[2, s], 2 * ORDERS[f][2])

    def project(part):
        f, q, s, lo, width = part
        w_val = wd_ref[:, pl.ds(pl.multiple_of(q * WIDTH + lo, LANES), width)]
        for place in range(8):
            e_val = jnp.dot(z_ref[seat(slot_of(f, place))], w_val, preferred_element_type=jnp.float32).astype(jnp.bfloat16)
            pair_buf[q, 0, place * rows:(place + 1) * rows, lo:lo + width] = e_val[:rows]
            side_buf[q, place * rows:(place + 1) * rows, lo:lo + width] = e_val[rows:]
        side(part).start()

    def send_far(part):
        side(part).wait_recv()
        hop_one(part).start()

    def choose(part, place, k, other):
        f, q, s, lo, width = part
        rel = rel_ref[seat(slot_of(f, place))][:, k:k + 1]
        at, cols = pl.ds(place * rows, rows), pl.ds(lo, width)
        far = 2 * ORDERS[f][0]
        val = near_buf[q, 1, at, cols].astype(jnp.float32)
        if other is not None:
            val = jnp.where(rel == far + 1, val, other)
        val = jnp.where(rel == far, near_buf[q, 0, at, cols].astype(jnp.float32), val)
        val = jnp.where(rel == 1, pair_buf[q, 1, at, cols].astype(jnp.float32), val)
        return jnp.where(rel == 0, pair_buf[q, 0, at, cols].astype(jnp.float32), val)

    def turn(part):
        f, q, s, lo, width = part
        hop_one(part).wait_recv()
        for k in range(2):
            for half in range(2):
                turn_buf[q, k, half * rows:(half + 1) * rows, lo:lo + width] = choose(part, 2 + half, k, None).astype(jnp.bfloat16)
        hop_two(part).start()

    def last(part):
        f, q, s, lo, width = part
        hop_two(part).wait_recv()
        for k in range(2):
            other = turn_in[q, k, rows:2 * rows, lo:lo + width].astype(jnp.float32)
            last_buf[q, k, :, lo:lo + width] = choose(part, 1, k, other).astype(jnp.bfloat16)
        hop_three(part).start()

    def finish(part):
        f, q, s, lo, width = part
        hop_three(part).wait_recv()
        g_bit = 2 * ORDERS[f][2]
        y_val = None
        for k in range(2):
            rel = rel_ref[0][:, k:k + 1]
            other = jnp.where((rel // g_bit) % 2 == 1, last_in[q, k, :, lo:lo + width].astype(jnp.float32), turn_in[q, k, :rows, lo:lo + width].astype(jnp.float32))
            add = gate_ref[:, k:k + 1] * choose(part, 0, k, other)
            y_val = add if y_val is None else y_val + add
        at = pl.ds(pl.multiple_of(q * WIDTH + lo, LANES), width)
        out_ref[:, at] = (x_ref[:, at].astype(jnp.float32) + y_val).astype(jnp.bfloat16)

    full = chunks // 3
    tail = [(f, chunks - 1, chunks - 1 + f, f * LANES, LANES) for f in range(2)]

    def body(f, j):
        return f, 3 * j + f, 3 * j + f, 0, WIDTH

    def sweep(step):
        @pl.loop(0, full)
        def _(j):
            for f in range(3):
                step(body(f, j))
        for part in tail:
            step(part)

    for f in range(3):
        project(body(f, 0))

    @pl.loop(1, full)
    def _(j):
        for f in range(3):
            project(body(f, j))
            send_far(body(f, j - 1))

    for part in tail:
        project(part)
    for part in [body(f, full - 1) for f in range(3)] + tail:
        send_far(part)
    sweep(turn)
    sweep(last)
    sweep(finish)

    def drain(part):
        side(part).wait_send()
        hop_one(part).wait_send()
        hop_two(part).wait_send()
        hop_three(part).wait_send()
    sweep(drain)


def gather_and_activate(h_ext, w_gate, w_up):
    rows, d_model = h_ext.shape[0], h_ext.shape[1] - LANES
    d_ff = w_gate.shape[0]
    tiles = (d_model + LANES) // LANES
    cuts = [LANES * ((tiles * f + 2) // 3) for f in range(4)]
    bounds = tuple((cuts[f], cuts[f + 1]) for f in range(3))
    vmem = pl.BlockSpec(memory_space=pltpu.VMEM)
    return pl.pallas_call(
        functools.partial(gather_kernel, bounds),
        name='gather_rows',
        out_shape=(jax.ShapeDtypeStruct((8, 2 * rows, d_ff), jnp.bfloat16), jax.ShapeDtypeStruct((8, rows, LANES), jnp.int32)),
        in_specs=[pl.BlockSpec(memory_space=pl.ANY)] * 3,
        out_specs=(vmem, vmem),
        scratch_shapes=[pltpu.VMEM((8, 2 * rows, hi - lo), jnp.bfloat16) for lo, hi in bounds] + [
            pltpu.VMEM(w_gate.shape, jnp.bfloat16), pltpu.VMEM(w_gate.shape, jnp.bfloat16),
            pltpu.SemaphoreType.DMA((5,)),
            pltpu.SemaphoreType.DMA((3, 8)), pltpu.SemaphoreType.DMA((3, 8)),
            pltpu.SemaphoreType.DMA((3, 8)), pltpu.SemaphoreType.DMA((3, 8))],
        compiler_params=pltpu.CompilerParams(collective_id=0, has_side_effects=True, vmem_limit_bytes=60 * 1024 * 1024),
    )(h_ext, w_gate, w_up)


def project_and_return(z_val, w_down, rel, gates, x_mid):
    rows, d_model = x_mid.shape
    chunks = d_model // WIDTH
    vmem = pl.BlockSpec(memory_space=pltpu.VMEM)
    return pl.pallas_call(
        return_kernel,
        name='return_rows',
        out_shape=jax.ShapeDtypeStruct((rows, d_model), jnp.bfloat16),
        in_specs=[vmem] * 5,
        out_specs=vmem,
        scratch_shapes=[
            pltpu.VMEM((chunks, 2, 8 * rows, WIDTH), jnp.bfloat16),
            pltpu.VMEM((chunks, 8 * rows, WIDTH), jnp.bfloat16),
            pltpu.VMEM((chunks, 2, 4 * rows, WIDTH), jnp.bfloat16),
            pltpu.VMEM((chunks, 2, 2 * rows, WIDTH), jnp.bfloat16),
            pltpu.VMEM((chunks, 2, 2 * rows, WIDTH), jnp.bfloat16),
            pltpu.VMEM((chunks, 2, rows, WIDTH), jnp.bfloat16),
            pltpu.VMEM((chunks, 2, rows, WIDTH), jnp.bfloat16),
            pltpu.SemaphoreType.DMA((chunks + 1,)), pltpu.SemaphoreType.DMA((chunks + 1,)),
            pltpu.SemaphoreType.DMA((3, chunks + 1)), pltpu.SemaphoreType.DMA((3, chunks + 1))],
        compiler_params=pltpu.CompilerParams(collective_id=1, has_side_effects=True, vmem_limit_bytes=63 * 1024 * 1024),
    )(z_val, w_down, rel, gates, x_mid)


def solution(mesh):
    def local_step(tokens, k_cache, v_cache, positions, expert_one, expert_two, eligible, ln1_gain, ln1_bias, w_query, b_query, w_key, b_key, w_value, b_value, w_out, b_out, ln2_gain, ln2_bias, w_router, w_gate, w_up, w_down):
        rows, seq_len, kv_heads, head_dim = k_cache.shape
        k_val, v_val, x_mid, h_ext, gates = attention_layer(tokens, k_cache, v_cache, positions, expert_one, expert_two, eligible, ln1_gain, ln1_bias, w_query, b_query, w_key, b_key, w_value, b_value, w_out, b_out, ln2_gain, ln2_bias, w_router)
        z_val, rel = gather_and_activate(h_ext, w_gate[0].T, w_up[0].T)
        tokens_out = project_and_return(z_val, w_down[0], rel, gates, x_mid)
        key_new, value_new = k_val.reshape(rows, kv_heads, head_dim), v_val.reshape(rows, kv_heads, head_dim)
        return tokens_out, key_new, value_new

    row_spec = P('ep', None)
    cache_spec = P('ep', None, None, None)
    vec_spec = P('ep')
    rep_one = P(None)
    rep_two = P(None, None)
    expert_spec = P('ep', None, None)
    in_specs = (row_spec, cache_spec, cache_spec, vec_spec, vec_spec, vec_spec, row_spec, rep_one, rep_one, rep_two, rep_one, rep_two, rep_one, rep_two, rep_one, rep_two, rep_one, rep_one, rep_one, rep_two, expert_spec, expert_spec, expert_spec)
    out_specs = (row_spec, expert_spec, expert_spec)
    return jax.shard_map(local_step, mesh=mesh, in_specs=in_specs, out_specs=out_specs, check_vma=False)
```

```python
import functools

import jax
import jax.numpy as jnp
from jax import lax
from jax.experimental import pallas as pl
from jax.experimental.pallas import tpu as pltpu
from jax.sharding import PartitionSpec as P

ROPE_BASE = 10000.0
LN_EPS = 1e-5

MESH = pl.DeviceIdType.MESH
ORDERS = ((1, 2, 4), (2, 4, 1), (4, 1, 2))
LANES = 128
WIDTH = 256
ALONG = (((1,), (1,)), ((), ()))


TILE = 512
HALF = 2048
GROUP = 8
PART = 8
DEPTH = 3
CHUNK = 64


def row_of(ref):
    return jnp.concatenate([ref[i:i + 1, :] for i in range(ref.shape[0])], axis=1).astype(jnp.float32)


def normed(x_f, gain, bias):
    mean_val = jnp.mean(x_f, axis=-1, keepdims=True)
    centered = x_f - mean_val
    var_val = jnp.mean(centered * centered, axis=-1, keepdims=True)
    return centered * lax.rsqrt(var_val + LN_EPS) * gain + bias


def attend_kernel(kv_heads, order_ref, pos_ref, span_ref, x_ref, g1_ref, c1_ref, g2_ref, c2_ref, bo_ref, bq_ref, bk_ref, bv_ref, rot_ref, elig_ref, one_ref, two_ref, wr_ref, wq_hbm, wk_hbm, wv_hbm, wo_hbm, k_hbm, v_hbm,
                  k_out, v_out, x_out, h_out, gate_out, w_buf, k_buf, v_buf, q_all, kn_all, vn_all, o_all, new_all, h_buf, where_ref, w_sem, o_sem, kv_sem):
    rows, d_model = x_ref.shape
    heads = q_all.shape[1]
    share = heads // kv_heads
    groups = rows // GROUP
    spans = k_hbm.shape[1] // (CHUNK * kv_heads)
    q_tiles = wq_hbm.shape[1] // TILE
    scale = LANES ** -0.5

    def weights(w_hbm, tile, slot):
        return [pltpu.make_async_copy(w_hbm.at[pl.ds(half * HALF, HALF), pl.ds(tile * TILE, TILE)], w_buf.at[slot + half], w_sem.at[slot + half]) for half in range(2)]

    loads = [weights(wq_hbm, i, 2 * i) for i in range(q_tiles)] + [weights(wk_hbm, 0, 2 * q_tiles), weights(wv_hbm, 0, 2 * q_tiles + 2)]
    for pair in loads:
        for copy in pair:
            copy.start()

    def copies(g, n):
        slot = lax.rem(g, DEPTH)
        size = n * CHUNK * kv_heads
        for j in range(GROUP):
            t = order_ref[g * GROUP + j]
            yield pltpu.make_async_copy(k_hbm.at[t, pl.ds(0, size)], k_buf.at[slot, j, pl.ds(0, size)], kv_sem.at[slot, 0])
            yield pltpu.make_async_copy(v_hbm.at[t, pl.ds(0, size)], v_buf.at[slot, j, pl.ds(0, size)], kv_sem.at[slot, 1])

    def each_span(g, body):
        for n in range(1, spans + 1):
            @pl.when(span_ref[g] == n)
            def _(n=n):
                body(n)

    def fetch(g):
        def body(n):
            for copy in copies(g, n):
                copy.start()
        each_span(g, body)

    for g in range(DEPTH - 1):
        fetch(jnp.int32(g))

    col = lax.broadcasted_iota(jnp.int32, where_ref.shape, 1)
    row = lax.broadcasted_iota(jnp.int32, where_ref.shape, 0)
    where_ref[...] = jnp.where(col % kv_heads == (row // share) % kv_heads, col // kv_heads, 1 << 20)
    h_buf[...] = normed(x_ref[...].astype(jnp.float32), row_of(g1_ref), row_of(c1_ref)).astype(jnp.bfloat16)

    def product(index, bias):
        slot = 2 * index
        for copy in loads[index]:
            copy.wait()
        lin = jnp.dot(h_buf[:, :HALF], w_buf[slot], preferred_element_type=jnp.float32) + jnp.dot(h_buf[:, HALF:], w_buf[slot + 1], preferred_element_type=jnp.float32)
        return lin + bias

    def turned(head):
        return (head * rot_ref[0] + pltpu.roll(head, LANES // 2, 1) * rot_ref[1]).astype(jnp.bfloat16)

    bq_row = row_of(bq_ref)
    for i in range(q_tiles):
        lin = product(i, bq_row[:, i * TILE:(i + 1) * TILE])
        for n in range(TILE // LANES):
            q_all[:, i * (TILE // LANES) + n, :] = turned(lin[:, n * LANES:(n + 1) * LANES]).astype(jnp.float32)
    lin = product(q_tiles, row_of(bk_ref))
    for n in range(kv_heads):
        val = turned(lin[:, n * LANES:(n + 1) * LANES])
        new_all[:, n, :] = val.astype(jnp.float32)
        for m in range(share):
            kn_all[:, n * share + m, :] = val.astype(jnp.float32)
    k_out[...] = new_all[...].astype(jnp.bfloat16)
    lin = product(q_tiles + 1, row_of(bv_ref))
    for n in range(kv_heads):
        val = lin[:, n * LANES:(n + 1) * LANES].astype(jnp.bfloat16)
        new_all[:, n, :] = val.astype(jnp.float32)
        for m in range(share):
            vn_all[:, n * share + m, :] = val.astype(jnp.float32)

    v_out[...] = new_all[...].astype(jnp.bfloat16)

    def out_weights(tile):
        return pltpu.make_async_copy(wo_hbm.at[:, pl.ds(tile * TILE, TILE)], w_buf.at[tile], o_sem.at[tile])

    for tile in range(d_model // TILE):
        out_weights(tile).start()

    block = lax.broadcasted_iota(jnp.int32, (PART * heads, 1), 0) // heads

    @pl.loop(0, groups)
    def _(g):
        @pl.when(g + DEPTH - 1 < groups)
        def _():
            fetch(g + DEPTH - 1)

        slot = lax.rem(g, DEPTH)

        def body(n):
            size = n * CHUNK * kv_heads
            for copy in copies(g, n):
                copy.wait()
            for lo in range(0, GROUP, PART):
                toks = [order_ref[g * GROUP + lo + j] for j in range(PART)]
                q_rows = [q_all[t] for t in toks]
                s_val = jnp.concatenate([lax.dot_general(q_rows[j].astype(jnp.bfloat16), k_buf[slot, lo + j, :size], ALONG, preferred_element_type=jnp.float32) for j in range(PART)], axis=0) * scale
                q_val = jnp.concatenate(q_rows, axis=0)
                kn_val = jnp.concatenate([kn_all[t] for t in toks], axis=0)
                vn_val = jnp.concatenate([vn_all[t] for t in toks], axis=0)
                s_new = jnp.sum(q_val * kn_val, axis=1, keepdims=True) * scale
                pos = jnp.zeros((PART * heads, 1), jnp.int32)
                for j in range(PART):
                    pos = jnp.where(block == j, pos_ref[g * GROUP + lo + j], pos)
                s_val = jnp.where(where_ref[:, :size] < pos, s_val, -jnp.inf)
                top = jnp.maximum(jnp.max(s_val, axis=1, keepdims=True), s_new)
                e_val, e_new = jnp.exp(s_val - top), jnp.exp(s_new - top)
                inv = 1.0 / (jnp.sum(e_val, axis=1, keepdims=True) + e_new)
                p_val = (e_val * inv).astype(jnp.bfloat16)
                p_new = (e_new * inv).astype(jnp.bfloat16).astype(jnp.float32)
                a_val = jnp.concatenate([jnp.dot(p_val[j * heads:(j + 1) * heads], v_buf[slot, lo + j, :size], preferred_element_type=jnp.float32) for j in range(PART)], axis=0)
                a_val = (a_val + p_new * vn_val).astype(jnp.bfloat16).astype(jnp.float32)
                for j in range(PART):
                    o_all[toks[j]] = a_val[j * heads:(j + 1) * heads]
        each_span(g, body)

    for n in range(heads):
        h_buf[:, n * LANES:(n + 1) * LANES] = o_all[:, n, :].astype(jnp.bfloat16)

    bo_row = row_of(bo_ref)
    for tile in range(d_model // TILE):
        out_weights(tile).wait()
        at = slice(tile * TILE, (tile + 1) * TILE)
        acc = jnp.dot(h_buf[:, :heads * LANES], w_buf[tile], preferred_element_type=jnp.float32)
        x_out[:, at] = (x_ref[:, at].astype(jnp.float32) + acc + bo_row[:, at]).astype(jnp.bfloat16)

    h_two = normed(x_out[...].astype(jnp.float32), row_of(g2_ref), row_of(c2_ref)).astype(jnp.bfloat16)
    h_out[:, :d_model] = h_two
    logits = lax.dot_general(h_two, wr_ref[...], ALONG, preferred_element_type=jnp.float32)
    experts = logits.shape[1]
    expert_ids = lax.broadcasted_iota(jnp.int32, logits.shape, 1)
    stacked = jnp.concatenate([elig_ref[...], one_ref[...], two_ref[...], jnp.zeros((rows - experts - 2, rows), jnp.int32)], axis=0)
    meta = stacked.astype(jnp.float32).T.astype(jnp.int32)
    pick_one, pick_two = meta[:, experts:experts + 1], meta[:, experts + 1:experts + 2]
    hit_one, hit_two = expert_ids == pick_one, expert_ids == pick_two
    keep_one = meta[:, :experts] == 1

    def gate(keep, hit):
        val = jnp.where(keep, logits, -jnp.inf)
        e_val = jnp.exp(val - jnp.max(val, axis=1, keepdims=True))
        return jnp.sum(jnp.where(hit, e_val, 0.0), axis=1, keepdims=True) / jnp.sum(e_val, axis=1, keepdims=True)

    lane = lax.broadcasted_iota(jnp.int32, gate_out.shape, 1)
    gate_out[...] = jnp.where(lane == 0, gate(keep_one, hit_one), gate(keep_one & jnp.logical_not(hit_one), hit_two))
    ids = jnp.where(lane == 0, pick_one, jnp.where(lane == 1, pick_two, 0))
    h_out[:, d_model:] = ids.astype(jnp.float32).astype(jnp.bfloat16)


def attention_layer(tokens, k_cache, v_cache, positions, expert_one, expert_two, eligible, ln1_gain, ln1_bias, w_query, b_query, w_key, b_key, w_value, b_value, w_out, b_out, ln2_gain, ln2_bias, w_router):
    rows, seq_len, kv_heads, head_dim = k_cache.shape
    d_model = tokens.shape[1]
    heads = w_query.shape[1] // head_dim
    kv_dim = kv_heads * head_dim
    ids = jnp.arange(rows, dtype=jnp.int32)
    ahead = (positions[None, :] < positions[:, None]) | ((positions[None, :] == positions[:, None]) & (ids[None, :] < ids[:, None]))
    rank = jnp.sum(ahead.astype(jnp.int32), axis=1)
    hit = rank[None, :] == ids[:, None]
    order = jnp.sum(jnp.where(hit, ids[None, :], 0), axis=1)
    pos_sorted = jnp.sum(jnp.where(hit, positions[None, :], 0), axis=1)
    span = jnp.clip((pos_sorted[GROUP - 1::GROUP] + CHUNK - 1) // CHUNK, 1, seq_len // CHUNK)
    half_dim = head_dim // 2
    inv_freq = ROPE_BASE ** (jnp.arange(half_dim, dtype=jnp.float32) * (-2.0 / head_dim))
    angles = positions.astype(jnp.float32)[:, None] * jnp.concatenate([inv_freq, inv_freq])[None, :]
    sign = jnp.where(jnp.arange(head_dim) < half_dim, -1.0, 1.0).astype(jnp.float32)
    rot = jnp.stack([jnp.cos(angles), jnp.sin(angles) * sign[None, :]])
    small = [p.reshape(-1, LANES) for p in (ln1_gain, ln1_bias, ln2_gain, ln2_bias, b_out, b_query, b_key, b_value)]
    vmem = pl.BlockSpec(memory_space=pltpu.VMEM)
    smem = pl.BlockSpec(memory_space=pltpu.SMEM)
    hbm = pl.BlockSpec(memory_space=pl.ANY)
    flat = (rows, seq_len * kv_heads, head_dim)
    spread = pltpu.VMEM((rows, heads, head_dim), jnp.float32)
    return pl.pallas_call(
        functools.partial(attend_kernel, kv_heads),
        name='attention_layer',
        out_shape=(jax.ShapeDtypeStruct((rows, kv_heads, head_dim), jnp.bfloat16), jax.ShapeDtypeStruct((rows, kv_heads, head_dim), jnp.bfloat16),
                   jax.ShapeDtypeStruct((rows, d_model), jnp.bfloat16), jax.ShapeDtypeStruct((rows, d_model + LANES), jnp.bfloat16),
                   jax.ShapeDtypeStruct((rows, LANES), jnp.float32)),
        in_specs=[smem, smem, smem] + [vmem] * 14 + [hbm, hbm, hbm, hbm, hbm, hbm],
        out_specs=(vmem,) * 5,
        scratch_shapes=[
            pltpu.VMEM((2 * (heads * head_dim + 2 * kv_dim) // TILE, HALF, TILE), jnp.bfloat16),
            pltpu.VMEM((DEPTH, GROUP) + flat[1:], jnp.bfloat16), pltpu.VMEM((DEPTH, GROUP) + flat[1:], jnp.bfloat16),
            spread, spread, spread, spread,
            pltpu.VMEM((rows, kv_heads, head_dim), jnp.float32),
            pltpu.VMEM((rows, d_model), jnp.bfloat16),
            pltpu.VMEM((PART * heads, flat[1]), jnp.int32),
            pltpu.SemaphoreType.DMA((2 * (heads * head_dim + 2 * kv_dim) // TILE,)),
            pltpu.SemaphoreType.DMA((d_model // TILE,)),
            pltpu.SemaphoreType.DMA((DEPTH, 2))],
        compiler_params=pltpu.CompilerParams(vmem_limit_bytes=62 * 1024 * 1024),
    )(order, pos_sorted, span, tokens, *small, rot, eligible.T, expert_one[None], expert_two[None], w_router.T, w_query, w_key, w_value, w_out, k_cache.reshape(flat), v_cache.reshape(flat))


def seat(slot):
    return {3: 4, 4: 3}.get(slot, slot)


def flip(me, bit):
    return me + bit - 2 * bit * ((me // bit) % 2)


def meet_neighbours():
    me = lax.axis_index('ep')
    barrier = pltpu.get_barrier_semaphore()
    for bit in (1, 2, 4, 8):
        pl.semaphore_signal(barrier, inc=1, device_id=(flip(me, bit),), device_id_type=MESH)
    pl.semaphore_wait(barrier, 4)
    return me


def gather_kernel(bounds, h_ref, wg_hbm, wu_hbm, z_ref, rel_ref, x_a, x_b, x_c, wg_ref, wu_ref, own_sem, send_sem, recv_sem, side_send, side_recv):
    rows = x_a.shape[1] // 2
    bufs = (x_a, x_b, x_c)
    copies = []
    for f in range(3):
        lo, hi = bounds[f]
        copies.append(pltpu.make_async_copy(h_ref.at[:, pl.ds(lo, hi - lo)], bufs[f].at[0, pl.ds(0, rows)], own_sem.at[f]))
        copies[-1].start()
    me = meet_neighbours()

    def hop(f, src, bit):
        return pltpu.make_async_remote_copy(
            src_ref=bufs[f].at[seat(src), pl.ds(0, rows)], dst_ref=bufs[f].at[seat(src ^ bit), pl.ds(0, rows)],
            send_sem=send_sem.at[f, src ^ bit], recv_sem=recv_sem.at[f, src ^ bit],
            device_id=(flip(me, 2 * bit),), device_id_type=MESH)

    def side(f, src):
        return pltpu.make_async_remote_copy(
            src_ref=bufs[f].at[seat(src), pl.ds(0, rows)], dst_ref=bufs[f].at[seat(src), pl.ds(rows, rows)],
            send_sem=side_send.at[f, src], recv_sem=side_recv.at[f, src],
            device_id=(flip(me, 1),), device_id_type=MESH)

    def landed(f, slot):
        hop(f, 0, slot).wait_recv()

    def activate(first, count):
        u_val = v_val = None
        for f in range(3):
            lo, hi = bounds[f]
            hi = min(hi, wg_ref.shape[1])
            x_val = bufs[f][first:first + count, :, : hi - lo].reshape(2 * rows * count, hi - lo)
            u_part = lax.dot_general(x_val, wg_ref[:, lo:hi], ALONG, preferred_element_type=jnp.float32)
            v_part = lax.dot_general(x_val, wu_ref[:, lo:hi], ALONG, preferred_element_type=jnp.float32)
            u_val = u_part if u_val is None else u_val + u_part
            v_val = v_part if v_val is None else v_val + v_part
        z_ref[first:first + count] = (jax.nn.silu(u_val) * v_val).astype(jnp.bfloat16).reshape(count, 2 * rows, -1)
        for i in range(first, first + count):
            ids = bufs[2][i, :rows, bounds[2][1] - bounds[2][0] - LANES:]
            rel_ref[i] = ids.astype(jnp.float32).astype(jnp.int32) ^ me

    for f in range(3):
        copies[f].wait()
        hop(f, 0, ORDERS[f][0]).start()
    weights = [pltpu.make_async_copy(src, dst, own_sem.at[3 + i]) for i, (src, dst) in enumerate(((wg_hbm, wg_ref), (wu_hbm, wu_ref)))]
    for f in range(3):
        side(f, 0).start()
    for copy in weights:
        copy.start()
    for stage in (1, 2):
        for f in range(3):
            hop(f, 0, ORDERS[f][stage]).start()
    for f in range(3):
        side(f, 0).wait_recv()
    for copy in weights:
        copy.wait()
    activate(0, 1)
    for f in range(3):
        a, b, g = ORDERS[f]
        landed(f, a)
        hop(f, a, b).start()
        hop(f, a, g).start()
        side(f, a).start()
    for f in range(3):
        a, b, g = ORDERS[f]
        landed(f, b)
        hop(f, b, g).start()
        side(f, b).start()
    for f in range(3):
        a, b, g = ORDERS[f]
        landed(f, a ^ b)
        hop(f, a ^ b, g).start()
        side(f, a ^ b).start()
    for f in range(3):
        g = ORDERS[f][2]
        landed(f, g)
        side(f, g).start()
    for f in range(3):
        for slot in (1, 2, 4):
            side(f, slot).wait_recv()

    activate(1, 3)
    for f in range(3):
        a, b, g = ORDERS[f]
        landed(f, a ^ g)
        side(f, a ^ g).start()
        landed(f, b ^ g)
        side(f, b ^ g).start()
    for f in range(3):
        for slot in (3, 5, 6):
            side(f, slot).wait_recv()

    activate(4, 3)
    for f in range(3):
        landed(f, 7)
        side(f, 7).start()
    for f in range(3):
        side(f, 7).wait_recv()
    activate(7, 1)
    for f in range(3):
        for slot in range(8):
            side(f, slot).wait_send()
        for slot in range(1, 8):
            hop(f, 0, slot).wait_send()


def return_kernel(z_hbm, wd_hbm, rel_ref, gate_ref, x_hbm, out_ref, z_ref, wd_ref, x_ref, in_sem, pair_buf, side_buf, near_buf, turn_buf, turn_in, last_buf, last_in, side_send, side_recv, hop_send, hop_recv):
    rows = x_ref.shape[0]
    chunks = pair_buf.shape[0]
    loads = [pltpu.make_async_copy(src, dst, in_sem.at[i]) for i, (src, dst) in enumerate(((z_hbm, z_ref), (wd_hbm, wd_ref), (x_hbm, x_ref)))]
    for copy in loads:
        copy.start()
    me = meet_neighbours()

    def slot_of(f, place):
        a, b, g = ORDERS[f]
        return a * (place // 4) + b * (place // 2 % 2) + g * (place % 2)

    def remote(src, dst, send, recv, bit):
        return pltpu.make_async_remote_copy(src_ref=src, dst_ref=dst, send_sem=send, recv_sem=recv, device_id=(flip(me, bit),), device_id_type=MESH)

    def side(part):
        f, q, s, lo, width = part
        cols = pl.ds(lo, width)
        return remote(side_buf.at[q, :, cols], pair_buf.at[q, 1, :, cols], side_send.at[s], side_recv.at[s], 1)

    def hop_one(part):
        f, q, s, lo, width = part
        cols = pl.ds(lo, width)
        return remote(pair_buf.at[q, :, pl.ds(4 * rows, 4 * rows), cols], near_buf.at[q, :, :, cols], hop_send.at[0, s], hop_recv.at[0, s], 2 * ORDERS[f][0])

    def hop_two(part):
        f, q, s, lo, width = part
        cols = pl.ds(lo, width)
        return remote(turn_buf.at[q, :, :, cols], turn_in.at[q, :, :, cols], hop_send.at[1, s], hop_recv.at[1, s], 2 * ORDERS[f][1])

    def hop_three(part):
        f, q, s, lo, width = part
        cols = pl.ds(lo, width)
        return remote(last_buf.at[q, :, :, cols], last_in.at[q, :, :, cols], hop_send.at[2, s], hop_recv.at[2, s], 2 * ORDERS[f][2])

    def project(part):
        f, q, s, lo, width = part
        w_val = wd_ref[:, pl.ds(pl.multiple_of(q * WIDTH + lo, LANES), width)]
        for place in range(8):
            e_val = jnp.dot(z_ref[seat(slot_of(f, place))], w_val, preferred_element_type=jnp.float32).astype(jnp.bfloat16)
            pair_buf[q, 0, place * rows:(place + 1) * rows, lo:lo + width] = e_val[:rows]
            side_buf[q, place * rows:(place + 1) * rows, lo:lo + width] = e_val[rows:]
        side(part).start()

    def send_far(part):
        side(part).wait_recv()
        hop_one(part).start()

    def choose(part, place, k, other):
        f, q, s, lo, width = part
        rel = rel_ref[seat(slot_of(f, place))][:, k:k + 1]
        at, cols = pl.ds(place * rows, rows), pl.ds(lo, width)
        far = 2 * ORDERS[f][0]
        val = near_buf[q, 1, at, cols].astype(jnp.float32)
        if other is not None:
            val = jnp.where(rel == far + 1, val, other)
        val = jnp.where(rel == far, near_buf[q, 0, at, cols].astype(jnp.float32), val)
        val = jnp.where(rel == 1, pair_buf[q, 1, at, cols].astype(jnp.float32), val)
        return jnp.where(rel == 0, pair_buf[q, 0, at, cols].astype(jnp.float32), val)

    def turn(part):
        f, q, s, lo, width = part
        hop_one(part).wait_recv()
        for k in range(2):
            for half in range(2):
                turn_buf[q, k, half * rows:(half + 1) * rows, lo:lo + width] = choose(part, 2 + half, k, None).astype(jnp.bfloat16)
        hop_two(part).start()

    def last(part):
        f, q, s, lo, width = part
        hop_two(part).wait_recv()
        for k in range(2):
            other = turn_in[q, k, rows:2 * rows, lo:lo + width].astype(jnp.float32)
            last_buf[q, k, :, lo:lo + width] = choose(part, 1, k, other).astype(jnp.bfloat16)
        hop_three(part).start()

    def finish(part):
        f, q, s, lo, width = part
        hop_three(part).wait_recv()
        g_bit = 2 * ORDERS[f][2]
        y_val = None
        for k in range(2):
            rel = rel_ref[0][:, k:k + 1]
            other = jnp.where((rel // g_bit) % 2 == 1, last_in[q, k, :, lo:lo + width].astype(jnp.float32), turn_in[q, k, :rows, lo:lo + width].astype(jnp.float32))
            add = gate_ref[:, k:k + 1] * choose(part, 0, k, other)
            y_val = add if y_val is None else y_val + add
        at = pl.ds(pl.multiple_of(q * WIDTH + lo, LANES), width)
        out_ref[:, at] = (x_ref[:, at].astype(jnp.float32) + y_val).astype(jnp.bfloat16)

    full = chunks // 3
    tail = [(f, chunks - 1, chunks - 1 + f, f * LANES, LANES) for f in range(2)]

    def body(f, j):
        return f, 3 * j + f, 3 * j + f, 0, WIDTH

    def sweep(step):
        @pl.loop(0, full)
        def _(j):
            for f in range(3):
                step(body(f, j))
        for part in tail:
            step(part)

    for copy in loads[:2]:
        copy.wait()
    for f in range(3):
        project(body(f, 0))

    @pl.loop(1, full)
    def _(j):
        for f in range(3):
            project(body(f, j))
            send_far(body(f, j - 1))

    for part in tail:
        project(part)
    for part in [body(f, full - 1) for f in range(3)] + tail:
        send_far(part)
    sweep(turn)
    sweep(last)
    loads[2].wait()
    sweep(finish)

    def drain(part):
        side(part).wait_send()
        hop_one(part).wait_send()
        hop_two(part).wait_send()
        hop_three(part).wait_send()
    sweep(drain)


def gather_and_activate(h_ext, w_gate, w_up):
    rows, d_model = h_ext.shape[0], h_ext.shape[1] - LANES
    d_ff = w_gate.shape[0]
    tiles = (d_model + LANES) // LANES
    cuts = [LANES * ((tiles * f + 2) // 3) for f in range(4)]
    bounds = tuple((cuts[f], cuts[f + 1]) for f in range(3))
    vmem = pl.BlockSpec(memory_space=pltpu.VMEM)
    return pl.pallas_call(
        functools.partial(gather_kernel, bounds),
        name='gather_rows',
        out_shape=(jax.ShapeDtypeStruct((8, 2 * rows, d_ff), jnp.bfloat16), jax.ShapeDtypeStruct((8, rows, LANES), jnp.int32)),
        in_specs=[pl.BlockSpec(memory_space=pltpu.HBM)] * 3,
        out_specs=(vmem, vmem),
        scratch_shapes=[pltpu.VMEM((8, 2 * rows, hi - lo), jnp.bfloat16) for lo, hi in bounds] + [
            pltpu.VMEM(w_gate.shape, jnp.bfloat16), pltpu.VMEM(w_gate.shape, jnp.bfloat16),
            pltpu.SemaphoreType.DMA((5,)),
            pltpu.SemaphoreType.DMA((3, 8)), pltpu.SemaphoreType.DMA((3, 8)),
            pltpu.SemaphoreType.DMA((3, 8)), pltpu.SemaphoreType.DMA((3, 8))],
        compiler_params=pltpu.CompilerParams(collective_id=0, has_side_effects=True, vmem_limit_bytes=60 * 1024 * 1024),
    )(h_ext, w_gate, w_up)


def project_and_return(z_val, w_down, rel, gates, x_mid):
    rows, d_model = x_mid.shape
    chunks = d_model // WIDTH
    hbm = pl.BlockSpec(memory_space=pltpu.HBM)
    vmem = pl.BlockSpec(memory_space=pltpu.VMEM)
    return pl.pallas_call(
        return_kernel,
        name='return_rows',
        out_shape=jax.ShapeDtypeStruct((rows, d_model), jnp.bfloat16),
        in_specs=[hbm, hbm, vmem, vmem, hbm],
        out_specs=vmem,
        scratch_shapes=[
            pltpu.VMEM(z_val.shape, jnp.bfloat16), pltpu.VMEM(w_down.shape, jnp.bfloat16), pltpu.VMEM(x_mid.shape, jnp.bfloat16), pltpu.SemaphoreType.DMA((3,)),
            pltpu.VMEM((chunks, 2, 8 * rows, WIDTH), jnp.bfloat16),
            pltpu.VMEM((chunks, 8 * rows, WIDTH), jnp.bfloat16),
            pltpu.VMEM((chunks, 2, 4 * rows, WIDTH), jnp.bfloat16),
            pltpu.VMEM((chunks, 2, 2 * rows, WIDTH), jnp.bfloat16),
            pltpu.VMEM((chunks, 2, 2 * rows, WIDTH), jnp.bfloat16),
            pltpu.VMEM((chunks, 2, rows, WIDTH), jnp.bfloat16),
            pltpu.VMEM((chunks, 2, rows, WIDTH), jnp.bfloat16),
            pltpu.SemaphoreType.DMA((chunks + 1,)), pltpu.SemaphoreType.DMA((chunks + 1,)),
            pltpu.SemaphoreType.DMA((3, chunks + 1)), pltpu.SemaphoreType.DMA((3, chunks + 1))],
        compiler_params=pltpu.CompilerParams(collective_id=1, has_side_effects=True, vmem_limit_bytes=63 * 1024 * 1024),
    )(z_val, w_down, rel, gates, x_mid)


def solution(mesh):
    def local_step(tokens, k_cache, v_cache, positions, expert_one, expert_two, eligible, ln1_gain, ln1_bias, w_query, b_query, w_key, b_key, w_value, b_value, w_out, b_out, ln2_gain, ln2_bias, w_router, w_gate, w_up, w_down):
        key_new, value_new, x_mid, h_ext, gates = attention_layer(tokens, k_cache, v_cache, positions, expert_one, expert_two, eligible, ln1_gain, ln1_bias, w_query, b_query, w_key, b_key, w_value, b_value, w_out, b_out, ln2_gain, ln2_bias, w_router)
        z_val, rel = gather_and_activate(h_ext, w_gate[0].T, w_up[0].T)
        tokens_out = project_and_return(z_val, w_down[0], rel, gates, x_mid)
        return tokens_out, key_new, value_new

    row_spec = P('ep', None)
    cache_spec = P('ep', None, None, None)
    vec_spec = P('ep')
    rep_one = P(None)
    rep_two = P(None, None)
    expert_spec = P('ep', None, None)
    in_specs = (row_spec, cache_spec, cache_spec, vec_spec, vec_spec, vec_spec, row_spec, rep_one, rep_one, rep_two, rep_one, rep_two, rep_one, rep_two, rep_one, rep_two, rep_one, rep_one, rep_one, rep_two, expert_spec, expert_spec, expert_spec)
    out_specs = (row_spec, expert_spec, expert_spec)
    return jax.shard_map(local_step, mesh=mesh, in_specs=in_specs, out_specs=out_specs, check_vma=False)
```

```python
import functools

import jax
import jax.numpy as jnp
from jax import lax
from jax.experimental import pallas as pl
from jax.experimental.pallas import tpu as pltpu
from jax.sharding import PartitionSpec as P

ROPE_BASE = 10000.0
LN_EPS = 1e-5

MESH = pl.DeviceIdType.MESH
ORDERS = ((1, 2, 4), (2, 4, 1), (4, 1, 2))
LANES = 128
WIDTH = 256
ALONG = (((1,), (1,)), ((), ()))


TILE = 512
HALF = 2048
GROUP = 8
PART = 8
DEPTH = 4
CHUNK = 64


def row_of(ref):
    return jnp.concatenate([ref[i:i + 1, :] for i in range(ref.shape[0])], axis=1).astype(jnp.float32)


def normed(x_f, gain, bias):
    mean_val = jnp.mean(x_f, axis=-1, keepdims=True)
    centered = x_f - mean_val
    var_val = jnp.mean(centered * centered, axis=-1, keepdims=True)
    return centered * lax.rsqrt(var_val + LN_EPS) * gain + bias


def attend_kernel(kv_heads, order_ref, pos_ref, x_ref, g1_ref, c1_ref, g2_ref, c2_ref, bo_ref, bq_ref, bk_ref, bv_ref, cos_ref, sin_ref, elig_ref, one_ref, two_ref, wr_ref, wq_hbm, wk_hbm, wv_hbm, wo_hbm, k_hbm, v_hbm,
                  k_out, v_out, x_out, h_out, gate_out, w_buf, k_buf, v_buf, q_all, kn_all, vn_all, o_all, new_all, h_buf, where_ref, w_sem, o_sem, kv_sem):
    rows, d_model = x_ref.shape
    heads = q_all.shape[1]
    share = heads // kv_heads
    groups = rows // GROUP
    spans = k_hbm.shape[1] // (CHUNK * kv_heads)
    q_tiles = wq_hbm.shape[1] // TILE
    scale = LANES ** -0.5

    def weights(w_hbm, tile, slot):
        return [pltpu.make_async_copy(w_hbm.at[pl.ds(half * HALF, HALF), pl.ds(tile * TILE, TILE)], w_buf.at[slot + half], w_sem.at[slot + half]) for half in range(2)]

    loads = [weights(wq_hbm, i, 2 * i) for i in range(q_tiles)] + [weights(wk_hbm, 0, 2 * q_tiles), weights(wv_hbm, 0, 2 * q_tiles + 2)]
    for pair in loads:
        for copy in pair:
            copy.start()

    def copies(g, n):
        slot = lax.rem(g, DEPTH)
        size = n * CHUNK * kv_heads
        for j in range(GROUP):
            t = order_ref[g * GROUP + j]
            yield pltpu.make_async_copy(k_hbm.at[t, pl.ds(0, size)], k_buf.at[slot, j, pl.ds(0, size)], kv_sem.at[slot, 0])
            yield pltpu.make_async_copy(v_hbm.at[t, pl.ds(0, size)], v_buf.at[slot, j, pl.ds(0, size)], kv_sem.at[slot, 1])

    def each_span(g, body):
        span = jnp.clip(lax.div(pos_ref[g * GROUP] + (CHUNK - 1), CHUNK), 1, spans)
        for n in range(1, spans + 1):
            @pl.when(span == n)
            def _(n=n):
                body(n)

    def fetch(g):
        def body(n):
            for copy in copies(g, n):
                copy.start()
        each_span(g, body)

    for g in range(DEPTH - 1):
        fetch(jnp.int32(g))

    col = lax.broadcasted_iota(jnp.int32, where_ref.shape, 1)
    row = lax.broadcasted_iota(jnp.int32, where_ref.shape, 0)
    where_ref[...] = jnp.where(col % kv_heads == (row // share) % kv_heads, col // kv_heads, 1 << 20)
    h_buf[...] = normed(x_ref[...].astype(jnp.float32), row_of(g1_ref), row_of(c1_ref)).astype(jnp.bfloat16)

    def product(index, bias):
        slot = 2 * index
        for copy in loads[index]:
            copy.wait()
        lin = jnp.dot(h_buf[:, :HALF], w_buf[slot], preferred_element_type=jnp.float32) + jnp.dot(h_buf[:, HALF:], w_buf[slot + 1], preferred_element_type=jnp.float32)
        return lin + bias

    def turned(head):
        return (head * cos_ref[...] + pltpu.roll(head, LANES // 2, 1) * sin_ref[...]).astype(jnp.bfloat16)

    bq_row = row_of(bq_ref)
    for i in range(q_tiles):
        lin = product(i, bq_row[:, i * TILE:(i + 1) * TILE])
        for n in range(TILE // LANES):
            q_all[:, i * (TILE // LANES) + n, :] = turned(lin[:, n * LANES:(n + 1) * LANES]).astype(jnp.float32)
    lin = product(q_tiles, row_of(bk_ref))
    for n in range(kv_heads):
        val = turned(lin[:, n * LANES:(n + 1) * LANES])
        new_all[:, n, :] = val.astype(jnp.float32)
        for m in range(share):
            kn_all[:, n * share + m, :] = val.astype(jnp.float32)
    k_out[...] = new_all[...].astype(jnp.bfloat16)
    lin = product(q_tiles + 1, row_of(bv_ref))
    for n in range(kv_heads):
        val = lin[:, n * LANES:(n + 1) * LANES].astype(jnp.bfloat16)
        new_all[:, n, :] = val.astype(jnp.float32)
        for m in range(share):
            vn_all[:, n * share + m, :] = val.astype(jnp.float32)

    v_out[...] = new_all[...].astype(jnp.bfloat16)

    def out_weights(tile):
        return pltpu.make_async_copy(wo_hbm.at[:, pl.ds(pl.multiple_of(tile * TILE, TILE), TILE)], w_buf.at[tile], o_sem.at[tile])

    stride = groups // (d_model // TILE)

    block = lax.broadcasted_iota(jnp.int32, (PART * heads, 1), 0) // heads

    @pl.loop(0, groups)
    def _(g):
        @pl.when(g + DEPTH - 1 < groups)
        def _():
            fetch(g + DEPTH - 1)

        @pl.when(lax.rem(g, stride) == 0)
        def _():
            out_weights(lax.div(g, stride)).start()

        slot = lax.rem(g, DEPTH)

        def body(n):
            size = n * CHUNK * kv_heads
            for copy in copies(g, n):
                copy.wait()
            for lo in range(0, GROUP, PART):
                toks = [order_ref[g * GROUP + lo + j] for j in range(PART)]
                q_rows = [q_all[t] for t in toks]
                s_val = jnp.concatenate([lax.dot_general(q_rows[j].astype(jnp.bfloat16), k_buf[slot, lo + j, :size], ALONG, preferred_element_type=jnp.float32) for j in range(PART)], axis=0) * scale
                q_val = jnp.concatenate(q_rows, axis=0)
                kn_val = jnp.concatenate([kn_all[t] for t in toks], axis=0)
                vn_val = jnp.concatenate([vn_all[t] for t in toks], axis=0)
                s_new = jnp.sum(q_val * kn_val, axis=1, keepdims=True) * scale
                pos = jnp.zeros((PART * heads, 1), jnp.int32)
                for j in range(PART):
                    pos = jnp.where(block == j, pos_ref[g * GROUP + lo + j], pos)
                s_val = jnp.where(where_ref[:, :size] < pos, s_val, -jnp.inf)
                top = jnp.maximum(jnp.max(s_val, axis=1, keepdims=True), s_new)
                e_val, e_new = jnp.exp(s_val - top), jnp.exp(s_new - top)
                inv = 1.0 / (jnp.sum(e_val, axis=1, keepdims=True) + e_new)
                p_val = (e_val * inv).astype(jnp.bfloat16)
                p_new = (e_new * inv).astype(jnp.bfloat16).astype(jnp.float32)
                a_val = jnp.concatenate([jnp.dot(p_val[j * heads:(j + 1) * heads], v_buf[slot, lo + j, :size], preferred_element_type=jnp.float32) for j in range(PART)], axis=0)
                a_val = (a_val + p_new * vn_val).astype(jnp.bfloat16).astype(jnp.float32)
                for j in range(PART):
                    o_all[toks[j]] = a_val[j * heads:(j + 1) * heads]
        each_span(g, body)

    for n in range(heads):
        h_buf[:, n * LANES:(n + 1) * LANES] = o_all[:, n, :].astype(jnp.bfloat16)

    bo_row = row_of(bo_ref)
    for tile in range(d_model // TILE):
        out_weights(jnp.int32(tile)).wait()
        at = slice(tile * TILE, (tile + 1) * TILE)
        acc = jnp.dot(h_buf[:, :heads * LANES], w_buf[tile], preferred_element_type=jnp.float32)
        x_out[:, at] = (x_ref[:, at].astype(jnp.float32) + acc + bo_row[:, at]).astype(jnp.bfloat16)

    h_two = normed(x_out[...].astype(jnp.float32), row_of(g2_ref), row_of(c2_ref)).astype(jnp.bfloat16)
    h_out[:, :d_model] = h_two
    logits = lax.dot_general(h_two, wr_ref[...], ALONG, preferred_element_type=jnp.float32)
    experts = logits.shape[1]
    expert_ids = lax.broadcasted_iota(jnp.int32, logits.shape, 1)
    stacked = jnp.concatenate([elig_ref[...], one_ref[...], two_ref[...], jnp.zeros((rows - experts - 2, rows), jnp.int32)], axis=0)
    meta = stacked.astype(jnp.float32).T.astype(jnp.int32)
    pick_one, pick_two = meta[:, experts:experts + 1], meta[:, experts + 1:experts + 2]
    hit_one, hit_two = expert_ids == pick_one, expert_ids == pick_two
    keep_one = meta[:, :experts] == 1

    def gate(keep, hit):
        val = jnp.where(keep, logits, -jnp.inf)
        e_val = jnp.exp(val - jnp.max(val, axis=1, keepdims=True))
        return jnp.sum(jnp.where(hit, e_val, 0.0), axis=1, keepdims=True) / jnp.sum(e_val, axis=1, keepdims=True)

    lane = lax.broadcasted_iota(jnp.int32, gate_out.shape, 1)
    gate_out[...] = jnp.where(lane == 0, gate(keep_one, hit_one), gate(keep_one & jnp.logical_not(hit_one), hit_two))
    ids = jnp.where(lane == 0, pick_one, jnp.where(lane == 1, pick_two, 0))
    h_out[:, d_model:] = ids.astype(jnp.float32).astype(jnp.bfloat16)


def attention_layer(tokens, k_cache, v_cache, positions, expert_one, expert_two, eligible, ln1_gain, ln1_bias, w_query, b_query, w_key, b_key, w_value, b_value, w_out, b_out, ln2_gain, ln2_bias, w_router):
    rows, seq_len, kv_heads, head_dim = k_cache.shape
    d_model = tokens.shape[1]
    heads = w_query.shape[1] // head_dim
    kv_dim = kv_heads * head_dim
    ids = jnp.arange(rows, dtype=jnp.int32)
    ahead = (positions[None, :] > positions[:, None]) | ((positions[None, :] == positions[:, None]) & (ids[None, :] < ids[:, None]))
    rank = jnp.sum(ahead.astype(jnp.int32), axis=1)
    hit = rank[None, :] == ids[:, None]
    order = jnp.sum(jnp.where(hit, ids[None, :], 0), axis=1)
    pos_sorted = jnp.sum(jnp.where(hit, positions[None, :], 0), axis=1)
    half_dim = head_dim // 2
    inv_freq = ROPE_BASE ** (jnp.arange(half_dim, dtype=jnp.float32) * (-2.0 / head_dim))
    angles = positions.astype(jnp.float32)[:, None] * jnp.concatenate([inv_freq, inv_freq])[None, :]
    sign = jnp.where(jnp.arange(head_dim) < half_dim, -1.0, 1.0).astype(jnp.float32)
    small = [p.reshape(-1, LANES) for p in (ln1_gain, ln1_bias, ln2_gain, ln2_bias, b_out, b_query, b_key, b_value)]
    vmem = pl.BlockSpec(memory_space=pltpu.VMEM)
    smem = pl.BlockSpec(memory_space=pltpu.SMEM)
    hbm = pl.BlockSpec(memory_space=pl.ANY)
    flat = (rows, seq_len * kv_heads, head_dim)
    spread = pltpu.VMEM((rows, heads, head_dim), jnp.float32)
    return pl.pallas_call(
        functools.partial(attend_kernel, kv_heads),
        name='attention_layer',
        out_shape=(jax.ShapeDtypeStruct((rows, kv_heads, head_dim), jnp.bfloat16), jax.ShapeDtypeStruct((rows, kv_heads, head_dim), jnp.bfloat16),
                   jax.ShapeDtypeStruct((rows, d_model), jnp.bfloat16), jax.ShapeDtypeStruct((rows, d_model + LANES), jnp.bfloat16),
                   jax.ShapeDtypeStruct((rows, LANES), jnp.float32)),
        in_specs=[smem, smem] + [vmem] * 15 + [hbm, hbm, hbm, hbm, hbm, hbm],
        out_specs=(vmem,) * 5,
        scratch_shapes=[
            pltpu.VMEM((2 * (heads * head_dim + 2 * kv_dim) // TILE, HALF, TILE), jnp.bfloat16),
            pltpu.VMEM((DEPTH, GROUP) + flat[1:], jnp.bfloat16), pltpu.VMEM((DEPTH, GROUP) + flat[1:], jnp.bfloat16),
            spread, spread, spread, spread,
            pltpu.VMEM((rows, kv_heads, head_dim), jnp.float32),
            pltpu.VMEM((rows, d_model), jnp.bfloat16),
            pltpu.VMEM((PART * heads, flat[1]), jnp.int32),
            pltpu.SemaphoreType.DMA((2 * (heads * head_dim + 2 * kv_dim) // TILE,)),
            pltpu.SemaphoreType.DMA((d_model // TILE,)),
            pltpu.SemaphoreType.DMA((DEPTH, 2))],
        compiler_params=pltpu.CompilerParams(vmem_limit_bytes=62 * 1024 * 1024),
    )(order, pos_sorted, tokens, *small, jnp.cos(angles), jnp.sin(angles) * sign[None, :], eligible.T, expert_one[None], expert_two[None], w_router.T, w_query, w_key, w_value, w_out, k_cache.reshape(flat), v_cache.reshape(flat))


def seat(slot):
    return {3: 4, 4: 3}.get(slot, slot)


def flip(me, bit):
    return me + bit - 2 * bit * ((me // bit) % 2)


def meet_neighbours():
    me = lax.axis_index('ep')
    barrier = pltpu.get_barrier_semaphore()
    for bit in (1, 2, 4, 8):
        pl.semaphore_signal(barrier, inc=1, device_id=(flip(me, bit),), device_id_type=MESH)
    pl.semaphore_wait(barrier, 4)
    return me


def gather_kernel(bounds, h_ref, wg_hbm, wu_hbm, z_ref, rel_ref, x_a, x_b, x_c, wg_ref, wu_ref, own_sem, send_sem, recv_sem, side_send, side_recv):
    rows = x_a.shape[1] // 2
    bufs = (x_a, x_b, x_c)
    copies = []
    for f in range(3):
        lo, hi = bounds[f]
        copies.append(pltpu.make_async_copy(h_ref.at[:, pl.ds(lo, hi - lo)], bufs[f].at[0, pl.ds(0, rows)], own_sem.at[f]))
        copies[-1].start()
    me = meet_neighbours()

    def hop(f, src, bit):
        return pltpu.make_async_remote_copy(
            src_ref=bufs[f].at[seat(src), pl.ds(0, rows)], dst_ref=bufs[f].at[seat(src ^ bit), pl.ds(0, rows)],
            send_sem=send_sem.at[f, src ^ bit], recv_sem=recv_sem.at[f, src ^ bit],
            device_id=(flip(me, 2 * bit),), device_id_type=MESH)

    def side(f, src):
        return pltpu.make_async_remote_copy(
            src_ref=bufs[f].at[seat(src), pl.ds(0, rows)], dst_ref=bufs[f].at[seat(src), pl.ds(rows, rows)],
            send_sem=side_send.at[f, src], recv_sem=side_recv.at[f, src],
            device_id=(flip(me, 1),), device_id_type=MESH)

    def landed(f, slot):
        hop(f, 0, slot).wait_recv()

    def activate(place):
        u_val = v_val = None
        for f in range(3):
            lo, hi = bounds[f]
            hi = min(hi, wg_ref.shape[1])
            x_val = bufs[f][place, :, : hi - lo]
            u_part = lax.dot_general(x_val, wg_ref[:, lo:hi], ALONG, preferred_element_type=jnp.float32)
            v_part = lax.dot_general(x_val, wu_ref[:, lo:hi], ALONG, preferred_element_type=jnp.float32)
            u_val = u_part if u_val is None else u_val + u_part
            v_val = v_part if v_val is None else v_val + v_part
        z_ref[place] = (jax.nn.silu(u_val) * v_val).astype(jnp.bfloat16)
        ids = bufs[2][place, :rows, bounds[2][1] - bounds[2][0] - LANES:]
        rel_ref[place] = ids.astype(jnp.float32).astype(jnp.int32) ^ me

    for f in range(3):
        copies[f].wait()
        hop(f, 0, ORDERS[f][0]).start()
    weights = [pltpu.make_async_copy(src, dst, own_sem.at[3 + i]) for i, (src, dst) in enumerate(((wg_hbm, wg_ref), (wu_hbm, wu_ref)))]
    for f in range(3):
        side(f, 0).start()
    for copy in weights:
        copy.start()
    for stage in (1, 2):
        for f in range(3):
            hop(f, 0, ORDERS[f][stage]).start()
    for f in range(3):
        side(f, 0).wait_recv()
    for copy in weights:
        copy.wait()
    activate(0)
    for f in range(3):
        a, b, g = ORDERS[f]
        landed(f, a)
        hop(f, a, b).start()
        hop(f, a, g).start()
        side(f, a).start()
    for f in range(3):
        a, b, g = ORDERS[f]
        landed(f, b)
        hop(f, b, g).start()
        side(f, b).start()
    for f in range(3):
        a, b, g = ORDERS[f]
        landed(f, a ^ b)
        hop(f, a ^ b, g).start()
        side(f, a ^ b).start()
    for f in range(3):
        g = ORDERS[f][2]
        landed(f, g)
        side(f, g).start()
    for f in range(3):
        for slot in (1, 2, 4):
            side(f, slot).wait_recv()

    pl.loop(1, 4)(activate)
    for f in range(3):
        a, b, g = ORDERS[f]
        landed(f, a ^ g)
        side(f, a ^ g).start()
        landed(f, b ^ g)
        side(f, b ^ g).start()
    for f in range(3):
        for slot in (3, 5, 6):
            side(f, slot).wait_recv()

    pl.loop(4, 7)(activate)
    for f in range(3):
        landed(f, 7)
        side(f, 7).start()
    for f in range(3):
        side(f, 7).wait_recv()
    activate(7)
    for f in range(3):
        for slot in range(8):
            side(f, slot).wait_send()
        for slot in range(1, 8):
            hop(f, 0, slot).wait_send()


def return_kernel(z_hbm, wd_hbm, rel_ref, gate_ref, x_hbm, out_ref, z_ref, wd_ref, x_ref, in_sem, pair_buf, side_buf, near_buf, turn_buf, turn_in, last_buf, last_in, side_send, side_recv, hop_send, hop_recv):
    rows = x_ref.shape[0]
    chunks = pair_buf.shape[0]
    loads = [pltpu.make_async_copy(src, dst, in_sem.at[i]) for i, (src, dst) in enumerate(((z_hbm, z_ref), (wd_hbm, wd_ref), (x_hbm, x_ref)))]
    for copy in loads:
        copy.start()
    me = meet_neighbours()

    def slot_of(f, place):
        a, b, g = ORDERS[f]
        return a * (place // 4) + b * (place // 2 % 2) + g * (place % 2)

    def remote(src, dst, send, recv, bit):
        return pltpu.make_async_remote_copy(src_ref=src, dst_ref=dst, send_sem=send, recv_sem=recv, device_id=(flip(me, bit),), device_id_type=MESH)

    def side(part):
        f, q, s, lo, width = part
        cols = pl.ds(lo, width)
        return remote(side_buf.at[q, :, cols], pair_buf.at[q, 1, :, cols], side_send.at[s], side_recv.at[s], 1)

    def hop_one(part):
        f, q, s, lo, width = part
        cols = pl.ds(lo, width)
        return remote(pair_buf.at[q, :, pl.ds(4 * rows, 4 * rows), cols], near_buf.at[q, :, :, cols], hop_send.at[0, s], hop_recv.at[0, s], 2 * ORDERS[f][0])

    def hop_two(part):
        f, q, s, lo, width = part
        cols = pl.ds(lo, width)
        return remote(turn_buf.at[q, :, :, cols], turn_in.at[q, :, :, cols], hop_send.at[1, s], hop_recv.at[1, s], 2 * ORDERS[f][1])

    def hop_three(part):
        f, q, s, lo, width = part
        cols = pl.ds(lo, width)
        return remote(last_buf.at[q, :, :, cols], last_in.at[q, :, :, cols], hop_send.at[2, s], hop_recv.at[2, s], 2 * ORDERS[f][2])

    def project(part):
        f, q, s, lo, width = part
        w_val = wd_ref[:, pl.ds(pl.multiple_of(q * WIDTH + lo, LANES), width)]
        for place in range(8):
            e_val = jnp.dot(z_ref[seat(slot_of(f, place))], w_val, preferred_element_type=jnp.float32).astype(jnp.bfloat16)
            pair_buf[q, 0, place * rows:(place + 1) * rows, lo:lo + width] = e_val[:rows]
            side_buf[q, place * rows:(place + 1) * rows, lo:lo + width] = e_val[rows:]
        side(part).start()

    def send_far(part):
        side(part).wait_recv()
        hop_one(part).start()

    def choose(part, place, k, other):
        f, q, s, lo, width = part
        rel = rel_ref[seat(slot_of(f, place))][:, k:k + 1]
        at, cols = pl.ds(place * rows, rows), pl.ds(lo, width)
        far = 2 * ORDERS[f][0]
        val = near_buf[q, 1, at, cols].astype(jnp.float32)
        if other is not None:
            val = jnp.where(rel == far + 1, val, other)
        val = jnp.where(rel == far, near_buf[q, 0, at, cols].astype(jnp.float32), val)
        val = jnp.where(rel == 1, pair_buf[q, 1, at, cols].astype(jnp.float32), val)
        return jnp.where(rel == 0, pair_buf[q, 0, at, cols].astype(jnp.float32), val)

    def turn(part):
        f, q, s, lo, width = part
        hop_one(part).wait_recv()
        for k in range(2):
            for half in range(2):
                turn_buf[q, k, half * rows:(half + 1) * rows, lo:lo + width] = choose(part, 2 + half, k, None).astype(jnp.bfloat16)
        hop_two(part).start()

    def last(part):
        f, q, s, lo, width = part
        hop_two(part).wait_recv()
        for k in range(2):
            other = turn_in[q, k, rows:2 * rows, lo:lo + width].astype(jnp.float32)
            last_buf[q, k, :, lo:lo + width] = choose(part, 1, k, other).astype(jnp.bfloat16)
        hop_three(part).start()

    def finish(part):
        f, q, s, lo, width = part
        hop_three(part).wait_recv()
        g_bit = 2 * ORDERS[f][2]
        y_val = None
        for k in range(2):
            rel = rel_ref[0][:, k:k + 1]
            other = jnp.where((rel // g_bit) % 2 == 1, last_in[q, k, :, lo:lo + width].astype(jnp.float32), turn_in[q, k, :rows, lo:lo + width].astype(jnp.float32))
            add = gate_ref[:, k:k + 1] * choose(part, 0, k, other)
            y_val = add if y_val is None else y_val + add
        at = pl.ds(pl.multiple_of(q * WIDTH + lo, LANES), width)
        out_ref[:, at] = (x_ref[:, at].astype(jnp.float32) + y_val).astype(jnp.bfloat16)

    full = chunks // 3
    tail = [(f, chunks - 1, chunks - 1 + f, f * LANES, LANES) for f in range(2)]

    def body(f, j):
        return f, 3 * j + f, 3 * j + f, 0, WIDTH

    def sweep(step):
        @pl.loop(0, full)
        def _(j):
            for f in range(3):
                step(body(f, j))
        for part in tail:
            step(part)

    for copy in loads[:2]:
        copy.wait()
    for f in range(3):
        project(body(f, 0))

    @pl.loop(1, full)
    def _(j):
        for f in range(3):
            project(body(f, j))
            send_far(body(f, j - 1))

    for part in tail:
        project(part)
    for part in [body(f, full - 1) for f in range(3)] + tail:
        send_far(part)
    sweep(turn)
    sweep(last)
    loads[2].wait()
    sweep(finish)

    def drain(part):
        side(part).wait_send()
        hop_one(part).wait_send()
        hop_two(part).wait_send()
        hop_three(part).wait_send()
    sweep(drain)


def gather_and_activate(h_ext, w_gate, w_up):
    rows, d_model = h_ext.shape[0], h_ext.shape[1] - LANES
    d_ff = w_gate.shape[0]
    tiles = (d_model + LANES) // LANES
    cuts = [LANES * ((tiles * f + 2) // 3) for f in range(4)]
    bounds = tuple((cuts[f], cuts[f + 1]) for f in range(3))
    vmem = pl.BlockSpec(memory_space=pltpu.VMEM)
    return pl.pallas_call(
        functools.partial(gather_kernel, bounds),
        name='gather_rows',
        out_shape=(jax.ShapeDtypeStruct((8, 2 * rows, d_ff), jnp.bfloat16), jax.ShapeDtypeStruct((8, rows, LANES), jnp.int32)),
        in_specs=[pl.BlockSpec(memory_space=pltpu.HBM)] * 3,
        out_specs=(vmem, vmem),
        scratch_shapes=[pltpu.VMEM((8, 2 * rows, hi - lo), jnp.bfloat16) for lo, hi in bounds] + [
            pltpu.VMEM(w_gate.shape, jnp.bfloat16), pltpu.VMEM(w_gate.shape, jnp.bfloat16),
            pltpu.SemaphoreType.DMA((5,)),
            pltpu.SemaphoreType.DMA((3, 8)), pltpu.SemaphoreType.DMA((3, 8)),
            pltpu.SemaphoreType.DMA((3, 8)), pltpu.SemaphoreType.DMA((3, 8))],
        compiler_params=pltpu.CompilerParams(collective_id=0, has_side_effects=True, vmem_limit_bytes=60 * 1024 * 1024),
    )(h_ext, w_gate, w_up)


def project_and_return(z_val, w_down, rel, gates, x_mid):
    rows, d_model = x_mid.shape
    chunks = d_model // WIDTH
    hbm = pl.BlockSpec(memory_space=pltpu.HBM)
    vmem = pl.BlockSpec(memory_space=pltpu.VMEM)
    return pl.pallas_call(
        return_kernel,
        name='return_rows',
        out_shape=jax.ShapeDtypeStruct((rows, d_model), jnp.bfloat16),
        in_specs=[hbm, hbm, vmem, vmem, hbm],
        out_specs=vmem,
        scratch_shapes=[
            pltpu.VMEM(z_val.shape, jnp.bfloat16), pltpu.VMEM(w_down.shape, jnp.bfloat16), pltpu.VMEM(x_mid.shape, jnp.bfloat16), pltpu.SemaphoreType.DMA((3,)),
            pltpu.VMEM((chunks, 2, 8 * rows, WIDTH), jnp.bfloat16),
            pltpu.VMEM((chunks, 8 * rows, WIDTH), jnp.bfloat16),
            pltpu.VMEM((chunks, 2, 4 * rows, WIDTH), jnp.bfloat16),
            pltpu.VMEM((chunks, 2, 2 * rows, WIDTH), jnp.bfloat16),
            pltpu.VMEM((chunks, 2, 2 * rows, WIDTH), jnp.bfloat16),
            pltpu.VMEM((chunks, 2, rows, WIDTH), jnp.bfloat16),
            pltpu.VMEM((chunks, 2, rows, WIDTH), jnp.bfloat16),
            pltpu.SemaphoreType.DMA((chunks + 1,)), pltpu.SemaphoreType.DMA((chunks + 1,)),
            pltpu.SemaphoreType.DMA((3, chunks + 1)), pltpu.SemaphoreType.DMA((3, chunks + 1))],
        compiler_params=pltpu.CompilerParams(collective_id=1, has_side_effects=True, vmem_limit_bytes=63 * 1024 * 1024),
    )(z_val, w_down, rel, gates, x_mid)


def solution(mesh):
    def local_step(tokens, k_cache, v_cache, positions, expert_one, expert_two, eligible, ln1_gain, ln1_bias, w_query, b_query, w_key, b_key, w_value, b_value, w_out, b_out, ln2_gain, ln2_bias, w_router, w_gate, w_up, w_down):
        key_new, value_new, x_mid, h_ext, gates = attention_layer(tokens, k_cache, v_cache, positions, expert_one, expert_two, eligible, ln1_gain, ln1_bias, w_query, b_query, w_key, b_key, w_value, b_value, w_out, b_out, ln2_gain, ln2_bias, w_router)
        z_val, rel = gather_and_activate(h_ext, w_gate[0].T, w_up[0].T)
        tokens_out = project_and_return(z_val, w_down[0], rel, gates, x_mid)
        return tokens_out, key_new, value_new

    row_spec = P('ep', None)
    cache_spec = P('ep', None, None, None)
    vec_spec = P('ep')
    rep_one = P(None)
    rep_two = P(None, None)
    expert_spec = P('ep', None, None)
    in_specs = (row_spec, cache_spec, cache_spec, vec_spec, vec_spec, vec_spec, row_spec, rep_one, rep_one, rep_two, rep_one, rep_two, rep_one, rep_two, rep_one, rep_two, rep_one, rep_one, rep_one, rep_two, expert_spec, expert_spec, expert_spec)
    out_specs = (row_spec, expert_spec, expert_spec)
    return jax.shard_map(local_step, mesh=mesh, in_specs=in_specs, out_specs=out_specs, check_vma=False)
```

```python
import functools

import jax
import jax.numpy as jnp
from jax import lax
from jax.experimental import pallas as pl
from jax.experimental.pallas import tpu as pltpu
from jax.sharding import PartitionSpec as P

ROPE_BASE = 10000.0
LN_EPS = 1e-5

MESH = pl.DeviceIdType.MESH
ORDERS = ((1, 2, 4), (2, 4, 1), (4, 1, 2))
LANES = 128
WIDTH = 256
ALONG = (((1,), (1,)), ((), ()))


TILE = 512
HALF = 2048
GROUP = 8
PART = 8
DEPTH = 4
CHUNK = 64


def row_of(ref):
    return jnp.concatenate([ref[i:i + 1, :] for i in range(ref.shape[0])], axis=1).astype(jnp.float32)


def normed(x_f, gain, bias):
    mean_val = jnp.mean(x_f, axis=-1, keepdims=True)
    centered = x_f - mean_val
    var_val = jnp.mean(centered * centered, axis=-1, keepdims=True)
    return centered * lax.rsqrt(var_val + LN_EPS) * gain + bias


def attend_kernel(kv_heads, order_ref, pos_ref, x_ref, g1_ref, c1_ref, g2_ref, c2_ref, bo_ref, bq_ref, bk_ref, bv_ref, cos_ref, sin_ref, elig_ref, one_ref, two_ref, wr_ref, wq_hbm, wk_hbm, wv_hbm, wo_hbm, k_hbm, v_hbm,
                  k_out, v_out, x_out, h_out, gate_out, w_buf, k_buf, v_buf, q_all, kn_all, vn_all, o_all, new_all, h_buf, where_ref, w_sem, o_sem, kv_sem):
    rows, d_model = x_ref.shape
    heads = q_all.shape[1]
    share = heads // kv_heads
    groups = rows // GROUP
    spans = k_hbm.shape[1] // (CHUNK * kv_heads)
    q_tiles = wq_hbm.shape[1] // TILE
    scale = LANES ** -0.5

    def weights(w_hbm, tile, slot):
        return [pltpu.make_async_copy(w_hbm.at[pl.ds(half * HALF, HALF), pl.ds(tile * TILE, TILE)], w_buf.at[slot + half], w_sem.at[slot + half]) for half in range(2)]

    loads = [weights(wq_hbm, i, 2 * i) for i in range(q_tiles)] + [weights(wk_hbm, 0, 2 * q_tiles), weights(wv_hbm, 0, 2 * q_tiles + 2)]
    for pair in loads:
        for copy in pair:
            copy.start()

    def copies(g, n):
        slot = lax.rem(g, DEPTH)
        size = n * CHUNK * kv_heads
        for j in range(GROUP):
            t = order_ref[g * GROUP + j]
            yield pltpu.make_async_copy(k_hbm.at[t, pl.ds(0, size)], k_buf.at[slot, j, pl.ds(0, size)], kv_sem.at[slot, 0])
            yield pltpu.make_async_copy(v_hbm.at[t, pl.ds(0, size)], v_buf.at[slot, j, pl.ds(0, size)], kv_sem.at[slot, 1])

    def each_span(g, body):
        span = jnp.clip(lax.div(pos_ref[g * GROUP] + (CHUNK - 1), CHUNK), 1, spans)
        for n in range(1, spans + 1):
            @pl.when(span == n)
            def _(n=n):
                body(n)

    def fetch(g):
        def body(n):
            for copy in copies(g, n):
                copy.start()
        each_span(g, body)

    for g in range(DEPTH - 1):
        fetch(jnp.int32(g))

    col = lax.broadcasted_iota(jnp.int32, where_ref.shape, 1)
    row = lax.broadcasted_iota(jnp.int32, where_ref.shape, 0)
    where_ref[...] = jnp.where(col % kv_heads == (row // share) % kv_heads, col // kv_heads, 1 << 20)
    h_buf[...] = normed(x_ref[...].astype(jnp.float32), row_of(g1_ref), row_of(c1_ref)).astype(jnp.bfloat16)

    def product(index, bias):
        slot = 2 * index
        for copy in loads[index]:
            copy.wait()
        lin = jnp.dot(h_buf[:, :HALF], w_buf[slot], preferred_element_type=jnp.float32) + jnp.dot(h_buf[:, HALF:], w_buf[slot + 1], preferred_element_type=jnp.float32)
        return lin + bias

    def turned(head):
        return (head * cos_ref[...] + pltpu.roll(head, LANES // 2, 1) * sin_ref[...]).astype(jnp.bfloat16)

    bq_row = row_of(bq_ref)
    for i in range(q_tiles):
        lin = product(i, bq_row[:, i * TILE:(i + 1) * TILE])
        for n in range(TILE // LANES):
            q_all[:, i * (TILE // LANES) + n, :] = turned(lin[:, n * LANES:(n + 1) * LANES]).astype(jnp.float32)
    lin = product(q_tiles, row_of(bk_ref))
    for n in range(kv_heads):
        val = turned(lin[:, n * LANES:(n + 1) * LANES])
        new_all[:, n, :] = val.astype(jnp.float32)
        for m in range(share):
            kn_all[:, n * share + m, :] = val.astype(jnp.float32)
    k_out[...] = new_all[...].astype(jnp.bfloat16)
    lin = product(q_tiles + 1, row_of(bv_ref))
    for n in range(kv_heads):
        val = lin[:, n * LANES:(n + 1) * LANES].astype(jnp.bfloat16)
        new_all[:, n, :] = val.astype(jnp.float32)
        for m in range(share):
            vn_all[:, n * share + m, :] = val.astype(jnp.float32)

    v_out[...] = new_all[...].astype(jnp.bfloat16)

    def out_weights(tile):
        return pltpu.make_async_copy(wo_hbm.at[:, pl.ds(pl.multiple_of(tile * TILE, TILE), TILE)], w_buf.at[tile], o_sem.at[tile])

    stride = groups // (d_model // TILE)

    block = lax.broadcasted_iota(jnp.int32, (PART * heads, 1), 0) // heads

    @pl.loop(0, groups)
    def _(g):
        @pl.when(g + DEPTH - 1 < groups)
        def _():
            fetch(g + DEPTH - 1)

        @pl.when(lax.rem(g, stride) == 0)
        def _():
            out_weights(lax.div(g, stride)).start()

        slot = lax.rem(g, DEPTH)

        def body(n):
            size = n * CHUNK * kv_heads
            for copy in copies(g, n):
                copy.wait()
            for lo in range(0, GROUP, PART):
                toks = [order_ref[g * GROUP + lo + j] for j in range(PART)]
                q_rows = [q_all[t] for t in toks]
                s_val = jnp.concatenate([lax.dot_general(q_rows[j].astype(jnp.bfloat16), k_buf[slot, lo + j, :size], ALONG, preferred_element_type=jnp.float32) for j in range(PART)], axis=0) * scale
                q_val = jnp.concatenate(q_rows, axis=0)
                kn_val = jnp.concatenate([kn_all[t] for t in toks], axis=0)
                vn_val = jnp.concatenate([vn_all[t] for t in toks], axis=0)
                s_new = jnp.sum(q_val * kn_val, axis=1, keepdims=True) * scale
                pos = jnp.zeros((PART * heads, 1), jnp.int32)
                for j in range(PART):
                    pos = jnp.where(block == j, pos_ref[g * GROUP + lo + j], pos)
                s_val = jnp.where(where_ref[:, :size] < pos, s_val, -jnp.inf)
                top = jnp.maximum(jnp.max(s_val, axis=1, keepdims=True), s_new)
                e_val, e_new = jnp.exp(s_val - top), jnp.exp(s_new - top)
                inv = 1.0 / (jnp.sum(e_val, axis=1, keepdims=True) + e_new)
                p_val = (e_val * inv).astype(jnp.bfloat16)
                p_new = (e_new * inv).astype(jnp.bfloat16).astype(jnp.float32)
                a_val = jnp.concatenate([jnp.dot(p_val[j * heads:(j + 1) * heads], v_buf[slot, lo + j, :size], preferred_element_type=jnp.float32) for j in range(PART)], axis=0)
                a_val = (a_val + p_new * vn_val).astype(jnp.bfloat16).astype(jnp.float32)
                for j in range(PART):
                    o_all[toks[j]] = a_val[j * heads:(j + 1) * heads]
        each_span(g, body)

    for n in range(heads):
        h_buf[:, n * LANES:(n + 1) * LANES] = o_all[:, n, :].astype(jnp.bfloat16)

    bo_row = row_of(bo_ref)
    for tile in range(d_model // TILE):
        out_weights(jnp.int32(tile)).wait()
        at = slice(tile * TILE, (tile + 1) * TILE)
        acc = jnp.dot(h_buf[:, :heads * LANES], w_buf[tile], preferred_element_type=jnp.float32)
        x_out[:, at] = (x_ref[:, at].astype(jnp.float32) + acc + bo_row[:, at]).astype(jnp.bfloat16)

    h_two = normed(x_out[...].astype(jnp.float32), row_of(g2_ref), row_of(c2_ref)).astype(jnp.bfloat16)
    h_out[:, :d_model] = h_two
    logits = lax.dot_general(h_two, wr_ref[...], ALONG, preferred_element_type=jnp.float32)
    experts = logits.shape[1]
    expert_ids = lax.broadcasted_iota(jnp.int32, logits.shape, 1)
    stacked = jnp.concatenate([elig_ref[...], one_ref[...], two_ref[...], jnp.zeros((rows - experts - 2, rows), jnp.int32)], axis=0)
    meta = stacked.astype(jnp.float32).T.astype(jnp.int32)
    pick_one, pick_two = meta[:, experts:experts + 1], meta[:, experts + 1:experts + 2]
    hit_one, hit_two = expert_ids == pick_one, expert_ids == pick_two
    keep_one = meta[:, :experts] == 1

    def gate(keep, hit):
        val = jnp.where(keep, logits, -jnp.inf)
        e_val = jnp.exp(val - jnp.max(val, axis=1, keepdims=True))
        return jnp.sum(jnp.where(hit, e_val, 0.0), axis=1, keepdims=True) / jnp.sum(e_val, axis=1, keepdims=True)

    lane = lax.broadcasted_iota(jnp.int32, gate_out.shape, 1)
    gate_out[...] = jnp.where(lane == 0, gate(keep_one, hit_one), gate(keep_one & jnp.logical_not(hit_one), hit_two))
    ids = jnp.where(lane == 0, pick_one, jnp.where(lane == 1, pick_two, 0))
    h_out[:, d_model:] = ids.astype(jnp.float32).astype(jnp.bfloat16)


def attention_layer(tokens, k_cache, v_cache, positions, expert_one, expert_two, eligible, ln1_gain, ln1_bias, w_query, b_query, w_key, b_key, w_value, b_value, w_out, b_out, ln2_gain, ln2_bias, w_router):
    rows, seq_len, kv_heads, head_dim = k_cache.shape
    d_model = tokens.shape[1]
    heads = w_query.shape[1] // head_dim
    kv_dim = kv_heads * head_dim
    ids = jnp.arange(rows, dtype=jnp.int32)
    ahead = (positions[None, :] > positions[:, None]) | ((positions[None, :] == positions[:, None]) & (ids[None, :] < ids[:, None]))
    rank = jnp.sum(ahead.astype(jnp.int32), axis=1)
    hit = rank[None, :] == ids[:, None]
    order = jnp.sum(jnp.where(hit, ids[None, :], 0), axis=1)
    pos_sorted = jnp.sum(jnp.where(hit, positions[None, :], 0), axis=1)
    half_dim = head_dim // 2
    inv_freq = ROPE_BASE ** (jnp.arange(half_dim, dtype=jnp.float32) * (-2.0 / head_dim))
    angles = positions.astype(jnp.float32)[:, None] * jnp.concatenate([inv_freq, inv_freq])[None, :]
    sign = jnp.where(jnp.arange(head_dim) < half_dim, -1.0, 1.0).astype(jnp.float32)
    small = [p.reshape(-1, LANES) for p in (ln1_gain, ln1_bias, ln2_gain, ln2_bias, b_out, b_query, b_key, b_value)]
    vmem = pl.BlockSpec(memory_space=pltpu.VMEM)
    smem = pl.BlockSpec(memory_space=pltpu.SMEM)
    hbm = pl.BlockSpec(memory_space=pl.ANY)
    flat = (rows, seq_len * kv_heads, head_dim)
    spread = pltpu.VMEM((rows, heads, head_dim), jnp.float32)
    return pl.pallas_call(
        functools.partial(attend_kernel, kv_heads),
        name='attention_layer',
        out_shape=(jax.ShapeDtypeStruct((rows, kv_heads, head_dim), jnp.bfloat16), jax.ShapeDtypeStruct((rows, kv_heads, head_dim), jnp.bfloat16),
                   jax.ShapeDtypeStruct((rows, d_model), jnp.bfloat16), jax.ShapeDtypeStruct((rows, d_model + LANES), jnp.bfloat16),
                   jax.ShapeDtypeStruct((rows, LANES), jnp.float32)),
        in_specs=[smem, smem] + [vmem] * 15 + [hbm, hbm, hbm, hbm, hbm, hbm],
        out_specs=(vmem,) * 5,
        scratch_shapes=[
            pltpu.VMEM((2 * (heads * head_dim + 2 * kv_dim) // TILE, HALF, TILE), jnp.bfloat16),
            pltpu.VMEM((DEPTH, GROUP) + flat[1:], jnp.bfloat16), pltpu.VMEM((DEPTH, GROUP) + flat[1:], jnp.bfloat16),
            spread, spread, spread, spread,
            pltpu.VMEM((rows, kv_heads, head_dim), jnp.float32),
            pltpu.VMEM((rows, d_model), jnp.bfloat16),
            pltpu.VMEM((PART * heads, flat[1]), jnp.int32),
            pltpu.SemaphoreType.DMA((2 * (heads * head_dim + 2 * kv_dim) // TILE,)),
            pltpu.SemaphoreType.DMA((d_model // TILE,)),
            pltpu.SemaphoreType.DMA((DEPTH, 2))],
        compiler_params=pltpu.CompilerParams(vmem_limit_bytes=62 * 1024 * 1024),
    )(order, pos_sorted, tokens, *small, jnp.cos(angles), jnp.sin(angles) * sign[None, :], eligible.T, expert_one[None], expert_two[None], w_router.T, w_query, w_key, w_value, w_out, k_cache.reshape(flat), v_cache.reshape(flat))


def seat(slot):
    return {3: 4, 4: 3}.get(slot, slot)


def flip(me, bit):
    return me + bit - 2 * bit * ((me // bit) % 2)


def meet_neighbours():
    me = lax.axis_index('ep')
    barrier = pltpu.get_barrier_semaphore()
    for bit in (1, 2, 4, 8):
        pl.semaphore_signal(barrier, inc=1, device_id=(flip(me, bit),), device_id_type=MESH)
    pl.semaphore_wait(barrier, 4)
    return me


def gather_kernel(bounds, h_ref, wg_hbm, wu_hbm, z_ref, rel_ref, x_a, x_b, x_c, wg_ref, wu_ref, own_sem, send_sem, recv_sem, side_send, side_recv):
    rows = x_a.shape[1] // 2
    bufs = (x_a, x_b, x_c)
    copies = []
    for f in range(3):
        lo, hi = bounds[f]
        copies.append(pltpu.make_async_copy(h_ref.at[:, pl.ds(lo, hi - lo)], bufs[f].at[0, pl.ds(0, rows)], own_sem.at[f]))
        copies[-1].start()
    me = meet_neighbours()

    def hop(f, src, bit):
        return pltpu.make_async_remote_copy(
            src_ref=bufs[f].at[seat(src), pl.ds(0, rows)], dst_ref=bufs[f].at[seat(src ^ bit), pl.ds(0, rows)],
            send_sem=send_sem.at[f, src ^ bit], recv_sem=recv_sem.at[f, src ^ bit],
            device_id=(flip(me, 2 * bit),), device_id_type=MESH)

    def side(f, src):
        return pltpu.make_async_remote_copy(
            src_ref=bufs[f].at[seat(src), pl.ds(0, rows)], dst_ref=bufs[f].at[seat(src), pl.ds(rows, rows)],
            send_sem=side_send.at[f, src], recv_sem=side_recv.at[f, src],
            device_id=(flip(me, 1),), device_id_type=MESH)

    def landed(f, slot):
        hop(f, 0, slot).wait_recv()

    def activate(place, count=1):
        u_val = v_val = None
        span = pl.ds(place, count)
        for f in range(3):
            lo, hi = bounds[f]
            hi = min(hi, wg_ref.shape[1])
            x_val = bufs[f][span, :, : hi - lo].reshape(2 * rows * count, hi - lo)
            u_part = lax.dot_general(x_val, wg_ref[:, lo:hi], ALONG, preferred_element_type=jnp.float32)
            v_part = lax.dot_general(x_val, wu_ref[:, lo:hi], ALONG, preferred_element_type=jnp.float32)
            u_val = u_part if u_val is None else u_val + u_part
            v_val = v_part if v_val is None else v_val + v_part
        z_ref[span] = (jax.nn.silu(u_val) * v_val).astype(jnp.bfloat16).reshape(count, 2 * rows, -1)
        ids = bufs[2][span, :rows, bounds[2][1] - bounds[2][0] - LANES:]
        rel_ref[span] = ids.astype(jnp.float32).astype(jnp.int32) ^ me

    for f in range(3):
        copies[f].wait()
        hop(f, 0, ORDERS[f][0]).start()
    weights = [pltpu.make_async_copy(src, dst, own_sem.at[3 + i]) for i, (src, dst) in enumerate(((wg_hbm, wg_ref), (wu_hbm, wu_ref)))]
    for f in range(3):
        side(f, 0).start()
    for copy in weights:
        copy.start()
    for stage in (1, 2):
        for f in range(3):
            hop(f, 0, ORDERS[f][stage]).start()
    for f in range(3):
        side(f, 0).wait_recv()
    for copy in weights:
        copy.wait()
    activate(0)
    for f in range(3):
        a, b, g = ORDERS[f]
        landed(f, a)
        hop(f, a, b).start()
        hop(f, a, g).start()
        side(f, a).start()
    for f in range(3):
        a, b, g = ORDERS[f]
        landed(f, b)
        hop(f, b, g).start()
        side(f, b).start()
    for f in range(3):
        a, b, g = ORDERS[f]
        landed(f, a ^ b)
        hop(f, a ^ b, g).start()
        side(f, a ^ b).start()
    for f in range(3):
        g = ORDERS[f][2]
        landed(f, g)
        side(f, g).start()
    for f in range(3):
        for slot in (1, 2, 4):
            side(f, slot).wait_recv()

    @pl.loop(1, 4)
    def _(place):
        activate(place)

    for f in range(3):
        a, b, g = ORDERS[f]
        landed(f, a ^ g)
        side(f, a ^ g).start()
        landed(f, b ^ g)
        side(f, b ^ g).start()
    for f in range(3):
        for slot in (3, 5, 6):
            side(f, slot).wait_recv()

    activate(4, 3)
    for f in range(3):
        landed(f, 7)
        side(f, 7).start()
    for f in range(3):
        side(f, 7).wait_recv()
    activate(7)
    for f in range(3):
        for slot in range(8):
            side(f, slot).wait_send()
        for slot in range(1, 8):
            hop(f, 0, slot).wait_send()


def return_kernel(z_hbm, wd_hbm, rel_ref, gate_ref, x_hbm, out_ref, z_ref, wd_ref, x_ref, in_sem, pair_buf, side_buf, near_buf, turn_buf, turn_in, last_buf, last_in, side_send, side_recv, hop_send, hop_recv):
    rows = x_ref.shape[0]
    chunks = pair_buf.shape[0]
    loads = [pltpu.make_async_copy(src, dst, in_sem.at[i]) for i, (src, dst) in enumerate(((z_hbm, z_ref), (wd_hbm, wd_ref), (x_hbm, x_ref)))]
    for copy in loads:
        copy.start()
    me = meet_neighbours()

    def slot_of(f, place):
        a, b, g = ORDERS[f]
        return a * (place // 4) + b * (place // 2 % 2) + g * (place % 2)

    def remote(src, dst, send, recv, bit):
        return pltpu.make_async_remote_copy(src_ref=src, dst_ref=dst, send_sem=send, recv_sem=recv, device_id=(flip(me, bit),), device_id_type=MESH)

    def side(part):
        f, q, s, lo, width = part
        cols = pl.ds(lo, width)
        return remote(side_buf.at[q, :, cols], pair_buf.at[q, 1, :, cols], side_send.at[s], side_recv.at[s], 1)

    def hop_one(part):
        f, q, s, lo, width = part
        cols = pl.ds(lo, width)
        return remote(pair_buf.at[q, :, pl.ds(4 * rows, 4 * rows), cols], near_buf.at[q, :, :, cols], hop_send.at[0, s], hop_recv.at[0, s], 2 * ORDERS[f][0])

    def hop_two(part):
        f, q, s, lo, width = part
        cols = pl.ds(lo, width)
        return remote(turn_buf.at[q, :, :, cols], turn_in.at[q, :, :, cols], hop_send.at[1, s], hop_recv.at[1, s], 2 * ORDERS[f][1])

    def hop_three(part):
        f, q, s, lo, width = part
        cols = pl.ds(lo, width)
        return remote(last_buf.at[q, :, :, cols], last_in.at[q, :, :, cols], hop_send.at[2, s], hop_recv.at[2, s], 2 * ORDERS[f][2])

    def project(part):
        f, q, s, lo, width = part
        w_val = wd_ref[:, pl.ds(pl.multiple_of(q * WIDTH + lo, LANES), width)]
        for place in range(8):
            e_val = jnp.dot(z_ref[seat(slot_of(f, place))], w_val, preferred_element_type=jnp.float32).astype(jnp.bfloat16)
            pair_buf[q, 0, place * rows:(place + 1) * rows, lo:lo + width] = e_val[:rows]
            side_buf[q, place * rows:(place + 1) * rows, lo:lo + width] = e_val[rows:]
        side(part).start()

    def send_far(part):
        side(part).wait_recv()
        hop_one(part).start()

    def choose(part, place, k, other):
        f, q, s, lo, width = part
        rel = rel_ref[seat(slot_of(f, place))][:, k:k + 1]
        at, cols = pl.ds(place * rows, rows), pl.ds(lo, width)
        far = 2 * ORDERS[f][0]
        val = near_buf[q, 1, at, cols].astype(jnp.float32)
        if other is not None:
            val = jnp.where(rel == far + 1, val, other)
        val = jnp.where(rel == far, near_buf[q, 0, at, cols].astype(jnp.float32), val)
        val = jnp.where(rel == 1, pair_buf[q, 1, at, cols].astype(jnp.float32), val)
        return jnp.where(rel == 0, pair_buf[q, 0, at, cols].astype(jnp.float32), val)

    def turn(part):
        f, q, s, lo, width = part
        hop_one(part).wait_recv()
        for k in range(2):
            for half in range(2):
                turn_buf[q, k, half * rows:(half + 1) * rows, lo:lo + width] = choose(part, 2 + half, k, None).astype(jnp.bfloat16)
        hop_two(part).start()

    def last(part):
        f, q, s, lo, width = part
        hop_two(part).wait_recv()
        for k in range(2):
            other = turn_in[q, k, rows:2 * rows, lo:lo + width].astype(jnp.float32)
            last_buf[q, k, :, lo:lo + width] = choose(part, 1, k, other).astype(jnp.bfloat16)
        hop_three(part).start()

    def finish(part):
        f, q, s, lo, width = part
        hop_three(part).wait_recv()
        g_bit = 2 * ORDERS[f][2]
        y_val = None
        for k in range(2):
            rel = rel_ref[0][:, k:k + 1]
            other = jnp.where((rel // g_bit) % 2 == 1, last_in[q, k, :, lo:lo + width].astype(jnp.float32), turn_in[q, k, :rows, lo:lo + width].astype(jnp.float32))
            add = gate_ref[:, k:k + 1] * choose(part, 0, k, other)
            y_val = add if y_val is None else y_val + add
        at = pl.ds(pl.multiple_of(q * WIDTH + lo, LANES), width)
        out_ref[:, at] = (x_ref[:, at].astype(jnp.float32) + y_val).astype(jnp.bfloat16)

    full = chunks // 3
    tail = [(f, chunks - 1, chunks - 1 + f, f * LANES, LANES) for f in range(2)]

    def body(f, j):
        return f, 3 * j + f, 3 * j + f, 0, WIDTH

    def sweep(step):
        @pl.loop(0, full)
        def _(j):
            for f in range(3):
                step(body(f, j))
        for part in tail:
            step(part)

    for copy in loads[:2]:
        copy.wait()
    for f in range(3):
        project(body(f, 0))

    @pl.loop(1, full)
    def _(j):
        for f in range(3):
            project(body(f, j))
            send_far(body(f, j - 1))

    for part in tail:
        project(part)
    for part in [body(f, full - 1) for f in range(3)] + tail:
        send_far(part)
    sweep(turn)
    sweep(last)
    loads[2].wait()
    sweep(finish)

    def drain(part):
        side(part).wait_send()
        hop_one(part).wait_send()
        hop_two(part).wait_send()
        hop_three(part).wait_send()
    sweep(drain)


def gather_and_activate(h_ext, w_gate, w_up):
    rows, d_model = h_ext.shape[0], h_ext.shape[1] - LANES
    d_ff = w_gate.shape[0]
    tiles = (d_model + LANES) // LANES
    cuts = [LANES * ((tiles * f + 2) // 3) for f in range(4)]
    bounds = tuple((cuts[f], cuts[f + 1]) for f in range(3))
    vmem = pl.BlockSpec(memory_space=pltpu.VMEM)
    return pl.pallas_call(
        functools.partial(gather_kernel, bounds),
        name='gather_rows',
        out_shape=(jax.ShapeDtypeStruct((8, 2 * rows, d_ff), jnp.bfloat16), jax.ShapeDtypeStruct((8, rows, LANES), jnp.int32)),
        in_specs=[pl.BlockSpec(memory_space=pltpu.HBM)] * 3,
        out_specs=(vmem, vmem),
        scratch_shapes=[pltpu.VMEM((8, 2 * rows, hi - lo), jnp.bfloat16) for lo, hi in bounds] + [
            pltpu.VMEM(w_gate.shape, jnp.bfloat16), pltpu.VMEM(w_gate.shape, jnp.bfloat16),
            pltpu.SemaphoreType.DMA((5,)),
            pltpu.SemaphoreType.DMA((3, 8)), pltpu.SemaphoreType.DMA((3, 8)),
            pltpu.SemaphoreType.DMA((3, 8)), pltpu.SemaphoreType.DMA((3, 8))],
        compiler_params=pltpu.CompilerParams(collective_id=0, has_side_effects=True, vmem_limit_bytes=60 * 1024 * 1024),
    )(h_ext, w_gate, w_up)


def project_and_return(z_val, w_down, rel, gates, x_mid):
    rows, d_model = x_mid.shape
    chunks = d_model // WIDTH
    hbm = pl.BlockSpec(memory_space=pltpu.HBM)
    vmem = pl.BlockSpec(memory_space=pltpu.VMEM)
    return pl.pallas_call(
        return_kernel,
        name='return_rows',
        out_shape=jax.ShapeDtypeStruct((rows, d_model), jnp.bfloat16),
        in_specs=[hbm, hbm, vmem, vmem, hbm],
        out_specs=vmem,
        scratch_shapes=[
            pltpu.VMEM(z_val.shape, jnp.bfloat16), pltpu.VMEM(w_down.shape, jnp.bfloat16), pltpu.VMEM(x_mid.shape, jnp.bfloat16), pltpu.SemaphoreType.DMA((3,)),
            pltpu.VMEM((chunks, 2, 8 * rows, WIDTH), jnp.bfloat16),
            pltpu.VMEM((chunks, 8 * rows, WIDTH), jnp.bfloat16),
            pltpu.VMEM((chunks, 2, 4 * rows, WIDTH), jnp.bfloat16),
            pltpu.VMEM((chunks, 2, 2 * rows, WIDTH), jnp.bfloat16),
            pltpu.VMEM((chunks, 2, 2 * rows, WIDTH), jnp.bfloat16),
            pltpu.VMEM((chunks, 2, rows, WIDTH), jnp.bfloat16),
            pltpu.VMEM((chunks, 2, rows, WIDTH), jnp.bfloat16),
            pltpu.SemaphoreType.DMA((chunks + 1,)), pltpu.SemaphoreType.DMA((chunks + 1,)),
            pltpu.SemaphoreType.DMA((3, chunks + 1)), pltpu.SemaphoreType.DMA((3, chunks + 1))],
        compiler_params=pltpu.CompilerParams(collective_id=1, has_side_effects=True, vmem_limit_bytes=63 * 1024 * 1024),
    )(z_val, w_down, rel, gates, x_mid)


def solution(mesh):
    def local_step(tokens, k_cache, v_cache, positions, expert_one, expert_two, eligible, ln1_gain, ln1_bias, w_query, b_query, w_key, b_key, w_value, b_value, w_out, b_out, ln2_gain, ln2_bias, w_router, w_gate, w_up, w_down):
        key_new, value_new, x_mid, h_ext, gates = attention_layer(tokens, k_cache, v_cache, positions, expert_one, expert_two, eligible, ln1_gain, ln1_bias, w_query, b_query, w_key, b_key, w_value, b_value, w_out, b_out, ln2_gain, ln2_bias, w_router)
        z_val, rel = gather_and_activate(h_ext, w_gate[0].T, w_up[0].T)
        tokens_out = project_and_return(z_val, w_down[0], rel, gates, x_mid)
        return tokens_out, key_new, value_new

    row_spec = P('ep', None)
    cache_spec = P('ep', None, None, None)
    vec_spec = P('ep')
    rep_one = P(None)
    rep_two = P(None, None)
    expert_spec = P('ep', None, None)
    in_specs = (row_spec, cache_spec, cache_spec, vec_spec, vec_spec, vec_spec, row_spec, rep_one, rep_one, rep_two, rep_one, rep_two, rep_one, rep_two, rep_one, rep_two, rep_one, rep_one, rep_one, rep_two, expert_spec, expert_spec, expert_spec)
    out_specs = (row_spec, expert_spec, expert_spec)
    return jax.shard_map(local_step, mesh=mesh, in_specs=in_specs, out_specs=out_specs, check_vma=False)
```
